32 devices in a mesh: gy: 4 (over z), gx: 8 (over y, x, core).
Axes of the slice: x: 2, y: 2, z: 4, core: 2. Of those that a mesh axis runs over, the one named last changes fastest.
Arguments:
- height: float32 [384, 512], P('gx', 'gy'), may hold values from -6 to 6
- east_speed: float32 [384, 512], P('gx', 'gy'), may hold values from -3 to 3
- north_speed: float32 [384, 512], P('gx', 'gy'), may hold values from -3 to 3
- water_depth: float32 [384, 512], P('gx', 'gy'), may hold values from 0.5 to 2
- ocean_mask: int32 [384, 512], P('gx', 'gy'), may hold values 0 or 1
- fold_partner: int32 [8], replicated, may hold values from 0 to 7, each once
- love_factor: float32 [360], replicated, may hold values from 0.1 to 1
Outputs:
- sal_field: float32 [384, 512], P('gx', 'gy')
- east_next: float32 [384, 512], P('gx', 'gy')
- north_next: float32 [384, 512], P('gx', 'gy')
- height_next: float32 [384, 512], P('gx', 'gy')
The draws below stay inside these ranges and needn't reach their ends.
Inputs may be any that keep to these rules, and one draw needn't show every extreme that they name: `fold_partner`: a permutation of the tile columns.
All inputs are finite; a program needn't handle non-finite values. No bound on the sum of `ocean_mask` on one device may be relied on, other than what follows from the above.
Results may differ from the reference program's by a relative error of at most 0.00055.
Values sent between devices are 32-bit elements; how exact they have to be, the bound alone decides.
No kernel may reach another device: no remote copies, remote signals or barrier semaphores. Data moves between devices by JAX's collectives and lax.ppermute only.
A program may use at most 64 MiB of HBM per device.

```python
import math
import jax
import jax.numpy as jnp
from jax import lax

CLON = 48
L = 360
NLON = 384
NLAT = 512
N_GX = 8


def set_ends(entries, rng, smallest, top_value):
    longest = entries.shape.index(max(entries.shape))
    spots = []
    for shift in (0, 1):
        where = [jax.random.randint(jax.random.fold_in(rng, axis), (), 0, length) for axis, length in enumerate(entries.shape)]
        where[longest] = (where[longest] + shift) % entries.shape[longest]
        spots.append(tuple(where))
    return entries.at[spots[0]].set(smallest).at[spots[1]].set(top_value)


def block_levels(key, dims, cuts, low, top_value):
    factor_of = 1.0
    for axis_at, parts in cuts:
        steps = jax.random.uniform(jax.random.fold_in(jax.random.fold_in(key, 6), axis_at), (parts,), jnp.float32, low / len(cuts), top_value / len(cuts))
        factor_of = factor_of * jnp.repeat(jnp.exp(steps), dims[axis_at] // parts).reshape((-1,) + (1,) * (len(dims) - 1 - axis_at))
    return factor_of


def noise(rng, extent, spread, reach, pieces=(), kind=jnp.bfloat16):
    array = jax.random.normal(rng, extent, jnp.float32) * spread
    if len(pieces) > 0:
        array = block_levels(rng, extent, pieces, -0.22, 0.18) * array
    return jnp.clip(array, min=-reach, max=reach).astype(kind)


def setup_inputs(seed: int = 0) -> dict:
    arg_keys = jax.random.split(jax.random.key(seed), 8)
    height = noise(arg_keys[0], (NLON, NLAT), 1.0, 6.0, ((0, 8), (1, 4)), jnp.float32)
    east_speed = noise(arg_keys[1], (NLON, NLAT), 0.5, 3.0, ((0, 8), (1, 4)), jnp.float32)
    north_speed = noise(arg_keys[2], (NLON, NLAT), 0.5, 3.0, ((0, 8), (1, 4)), jnp.float32)
    water_depth = jnp.clip(jnp.exp(math.log(2.0) - 1.3862944 * jax.random.uniform(arg_keys[3], (NLON, NLAT), jnp.float32) ** block_levels(arg_keys[3], (NLON, NLAT), ((0, 8), (1, 4)), -0.2, 0.2)), 0.5, 2.0)
    ocean_mask = set_ends((jax.random.randint(arg_keys[4], (NLON, NLAT), 0, 5) < 4).astype(jnp.int32), jax.random.fold_in(arg_keys[4], 1), 0, 1)
    fold_partner = jax.random.permutation(arg_keys[5], N_GX).astype(jnp.int32)
    love_factor = jnp.clip(jnp.exp(jax.random.uniform(arg_keys[6], (L,), jnp.float32, math.log(0.1), math.log(1.0))), 0.1, 1.0)
    return {"height": height, "east_speed": east_speed, "north_speed": north_speed, "water_depth": water_depth, "ocean_mask": ocean_mask, "fold_partner": fold_partner, "love_factor": love_factor}


COURANT = 0.35

def trig_rows(first_column, number, lon_total, degrees):
    columns = first_column + jnp.arange(number, dtype=jnp.int32)
    orders = jnp.arange(degrees, dtype=jnp.int32)
    phases = columns[:, None] * orders[None, :] % lon_total
    angles = phases.astype(jnp.float32) * (2.0 * math.pi / lon_total)
    return jnp.concatenate([jnp.cos(angles), jnp.sin(angles)], axis=1)

def latitude_rows(first_row, number, lat_total, lon_total):
    rows_float = (first_row + jnp.arange(number, dtype=jnp.int32)).astype(jnp.float32)
    colatitude = math.pi * (rows_float + 0.5) / lat_total
    sines = jnp.sin(colatitude)
    quadrature = math.pi / lat_total * (2.0 * math.pi / lon_total) * sines
    return (jnp.cos(colatitude), sines, quadrature)

def seed_values(sines, degrees):
    orders = jnp.arange(degrees, dtype=jnp.float32)
    factors = jnp.arange(1, degrees, dtype=jnp.float32)
    increments = 0.5 * jnp.log((2.0 * factors + 1.0) / (2.0 * factors))
    seed_logs = jnp.concatenate([jnp.zeros((1,), jnp.float32), jnp.cumsum(increments)])
    exponent = orders[None, :] * jnp.log(sines)[:, None] + seed_logs[None, :]
    log_shift = jnp.clip(-exponent - 80.0, 0.0, 80.0)
    return (jnp.exp(exponent + log_shift) * (1.0 / math.sqrt(4.0 * math.pi)), jnp.exp(-log_shift))

def legendre_next(carry, degree, cosines, seed_rows, orders):
    previous, before = carry
    degree_value = degree.astype(jnp.float32)
    below_value = degree_value - 1.0
    growth = jnp.sqrt(jnp.maximum(4.0 * degree_value * degree_value - 1.0, 1.0) / jnp.maximum(degree_value * degree_value - orders * orders, 1.0))
    damping = jnp.sqrt(jnp.maximum(below_value * below_value - orders * orders, 0.0) / jnp.maximum(4.0 * below_value * below_value - 1.0, 1.0))
    stepped = growth[None, :] * (cosines[:, None] * previous - damping[None, :] * before)
    values = jnp.where(degree_value == orders[None, :], seed_rows, jnp.where(degree_value > orders[None, :], stepped, 0.0))
    return ((values, previous), values)

def reference(height, east_speed, north_speed, water_depth, ocean_mask, fold_partner, love_factor):
    lon_count = height.shape[0]
    lat_count = height.shape[1]
    degrees = love_factor.shape[0]
    wet_cells = ocean_mask.astype(jnp.float32)
    surface = wet_cells * height
    cosines, sines, quadrature = latitude_rows(0, lat_count, lat_count, lon_count)
    trig = trig_rows(0, lon_count, lon_count, degrees)
    fourier = lax.dot_general(surface, trig, (((0,), (0,)), ((), ())), precision=lax.Precision.HIGHEST)
    weighted = fourier * quadrature[:, None]
    orders = jnp.arange(degrees, dtype=jnp.float32)
    seed_rows, unscale = seed_values(sines, degrees)
    empty = jnp.zeros((lat_count, degrees), jnp.float32)

    def analyse(carry, degree):
        recurrence, scaled_values = legendre_next(carry, degree, cosines, seed_rows, orders)
        values = scaled_values * unscale
        cos_part = lax.optimization_barrier(jnp.sum(values * weighted[:, :degrees], axis=0))
        sin_part = lax.optimization_barrier(jnp.sum(values * weighted[:, degrees:], axis=0))
        return (recurrence, jnp.stack([cos_part, sin_part]))
    degree_list = jnp.arange(degrees, dtype=jnp.int32)
    finished, spectrum = lax.scan(analyse, (empty, empty), degree_list)
    multiplicity = jnp.where(jnp.arange(degrees) == 0, 1.0, 2.0).astype(jnp.float32)
    scaled = spectrum * love_factor[:, None, None] * multiplicity[None, None, :]

    def synthesise(carry, inputs):
        degree, coeff_rows = inputs
        recurrence, scaled_values = legendre_next(carry[0], degree, cosines, seed_rows, orders)
        values = scaled_values * unscale
        total = carry[1] + jnp.concatenate([values * coeff_rows[0][None, :], values * coeff_rows[1][None, :]], axis=1)
        return ((recurrence, total), None)
    start_total = jnp.zeros((lat_count, 2 * degrees), jnp.float32)
    (finished_two, grid_terms), unused = lax.scan(synthesise, ((empty, empty), start_total), (degree_list, scaled))
    sal_field = lax.dot_general(trig, grid_terms, (((1,), (1,)), ((), ())), precision=lax.Precision.HIGHEST)
    pressure = surface - sal_field
    columns = jnp.arange(lon_count, dtype=jnp.int32)
    partner_columns = fold_partner[columns // CLON] * CLON + (CLON - 1 - columns % CLON)

    def north_of(field):
        return jnp.concatenate([field[:, 1:], field[partner_columns, lat_count - 1][:, None]], axis=1)

    def east_of(field):
        return jnp.roll(field, -1, axis=0)
    east_next = wet_cells * east_of(wet_cells) * (east_speed - COURANT * (east_of(pressure) - pressure))
    north_next = wet_cells * north_of(wet_cells) * (north_speed - COURANT * (north_of(pressure) - pressure))
    east_flux = 0.5 * (water_depth + east_of(water_depth)) * east_next
    north_flux = 0.5 * (water_depth + north_of(water_depth)) * north_next
    west_flux = jnp.roll(east_flux, 1, axis=0)
    south_flux = jnp.concatenate([jnp.zeros((lon_count, 1), jnp.float32), north_flux[:, :-1]], axis=1)
    height_next = wet_cells * (surface - COURANT * (east_flux - west_flux + north_flux - south_flux))
    return (sal_field, east_next, north_next, height_next)
```

```python
import math

import numpy as np

import jax
import jax.numpy as jnp
from jax import lax
from jax.experimental import pallas as pl
from jax.experimental.pallas import tpu as pltpu
from jax.sharding import PartitionSpec as P

COURANT = 0.35
GROUP = 8
STEPS = 32
ROWS = GROUP * STEPS
CHAINS = 2
EDGE = 8
F32 = jnp.float32
BF16 = jnp.bfloat16
HIGHEST = lax.Precision.HIGHEST


class Plan:
    def __init__(self, tile_lon, tile_lat, n_gx, n_gy, degrees):
        self.tile_lon, self.tile_lat = tile_lon, tile_lat
        self.n_gx, self.n_gy, self.degrees = n_gx, n_gy, degrees
        self.nlon, self.nlat = tile_lon * n_gx, tile_lat * n_gy
        self.half = self.nlat // 2
        self.n_groups = -(-degrees // GROUP)
        self.n_slots = -(-self.n_groups // n_gx)
        self.k_dev = 2 * self.n_slots * GROUP
        self.k_all = self.k_dev * n_gx
        self.group_of = np.array(
            [
                [s * n_gx + (c if s % 2 == 0 else n_gx - 1 - c) for s in range(self.n_slots)]
                for c in range(n_gx)
            ],
            np.int32,
        )
        self._schedule()
        self._tables()

    def _schedule(self):
        per_device = []
        for c in range(self.n_gx):
            work = []
            for s in range(self.n_slots):
                left = self.degrees - GROUP * int(self.group_of[c, s])
                if left > 0:
                    work.append((-(-left // STEPS), s))
            work.sort(reverse=True)
            chains = [[] for _ in range(CHAINS)]
            for chunks, s in work:
                chain = min(chains, key=len)
                chain.extend((s, k) for k in range(chunks))
            per_device.append(chains)
        longest = max(len(chain) for chains in per_device for chain in chains)
        self.n_iter = longest + longest % 2
        length = self.n_iter + 1
        table = np.zeros((self.n_gx, length, CHAINS, 2), np.int32)
        window = 0
        for c, chains in enumerate(per_device):
            for h, chain in enumerate(chains):
                filled = list(chain)
                while len(filled) < length:
                    s, k = filled[-1] if filled else (0, 0)
                    idle = -(-self.degrees // STEPS)
                    filled.append((s, max(k + 1, idle)))
                for i, (s, k) in enumerate(filled):
                    table[c, i, h] = (s, k)
                    window = max(window, int(self.group_of[c, s]) + k * (STEPS // GROUP))
        self.sched = table.reshape(-1)
        self.sched_stride = length * CHAINS * 2
        self.n_windows = -(-(window + 1) // 8) * 8
        self.love_rows = self.n_windows + 8

    def _tables(self):
        rows = np.arange(self.half)
        theta = np.pi * (rows + 0.5) / self.nlat
        self.geo = np.zeros((8, self.half), np.float32)
        self.geo[0] = np.cos(theta)
        self.geo[1] = np.log(np.sin(theta))
        all_theta = np.pi * (np.arange(self.nlat) + 0.5) / self.nlat
        quad = np.pi / self.nlat * (2.0 * np.pi / self.nlon) * np.sin(all_theta)
        self.quad = np.repeat(
            quad.reshape(self.n_gy, 1, self.tile_lat), 8, axis=1
        ).astype(np.float32)
        top = GROUP * (int(self.group_of.max()) + 1)
        factors = np.arange(1, top, dtype=np.float64)
        logs = np.concatenate([[0.0], np.cumsum(0.5 * np.log((2 * factors + 1) / (2 * factors)))])
        orders = self.group_of[:, :, None] * GROUP + np.arange(GROUP)[None, None, :]
        self.seed_logs = np.repeat(
            logs[orders].reshape(self.n_gx, self.n_slots * GROUP, 1), 128, axis=2
        ).astype(np.float32)
        lam = 2.0 * np.pi / self.nlon
        cols = np.arange(self.nlon)
        base = (self.group_of[:, :, None] * GROUP * cols[None, None, :]) % self.nlon
        u = np.stack([np.cos(lam * base), np.sin(lam * base)], axis=2)
        pad = -(-2 * self.n_slots // 8) * 8
        self.u_rows = pad
        self.u_table = np.zeros((self.n_gx, pad, self.nlon), np.float32)
        self.u_table[:, : 2 * self.n_slots] = u.reshape(self.n_gx, 2 * self.n_slots, self.nlon)
        small = (np.arange(GROUP)[:, None] * cols[None, :]) % self.nlon
        self.v_table = np.concatenate([np.cos(lam * small), np.sin(lam * small)]).astype(np.float32)
        m = np.concatenate(
            [np.tile(orders[c].reshape(-1), 2) for c in range(self.n_gx)]
        )
        sine = np.tile(np.repeat([0, 1], self.k_dev // 2), self.n_gx)
        nu = np.where(m == 0, 1.0, 2.0) * (m < self.degrees)
        starts = np.arange(self.n_gx) * self.tile_lon
        phase = lam * ((starts[:, None] * m[None, :]) % self.nlon)
        a1 = nu * np.where(sine == 0, np.cos(phase), np.sin(phase))
        a2 = nu * np.where(sine == 0, -np.sin(phase), np.cos(phase))
        self.a_table = np.zeros((self.n_gx, 8, self.k_all), np.float32)
        self.a_table[:, 0] = a1
        self.a_table[:, 1] = a2
        offsets = np.concatenate(
            [
                np.arange(self.tile_lon),
                [self.tile_lon, -1],
                np.zeros(EDGE - 2),
                np.arange(self.tile_lon)[::-1],
            ]
        ).astype(np.int64)
        phase = lam * ((offsets[:, None] * m[None, :]) % self.nlon)
        self.b_table = np.stack([np.cos(phase), np.sin(phase)]).astype(np.float32)
        self.o_rows = offsets.shape[0]


def iota(shape, axis):
    return lax.broadcasted_iota(jnp.int32, shape, axis)


def dot(a, b):
    return lax.dot_general(
        a, b, (((1,), (0,)), ((), ())), precision=HIGHEST, preferred_element_type=F32
    )


def flip_matrix(size, flipped):
    row = iota((size, size), 0)
    col = iota((size, size), 1)
    target = jnp.where(flipped, size - 1 - col, col)
    return jnp.where(row == target, 1.0, 0.0).astype(F32)


def pack_kernel(height, mask, depth, east, out, surface_out):
    lon, lat = height.shape
    wet = mask[...].astype(F32)
    surface = wet * height[...]
    surface_out[...] = surface
    out[:lon, :] = surface
    out[lon : lon + 1, :] = depth[:1, :]
    out[lon + 1 : lon + 2, :] = wet[:1, :]
    out[lon + 2 : lon + 3, :] = depth[lon - 1 :, :]
    out[lon + 3 : lon + 4, :] = wet[lon - 1 :, :]
    out[lon + 4 : lon + 5, :] = east[lon - 1 :, :]
    out[lon + 5 : lon + EDGE, :] = jnp.zeros((EDGE - 5, lat), F32)
    lane = iota((lon, lat), 1)
    out[lon + EDGE :, :] = jnp.where(
        lane == 0, depth[:, lat - 1 :], jnp.where(lane == 1, wet[:, lat - 1 :], 0.0)
    )


def fourier_kernel(plan, idx, fold, gathered, u, v, quad, surface, depth, mask, north, out, edges):
    lon, lat = plan.tile_lon, plan.tile_lat
    n_gx, slots = plan.n_gx, plan.n_slots
    c, r = idx[0], idx[1]
    field = jnp.concatenate([gathered[d, :lon, :] for d in range(n_gx)], axis=0)
    vc, vs = v[:GROUP, :], v[GROUP:, :]
    cos_rows, sin_rows = [], []
    for s in range(slots):
        uc = u[0, 2 * s : 2 * s + 1, :]
        us = u[0, 2 * s + 1 : 2 * s + 2, :]
        cos_rows.append(uc * vc - us * vs)
        sin_rows.append(us * vc + uc * vs)
    trig = jnp.concatenate(cos_rows + sin_rows, axis=0)
    sums = dot(trig, field) * quad[0, :1, :]
    out[lon:, :] = dot(sums, flip_matrix(lat, r >= plan.n_gy // 2))
    wet = mask[...].astype(F32)
    lane = iota((lon, lat), 1)
    tile = jnp.zeros((lon, lat), F32)
    last = [surface, depth, wet, north]
    for k, array in enumerate(last):
        tile = jnp.where(lane == k, array[:, lat - 1 :], tile)
    for k, array in enumerate([surface, depth, wet]):
        tile = jnp.where(lane == 4 + k, array[:, :1], tile)
    out[:lon, :] = tile
    after = lax.rem(c + 1, n_gx)
    before = lax.rem(c + n_gx - 1, n_gx)
    partner = fold[c]
    edges[0:1, :] = gathered[after, 0:1, :]
    edges[1:3, :] = gathered[after, lon : lon + 2, :]
    edges[3:4, :] = gathered[before, lon - 1 : lon, :]
    edges[4:7, :] = gathered[before, lon + 2 : lon + 5, :]
    edges[7:8, :] = jnp.zeros((1, lat), F32)
    across = jnp.where(
        lane == 2, gathered[partner, :lon, lat - 1 :], gathered[partner, lon + EDGE :, :]
    )
    edges[EDGE:, :] = dot(flip_matrix(lon, True), across)


def legendre_kernel(plan, idx, sched, *refs):
    n_gy, slots, half = plan.n_gy, plan.n_slots, plan.half
    lon, lat, k_half = plan.tile_lon, plan.tile_lat, plan.k_dev // 2
    blocks = refs[:n_gy]
    geo, seed_logs, love, out = refs[n_gy : n_gy + 4]
    (fabs, lhs, seeds, unscale, windows, acc, state, p_hi0, p_lo0, p_hi1, p_lo1, north_b, south_b) = refs[
        n_gy + 4 :
    ]
    c, r = idx[0], idx[1]
    n_half = n_gy // 2
    for k in range(n_gy):
        fabs[lax.rem(r - k + n_gy, n_gy)] = blocks[k][lon:, :]
    sym, anti = [], []
    for b in range(n_half):
        north, south = fabs[b], fabs[n_gy - 1 - b]
        sym.append(north + south)
        anti.append(north - south)
    sym = jnp.concatenate(sym, axis=1)
    anti = jnp.concatenate(anti, axis=1)
    log_sin = geo[1:2, :]
    sub = iota((GROUP, half), 0)
    for s in range(slots):
        lo, hi = s * GROUP, (s + 1) * GROUP
        rows = jnp.concatenate(
            [sym[lo:hi], anti[lo:hi], sym[k_half + lo : k_half + hi], anti[k_half + lo : k_half + hi]],
            axis=0,
        )
        rows_hi = rows.astype(BF16)
        lhs[s, : 4 * GROUP, :] = rows_hi
        lhs[s, 4 * GROUP :, :] = (rows - rows_hi.astype(F32)).astype(BF16)
        group = s * plan.n_gx + (c if s % 2 == 0 else plan.n_gx - 1 - c)
        order = (sub + group * GROUP).astype(F32)
        logs = jnp.concatenate([seed_logs[0, lo:hi, :]] * (half // 128), axis=1)
        exponent = order * log_sin + logs
        shift = jnp.clip(-exponent - 80.0, 0.0, 80.0)
        seeds[s] = jnp.exp(exponent + shift) * (1.0 / math.sqrt(4.0 * math.pi))
        unscale[s] = jnp.exp(-shift)
    acc[...] = jnp.zeros(acc.shape, F32)
    state[...] = jnp.zeros(state.shape, F32)
    spread = jnp.zeros((plan.n_windows, ROWS), F32)
    per = STEPS // GROUP
    for q in range(per):
        lane_degree = iota((GROUP, ROWS), 1) // GROUP - q * GROUP
        select = jnp.where(lane_degree == iota((GROUP, ROWS), 0), 1.0, 0.0).astype(F32)
        spread = spread + dot(love[q : q + plan.n_windows, :], select)
    windows[...] = spread.reshape(plan.n_windows, 1, ROWS)
    x = jnp.broadcast_to(geo[0:1, :], (GROUP, half))
    row = iota((4 * GROUP, ROWS), 0)
    lane = iota((4 * GROUP, ROWS), 1)
    i_row, i_lane, t_lane = row % GROUP, lane % GROUP, lane // GROUP
    keep = jnp.where(
        (i_row == i_lane) & ((t_lane + i_row) % 2 == (row // GROUP) % 2), 1.0, 0.0
    ).astype(F32)
    sub_c = iota((GROUP, 128), 0)
    lane_c = iota((GROUP, 128), 1)
    base = c * plan.sched_stride

    def item(i, h):
        at = base + (i * CHAINS + h) * 2
        slot, chunk = sched[at], sched[at + 1]
        even = lax.rem(slot, 2) == 0
        group = slot * plan.n_gx + jnp.where(even, c, plan.n_gx - 1 - c)
        return slot, chunk, group

    def generate(i, h, p_hi, p_lo):
        slot, chunk, group = item(i, h)
        first = chunk == 0
        m0 = group * GROUP
        degree = (m0 + chunk * STEPS + lane_c).astype(F32)
        order = (m0 + sub_c).astype(F32)
        below = degree - 1.0
        growth = jnp.sqrt(
            jnp.maximum(4.0 * degree * degree - 1.0, 1.0)
            / jnp.maximum(degree * degree - order * order, 1.0)
        )
        damping = jnp.sqrt(
            jnp.maximum(below * below - order * order, 0.0)
            / jnp.maximum(4.0 * below * below - 1.0, 1.0)
        )
        fall = growth * damping
        started = jnp.where(first, 0.0, 1.0).astype(F32)
        previous = state[h, 0] * started
        before = state[h, 1] * started
        seed = seeds[slot] * (1.0 - started)
        scale = unscale[slot]
        pair = []
        for t in range(STEPS):
            a = jnp.broadcast_to(growth[:, t : t + 1], (GROUP, half))
            b = jnp.broadcast_to(fall[:, t : t + 1], (GROUP, half))
            value = (a * x) * previous - b * before
            if t < GROUP:
                value = value + jnp.where(sub == t, seed, 0.0)
            previous, before = value, previous
            pair.append(value * scale)
            if t % 2 == 1:
                both = jnp.concatenate(pair, axis=0)
                both_hi = both.astype(BF16)
                at = (t - 1) * GROUP
                p_hi[h, at : at + 2 * GROUP, :] = both_hi
                p_lo[h, at : at + 2 * GROUP, :] = (both - both_hi.astype(F32)).astype(BF16)
                pair = []
        state[h, 0] = previous
        state[h, 1] = before

    def transform(i, h, p_hi, p_lo):
        slot, chunk, group = item(i, h)
        nt = (((1,), (1,)), ((), ()))
        nn = (((1,), (0,)), ((), ()))
        hi, lo = p_hi[h], p_lo[h]
        left = lhs[slot]
        n = 4 * GROUP
        one = lax.dot_general(left, hi, nt, preferred_element_type=F32)
        two = lax.dot_general(left[:n], lo, nt, preferred_element_type=F32)
        coeff = (one[:n] + one[n:] + two) * keep * windows[group + chunk * per]
        coeff_hi = coeff.astype(BF16)
        coeff_lo = (coeff - coeff_hi.astype(F32)).astype(BF16)
        right = jnp.concatenate([coeff_hi, coeff_lo], axis=0)
        three = lax.dot_general(right, hi, nn, preferred_element_type=F32)
        four = lax.dot_general(coeff_hi, lo, nn, preferred_element_type=F32)
        acc[slot] += three[:n] + three[n:] + four

    for h in range(CHAINS):
        generate(0, h, p_hi0, p_lo0)

    def body(k, carry):
        for h in range(CHAINS):
            transform(2 * k, h, p_hi0, p_lo0)
        for h in range(CHAINS):
            generate(2 * k + 1, h, p_hi1, p_lo1)
        for h in range(CHAINS):
            transform(2 * k + 1, h, p_hi1, p_lo1)
        for h in range(CHAINS):
            generate(2 * k + 2, h, p_hi0, p_lo0)
        return carry

    lax.fori_loop(0, plan.n_iter // 2, body, 0)

    for s in range(slots):
        lo, hi = s * GROUP, (s + 1) * GROUP
        g = acc[s]
        for part in range(2):
            even = g[2 * part * GROUP : (2 * part + 1) * GROUP]
            odd = g[(2 * part + 1) * GROUP : (2 * part + 2) * GROUP]
            for b in range(n_half):
                lanes = slice(b * lat, (b + 1) * lat)
                where = slice(part * k_half + lo, part * k_half + hi)
                north_b[b, where, :] = even[:, lanes] + odd[:, lanes]
                south_b[b, where, :] = even[:, lanes] - odd[:, lanes]
    is_north = r < n_half
    mine = jnp.where(is_north, r, n_gy - 1 - r)
    own = jnp.where(is_north, north_b[mine], south_b[mine])
    out[:, :lat] = dot(own, flip_matrix(lat, jnp.logical_not(is_north)))
    up_n = jnp.minimum(r + 1, n_half - 1)
    up_s = jnp.clip(n_gy - 2 - r, 0, n_half - 1)
    up = jnp.where(r + 1 < n_half, north_b[up_n][:, :1], south_b[up_s][:, lat - 1 :])
    down_n = jnp.clip(r - 1, 0, n_half - 1)
    down_s = jnp.clip(n_gy - r, 0, n_half - 1)
    down = jnp.where(r - 1 < n_half, north_b[down_n][:, lat - 1 :], south_b[down_s][:, :1])
    lane_o = iota((plan.k_dev, lat), 1)
    out[:, lat:] = jnp.where(lane_o == 0, up, jnp.where(lane_o == 1, down, 0.0))


def finish_kernel(
    plan, idx, fold, terms, a_own, a_fold, b_table, north_tile, south_tile, edges,
    surface_ref, depth_ref, mask, east_ref, north_ref,
    sal_out, east_out, north_out, height_out,
):
    lon, lat = plan.tile_lon, plan.tile_lat
    r = idx[1]
    split = lon + EDGE
    own_trig = a_own[0, 0:1, :] * b_table[0, :split, :] + a_own[0, 1:2, :] * b_table[1, :split, :]
    fold_trig = a_fold[0, 0:1, :] * b_table[0, split:, :] + a_fold[0, 1:2, :] * b_table[1, split:, :]
    trig = jnp.concatenate([own_trig, fold_trig], axis=0)
    sal_all = dot(trig, terms[...])
    sal = sal_all[:lon, :lat]
    sal_out[...] = sal
    is_top = r == plan.n_gy - 1
    sal_n = jnp.where(is_top, sal_all[split:, lat - 1 : lat], sal_all[:lon, lat : lat + 1])
    sal_s = sal_all[:lon, lat + 1 : lat + 2]
    surface, depth = surface_ref[...], depth_ref[...]
    wet = mask[...].astype(F32)
    east, north = east_ref[...], north_ref[...]
    across = edges[EDGE:, :]
    surf_n = jnp.where(is_top, across[:, 2:3], north_tile[:, 4:5])
    depth_n = jnp.where(is_top, across[:, 0:1], north_tile[:, 5:6])
    wet_n = jnp.where(is_top, across[:, 1:2], north_tile[:, 6:7])
    pressure = surface - sal
    row = iota((lon, lat), 0)
    lane = iota((lon, lat), 1)

    def east_of(field, edge):
        return jnp.where(row == lon - 1, edge, pltpu.roll(field, lon - 1, 0))

    def north_of(field, edge):
        return jnp.where(lane == lat - 1, edge, pltpu.roll(field, lat - 1, 1))

    p_e = edges[0:1, :] - sal_all[lon : lon + 1, :lat]
    p_w = edges[3:4, :] - sal_all[lon + 1 : lon + 2, :lat]
    east_next = wet * east_of(wet, edges[2:3, :]) * (
        east - COURANT * (east_of(pressure, p_e) - pressure)
    )
    north_next = wet * north_of(wet, wet_n) * (
        north - COURANT * (north_of(pressure, surf_n - sal_n) - pressure)
    )
    east_out[...] = east_next
    north_out[...] = north_next
    east_flux = 0.5 * (depth + east_of(depth, edges[1:2, :])) * east_next
    north_flux = 0.5 * (depth + north_of(depth, depth_n)) * north_next
    west_face = edges[5:6, :] * wet[:1] * (edges[6:7, :] - COURANT * (pressure[:1] - p_w))
    west_edge = 0.5 * (edges[4:5, :] + depth[:1]) * west_face
    south_face = south_tile[:, 2:3] * wet[:, :1] * (
        south_tile[:, 3:4] - COURANT * (pressure[:, :1] - (south_tile[:, 0:1] - sal_s))
    )
    south_edge = 0.5 * (south_tile[:, 1:2] + depth[:, :1]) * south_face
    south_edge = jnp.where(r > 0, south_edge, 0.0)
    west_flux = jnp.where(row == 0, west_edge, pltpu.roll(east_flux, 1, 0))
    south_flux = jnp.where(lane == 0, south_edge, pltpu.roll(north_flux, 1, 1))
    height_out[...] = wet * (
        surface - COURANT * (east_flux - west_flux + north_flux - south_flux)
    )


def full(shape):
    return pl.BlockSpec(shape, lambda i, *_: (0,) * len(shape))


def on_device(height, east_speed, north_speed, water_depth, ocean_mask, fold_partner, love_factor):
    lon, lat = height.shape
    n_gx, n_gy = lax.axis_size("gx"), lax.axis_size("gy")
    plan = Plan(lon, lat, n_gx, n_gy, love_factor.shape[0])
    idx = jnp.stack([lax.axis_index("gx"), lax.axis_index("gy")]).astype(jnp.int32)
    tile = jax.ShapeDtypeStruct((lon, lat), F32)
    sent = 2 * lon + EDGE
    packed, surface = pl.pallas_call(
        pack_kernel, out_shape=(jax.ShapeDtypeStruct((sent, lat), F32), tile), name="pack"
    )(height, ocean_mask, water_depth, east_speed)
    gathered = lax.all_gather(packed, "gx", axis=0, tiled=False)
    rows = lon + plan.k_dev
    tile_spec = full((lon, lat))
    mine, edges = pl.pallas_call(
        lambda *refs: fourier_kernel(plan, *refs),
        grid_spec=pltpu.PrefetchScalarGridSpec(
            num_scalar_prefetch=2,
            grid=(1,),
            in_specs=[
                full((n_gx, sent, lat)),
                pl.BlockSpec((1, plan.u_rows, plan.nlon), lambda i, idx, fold: (idx[0], 0, 0)),
                full((2 * GROUP, plan.nlon)),
                pl.BlockSpec((1, 8, lat), lambda i, idx, fold: (idx[1], 0, 0)),
                tile_spec, tile_spec, tile_spec, tile_spec,
            ],
            out_specs=[full((rows, lat)), full((lon + EDGE, lat))],
        ),
        out_shape=(
            jax.ShapeDtypeStruct((rows, lat), F32),
            jax.ShapeDtypeStruct((lon + EDGE, lat), F32),
        ),
        name="fourier",
    )(
        idx, fold_partner, gathered, plan.u_table, plan.v_table, plan.quad,
        surface, water_depth, ocean_mask, north_speed,
    )
    blocks = [mine]
    for k in range(1, n_gy):
        ring = [(i, (i + k) % n_gy) for i in range(n_gy)]
        blocks.append(lax.ppermute(mine, "gy", ring))
    padded = jnp.zeros((plan.love_rows * GROUP,), F32).at[: plan.degrees].set(love_factor)
    love = padded.reshape(plan.love_rows, GROUP)
    slots, half = plan.n_slots, plan.half
    p_shape = pltpu.VMEM((CHAINS, ROWS, half), BF16)
    split_shape = pltpu.VMEM((n_gy // 2, plan.k_dev, lat), F32)
    terms = pl.pallas_call(
        lambda *refs: legendre_kernel(plan, *refs),
        grid_spec=pltpu.PrefetchScalarGridSpec(
            num_scalar_prefetch=2,
            grid=(1,),
            in_specs=[full((rows, lat))] * n_gy
            + [
                full((8, half)),
                pl.BlockSpec((1, slots * GROUP, 128), lambda i, idx, sched: (idx[0], 0, 0)),
                full((plan.love_rows, GROUP)),
            ],
            out_specs=full((plan.k_dev, 2 * lat)),
            scratch_shapes=[
                pltpu.VMEM((n_gy, plan.k_dev, lat), F32),
                pltpu.VMEM((slots, 8 * GROUP, half), BF16),
                pltpu.VMEM((slots, GROUP, half), F32),
                pltpu.VMEM((slots, GROUP, half), F32),
                pltpu.VMEM((plan.n_windows, 1, ROWS), F32),
                pltpu.VMEM((slots, 4 * GROUP, half), F32),
                pltpu.VMEM((CHAINS, 2, GROUP, half), F32),
                p_shape, p_shape, p_shape, p_shape,
                split_shape, split_shape,
            ],
        ),
        out_shape=jax.ShapeDtypeStruct((plan.k_dev, 2 * lat), F32),
        name="legendre",
    )(idx, jnp.asarray(plan.sched), *blocks, plan.geo, plan.seed_logs, love)
    everything = lax.all_gather(terms, "gx", axis=0, tiled=True)
    halo_spec = full((lon, lat))
    a_spec = (1, 8, plan.k_all)
    return pl.pallas_call(
        lambda *refs: finish_kernel(plan, *refs),
        grid_spec=pltpu.PrefetchScalarGridSpec(
            num_scalar_prefetch=2,
            grid=(1,),
            in_specs=[
                full((plan.k_all, 2 * lat)),
                pl.BlockSpec(a_spec, lambda i, idx, fold: (idx[0], 0, 0)),
                pl.BlockSpec(a_spec, lambda i, idx, fold: (fold[idx[0]], 0, 0)),
                full((2, plan.o_rows, plan.k_all)),
                halo_spec, halo_spec,
                full((lon + EDGE, lat)),
                tile_spec, tile_spec, tile_spec, tile_spec, tile_spec,
            ],
            out_specs=[tile_spec] * 4,
        ),
        out_shape=(tile,) * 4,
        name="finish",
    )(
        idx, fold_partner, everything, plan.a_table, plan.a_table, plan.b_table,
        blocks[n_gy - 1], blocks[1], edges,
        surface, water_depth, ocean_mask, east_speed, north_speed,
    )


def solution(mesh):
    spec = P("gx", "gy")
    return jax.shard_map(
        on_device,
        mesh=mesh,
        in_specs=(spec, spec, spec, spec, spec, P(), P()),
        out_specs=(spec,) * 4,
        check_vma=False,
    )
```

```python
import math

import numpy as np

import jax
import jax.numpy as jnp
from jax import lax
from jax.experimental import pallas as pl
from jax.experimental.pallas import tpu as pltpu
from jax.sharding import PartitionSpec as P

COURANT = 0.35
GROUP = 8
STEPS = 32
ROWS = GROUP * STEPS
CHAINS = 2
UNROLL = 2
EDGE = 8
F32 = jnp.float32
BF16 = jnp.bfloat16
HIGHEST = lax.Precision.HIGHEST
PARAMS = pltpu.CompilerParams(vmem_limit_bytes=16 * 1024 * 1024)


class Plan:
    def __init__(self, tile_lon, tile_lat, n_gx, n_gy, degrees):
        self.tile_lon, self.tile_lat = tile_lon, tile_lat
        self.n_gx, self.n_gy, self.degrees = n_gx, n_gy, degrees
        self.nlon, self.nlat = tile_lon * n_gx, tile_lat * n_gy
        self.half = self.nlat // 2
        self.n_groups = -(-degrees // GROUP)
        self.n_slots = -(-self.n_groups // n_gx)
        self.k_dev = 2 * self.n_slots * GROUP
        self.k_all = self.k_dev * n_gx
        self.group_of = np.array(
            [
                [s * n_gx + (c if s % 2 == 0 else n_gx - 1 - c) for s in range(self.n_slots)]
                for c in range(n_gx)
            ],
            np.int32,
        )
        self._schedule()
        self._tables()

    def _schedule(self):
        lists = []
        for c in range(self.n_gx):
            counts = []
            for s in range(self.n_slots):
                left = self.degrees - GROUP * int(self.group_of[c, s])
                counts.append(-(-max(left, 0) // STEPS))
            lists.append(counts)
        longest = max(-(-sum(counts) // CHAINS) for counts in lists)
        longest = max(longest, max(max(counts) for counts in lists))
        self.n_iter = -(-longest // UNROLL) * UNROLL
        idle = -(-self.degrees // STEPS)
        per_row = self.n_iter * CHAINS * 2
        self.sched_width = -(-per_row // 128) * 128
        self.sched = np.zeros((self.n_gx, 1, self.sched_width), np.int32)
        for c, counts in enumerate(lists):
            first, second, room = [], [], self.n_iter
            for s, count in enumerate(counts):
                if room >= count:
                    first += [(s, k) for k in range(count)]
                    room -= count
                else:
                    head = count - room
                    second += [(s, k) for k in range(head)]
                    first += [(s, k) for k in range(head, count)]
                    room = 0
            last = max(range(self.n_slots), key=lambda s: counts[s])
            for chain in (first, second):
                while len(chain) < self.n_iter:
                    chain.append((self.n_slots, idle))
            for i in range(self.n_iter):
                for h, chain in enumerate((first, second)):
                    at = (i * CHAINS + h) * 2
                    self.sched[c, 0, at : at + 2] = chain[i]
        self.love_width = -(-(self.degrees + GROUP * self.n_gx * (self.n_slots + 1) + STEPS * (idle + 1)) // 128) * 128

    def _tables(self):
        rows = np.arange(self.half)
        theta = np.pi * (rows + 0.5) / self.nlat
        self.geo = np.zeros((8, self.half), np.float32)
        self.geo[0] = np.cos(theta)
        self.geo[1] = np.log(np.sin(theta))
        all_theta = np.pi * (np.arange(self.nlat) + 0.5) / self.nlat
        quad = np.pi / self.nlat * (2.0 * np.pi / self.nlon) * np.sin(all_theta)
        self.quad = np.repeat(
            quad.reshape(self.n_gy, 1, self.tile_lat), 8, axis=1
        ).astype(np.float32)
        top = GROUP * (int(self.group_of.max()) + 1)
        factors = np.arange(1, top, dtype=np.float64)
        logs = np.concatenate([[0.0], np.cumsum(0.5 * np.log((2 * factors + 1) / (2 * factors)))])
        orders = self.group_of[:, :, None] * GROUP + np.arange(GROUP)[None, None, :]
        lanes = -(-self.n_gx // 128) * 128
        self.seed_logs = np.zeros((self.n_slots * GROUP, lanes), np.float32)
        self.seed_logs[:, : self.n_gx] = logs[orders].reshape(self.n_gx, -1).T
        lam = 2.0 * np.pi / self.nlon
        cols = np.arange(self.nlon)
        base = (self.group_of[:, :, None] * GROUP * cols[None, None, :]) % self.nlon
        u = np.stack([np.cos(lam * base), np.sin(lam * base)], axis=2)
        pad = -(-2 * self.n_slots // 8) * 8
        self.u_rows = pad
        self.u_table = np.zeros((self.n_gx, pad, self.nlon), np.float32)
        self.u_table[:, : 2 * self.n_slots] = u.reshape(self.n_gx, 2 * self.n_slots, self.nlon)
        small = (np.arange(GROUP)[:, None] * cols[None, :]) % self.nlon
        self.v_table = np.concatenate([np.cos(lam * small), np.sin(lam * small)]).astype(np.float32)
        m = np.concatenate(
            [np.tile(orders[c].reshape(-1), 2) for c in range(self.n_gx)]
        )
        sine = np.tile(np.repeat([0, 1], self.k_dev // 2), self.n_gx)
        nu = np.where(m == 0, 1.0, 2.0) * (m < self.degrees)
        starts = np.arange(self.n_gx) * self.tile_lon
        phase = lam * ((starts[:, None] * m[None, :]) % self.nlon)
        a1 = nu * np.where(sine == 0, np.cos(phase), np.sin(phase))
        a2 = nu * np.where(sine == 0, -np.sin(phase), np.cos(phase))
        self.a_table = np.zeros((self.n_gx, 8, self.k_all), np.float32)
        self.a_table[:, 0] = a1
        self.a_table[:, 1] = a2
        offsets = np.concatenate(
            [
                np.arange(self.tile_lon),
                [self.tile_lon, -1],
                np.zeros(EDGE - 2),
                np.arange(self.tile_lon)[::-1],
            ]
        ).astype(np.int64)
        phase = lam * ((offsets[:, None] * m[None, :]) % self.nlon)
        self.b_table = np.stack([np.cos(phase), np.sin(phase)]).astype(np.float32)
        self.o_rows = offsets.shape[0]


def iota(shape, axis):
    return lax.broadcasted_iota(jnp.int32, shape, axis)


def dot(a, b):
    return lax.dot_general(
        a, b, (((1,), (0,)), ((), ())), precision=HIGHEST, preferred_element_type=F32
    )


def flip_matrix(size, flipped):
    row = iota((size, size), 0)
    col = iota((size, size), 1)
    target = jnp.where(flipped, size - 1 - col, col)
    return jnp.where(row == target, 1.0, 0.0).astype(F32)


def here():
    return lax.axis_index("gx"), lax.axis_index("gy")


def pack_kernel(plan, *refs):
    count = len(refs) // 2 - 1
    height, mask, depth, east = refs[:4]
    sources = refs[:count]
    out, surface_out = refs[count : count + 2]
    kept = refs[count + 2 : 2 * count + 1]
    height_v, sem = refs[2 * count + 1 :]
    c, r = here()
    targets = (height_v,) + tuple(kept)
    copies = []
    for k, (source, target) in enumerate(zip(sources, targets)):
        if k in SLICED_GX:
            source = source.at[c]
        elif k in SLICED_GY:
            source = source.at[r]
        copies.append(pltpu.make_async_copy(source, target, sem.at[k]))
    for copy in copies:
        copy.start()
    for copy in copies[:4]:
        copy.wait()
    _, mask_v, depth_v, east_v = targets[:4]
    lon, lat = height_v.shape
    wet = mask_v[...].astype(F32)
    surface = wet * height_v[...]
    surface_out[...] = surface
    out[:lon, :] = surface
    out[lon : lon + 1, :] = depth_v[:1, :]
    out[lon + 1 : lon + 2, :] = wet[:1, :]
    out[lon + 2 : lon + 3, :] = depth_v[lon - 1 :, :]
    out[lon + 3 : lon + 4, :] = wet[lon - 1 :, :]
    out[lon + 4 : lon + 5, :] = east_v[lon - 1 :, :]
    out[lon + 5 : lon + EDGE, :] = jnp.zeros((EDGE - 5, lat), F32)
    lane = iota((lon, lat), 1)
    out[lon + EDGE :, :] = jnp.where(
        lane == 0, depth_v[:, lat - 1 :], jnp.where(lane == 1, wet[:, lat - 1 :], 0.0)
    )
    for copy in copies[4:]:
        copy.wait()


def fourier_kernel(
    plan, gathered, u, v, quad, surface, depth, mask, north, fold_v, out, edges, fold, sem
):
    lon, lat = plan.tile_lon, plan.tile_lat
    n_gx, slots = plan.n_gx, plan.n_slots
    c, r = here()
    fetch = pltpu.make_async_copy(fold_v, fold, sem)
    fetch.start()
    field = jnp.concatenate([gathered[d, :lon, :] for d in range(n_gx)], axis=0)
    vc, vs = v[:GROUP, :], v[GROUP:, :]
    cos_rows, sin_rows = [], []
    for s in range(slots):
        uc = u[2 * s : 2 * s + 1, :]
        us = u[2 * s + 1 : 2 * s + 2, :]
        cos_rows.append(uc * vc - us * vs)
        sin_rows.append(us * vc + uc * vs)
    trig = jnp.concatenate(cos_rows + sin_rows, axis=0)
    sums = dot(trig, field) * quad[:1, :]
    out[lon:, :] = dot(sums, flip_matrix(lat, r >= plan.n_gy // 2))
    wet = mask[...].astype(F32)
    lane = iota((lon, lat), 1)
    tile = jnp.zeros((lon, lat), F32)
    last = [surface, depth, wet, north]
    for k, array in enumerate(last):
        tile = jnp.where(lane == k, array[:, lat - 1 :], tile)
    for k, array in enumerate([surface, depth, wet]):
        tile = jnp.where(lane == 4 + k, array[:, :1], tile)
    out[:lon, :] = tile
    after = lax.rem(c + 1, n_gx)
    before = lax.rem(c + n_gx - 1, n_gx)
    fetch.wait()
    partner = fold[c]
    edges[0:1, :] = gathered[after, 0:1, :]
    edges[1:3, :] = gathered[after, lon : lon + 2, :]
    edges[3:4, :] = gathered[before, lon - 1 : lon, :]
    edges[4:7, :] = gathered[before, lon + 2 : lon + 5, :]
    edges[7:8, :] = jnp.zeros((1, lat), F32)
    across = jnp.where(
        lane == 2, gathered[partner, :lon, lat - 1 :], gathered[partner, lon + EDGE :, :]
    )
    edges[EDGE:, :] = dot(flip_matrix(lon, True), across)


def scheduled(plan, c, sched, i, h):
    at = (i * CHAINS + h) * 2
    slot, chunk = sched[0, at], sched[0, at + 1]
    even = lax.rem(slot, 2) == 0
    group = slot * plan.n_gx + jnp.where(even, c, plan.n_gx - 1 - c)
    return slot, chunk, group


def basis_kernel(plan, sched_v, geo, seed_logs, p_out, seeds, unscale, state, sched, sem):
    slots, half = plan.n_slots, plan.half
    c, _ = here()
    fetch = pltpu.make_async_copy(sched_v, sched, sem)
    fetch.start()
    log_sin = geo[1:2, :]
    sub = iota((GROUP, half), 0)
    pick = iota(seed_logs.shape, 1) == c
    logs = jnp.sum(jnp.where(pick, seed_logs[...], 0.0), axis=1, keepdims=True)
    for s in range(slots):
        group = s * plan.n_gx + (c if s % 2 == 0 else plan.n_gx - 1 - c)
        order = (sub + group * GROUP).astype(F32)
        exponent = order * log_sin + logs[s * GROUP : (s + 1) * GROUP]
        shift = jnp.clip(-exponent - 80.0, 0.0, 80.0)
        seeds[s] = jnp.exp(exponent + shift) * (1.0 / math.sqrt(4.0 * math.pi))
        unscale[s] = jnp.exp(-shift)
    state[...] = jnp.zeros(state.shape, F32)
    seeds[slots] = jnp.zeros((GROUP, half), F32)
    unscale[slots] = jnp.zeros((GROUP, half), F32)
    x = jnp.broadcast_to(geo[0:1, :], (GROUP, half))
    sub_c = iota((GROUP, 128), 0)
    lane_c = iota((GROUP, 128), 1)
    fetch.wait()

    def begin(i, h):
        slot, chunk, group = scheduled(plan, c, sched, i, h)
        m0 = group * GROUP
        degree = (m0 + chunk * STEPS + lane_c).astype(F32)
        order = (m0 + sub_c).astype(F32)
        below = degree - 1.0
        growth = jnp.sqrt(
            jnp.maximum(4.0 * degree * degree - 1.0, 1.0)
            / jnp.maximum(degree * degree - order * order, 1.0)
        )
        damping = jnp.sqrt(
            jnp.maximum(below * below - order * order, 0.0)
            / jnp.maximum(4.0 * below * below - 1.0, 1.0)
        )
        started = jnp.where(chunk == 0, 0.0, 1.0).astype(F32)
        seed = seeds[slot] * (1.0 - started)
        return slot, growth, growth * damping, seed, unscale[slot], state[slot, 0], state[slot, 1]

    def body(i, carry):
        lanes = [begin(i, h) for h in range(CHAINS)]
        previous = [lane[5] for lane in lanes]
        before = [lane[6] for lane in lanes]
        pairs = [[] for _ in range(CHAINS)]
        for t in range(STEPS):
            for h, (_, growth, fall, seed, scale, _, _) in enumerate(lanes):
                a = jnp.broadcast_to(growth[:, t : t + 1], (GROUP, half))
                b = jnp.broadcast_to(fall[:, t : t + 1], (GROUP, half))
                value = (a * x) * previous[h] - b * before[h]
                if t < GROUP:
                    value = value + jnp.where(sub == t, seed, 0.0)
                previous[h], before[h] = value, previous[h]
                pairs[h].append(value * scale)
                if t % 2 == 1:
                    both = jnp.concatenate(pairs[h], axis=0)
                    both_hi = both.astype(BF16)
                    at = (t - 1) * GROUP
                    p_out[i, h, 0, at : at + 2 * GROUP, :] = both_hi
                    p_out[i, h, 1, at : at + 2 * GROUP, :] = (
                        both - both_hi.astype(F32)
                    ).astype(BF16)
                    pairs[h] = []
        for h, lane in enumerate(lanes):
            state[lane[0], 0] = previous[h]
            state[lane[0], 1] = before[h]
        return carry

    lax.fori_loop(0, plan.n_iter, body, 0)


def legendre_kernel(plan, *refs):
    n_gy, slots, half = plan.n_gy, plan.n_slots, plan.half
    lon, lat, k_half = plan.tile_lon, plan.tile_lat, plan.k_dev // 2
    blocks = refs[:n_gy]
    basis, love, sched_v, out = refs[n_gy : n_gy + 4]
    (fabs, lhs, weights, shifted, acc, coeffs, north_b, south_b, sched, sem) = refs[n_gy + 4 :]
    c, r = here()
    fetch = pltpu.make_async_copy(sched_v, sched, sem)
    fetch.start()
    n_half = n_gy // 2
    for k in range(n_gy):
        fabs[lax.rem(r - k + n_gy, n_gy)] = blocks[k][lon:, :]
    sym, anti = [], []
    for b in range(n_half):
        north, south = fabs[b], fabs[n_gy - 1 - b]
        sym.append(north + south)
        anti.append(north - south)
    sym = jnp.concatenate(sym, axis=1)
    anti = jnp.concatenate(anti, axis=1)
    for s in range(slots):
        lo, hi = s * GROUP, (s + 1) * GROUP
        rows = jnp.concatenate(
            [sym[lo:hi], anti[lo:hi], sym[k_half + lo : k_half + hi], anti[k_half + lo : k_half + hi]],
            axis=0,
        )
        rows_hi = rows.astype(BF16)
        lhs[s, : 4 * GROUP, :] = rows_hi
        lhs[s, 4 * GROUP :, :] = (rows - rows_hi.astype(F32)).astype(BF16)
    acc[...] = jnp.zeros(acc.shape, F32)
    lhs[slots] = jnp.zeros((8 * GROUP, half), BF16)
    padded = jnp.concatenate(
        [love[...].reshape(1, -1), jnp.zeros((1, plan.love_width - plan.degrees), F32)], axis=1
    )
    padded = jnp.broadcast_to(padded, (8, plan.love_width))
    fetch.wait()
    items = plan.n_iter * CHAINS
    for item in range(items):
        _, chunk, group = scheduled(plan, c, sched, item // CHAINS, item % CHAINS)
        start = group * GROUP + chunk * STEPS
        rolled = pltpu.roll(padded, plan.love_width - start, 1)
        shifted[item : item + 1, :] = rolled[:1, :128]
    spread = iota((128, ROWS), 1) // GROUP == iota((128, ROWS), 0)
    weights[...] = dot(shifted[...], jnp.where(spread, 1.0, 0.0).astype(F32)).reshape(
        items, 1, ROWS
    )
    row = iota((4 * GROUP, ROWS), 0)
    lane = iota((4 * GROUP, ROWS), 1)
    i_row, i_lane, t_lane = row % GROUP, lane % GROUP, lane // GROUP
    keep = jnp.where(
        (i_row == i_lane) & ((t_lane + i_row) % 2 == (row // GROUP) % 2), 1.0, 0.0
    ).astype(F32)
    nt = (((1,), (1,)), ((), ()))
    nn = (((1,), (0,)), ((), ()))
    n = 4 * GROUP

    def analyse(i, h):
        slot, _, _ = scheduled(plan, c, sched, i, h)
        left = lhs[slot]
        one = lax.dot_general(left, basis[i, h, 0], nt, preferred_element_type=F32)
        two = lax.dot_general(left[:n], basis[i, h, 1], nt, preferred_element_type=F32)
        coeff = (one[:n] + one[n:] + two) * keep * weights[i * CHAINS + h]
        coeff_hi = coeff.astype(BF16)
        coeff_lo = (coeff - coeff_hi.astype(F32)).astype(BF16)
        return jnp.concatenate([coeff_hi, coeff_lo], axis=0)

    def synthesise(i, h):
        right = coeffs[i, h]
        three = lax.dot_general(right, basis[i, h, 0], nn, preferred_element_type=F32)
        four = lax.dot_general(right[:n], basis[i, h, 1], nn, preferred_element_type=F32)
        return three[:n] + three[n:] + four

    def analyse_all(k):
        for j in range(UNROLL):
            for h in range(CHAINS):
                i = k * UNROLL + j
                coeffs[i, h] = analyse(i, h)

    def synthesise_all(k):
        found = [
            (scheduled(plan, c, sched, k * UNROLL + j, h)[0], synthesise(k * UNROLL + j, h))
            for j in range(UNROLL)
            for h in range(CHAINS)
        ]
        return found

    def accumulate(found):
        for slot, part in found:
            acc[slot] += part

    trips = plan.n_iter // UNROLL
    analyse_all(0)

    def body(k, carry):
        found = synthesise_all(k - 1)
        analyse_all(k)
        accumulate(found)
        return carry

    lax.fori_loop(1, trips, body, 0)
    accumulate(synthesise_all(trips - 1))

    for s in range(slots):
        lo, hi = s * GROUP, (s + 1) * GROUP
        g = acc[s]
        for part in range(2):
            even = g[2 * part * GROUP : (2 * part + 1) * GROUP]
            odd = g[(2 * part + 1) * GROUP : (2 * part + 2) * GROUP]
            for b in range(n_half):
                lanes = slice(b * lat, (b + 1) * lat)
                where = slice(part * k_half + lo, part * k_half + hi)
                north_b[b, where, :] = even[:, lanes] + odd[:, lanes]
                south_b[b, where, :] = even[:, lanes] - odd[:, lanes]
    is_north = r < n_half
    mine = jnp.where(is_north, r, n_gy - 1 - r)
    own = jnp.where(is_north, north_b[mine], south_b[mine])
    out[:, :lat] = dot(own, flip_matrix(lat, jnp.logical_not(is_north)))
    up_n = jnp.minimum(r + 1, n_half - 1)
    up_s = jnp.clip(n_gy - 2 - r, 0, n_half - 1)
    up = jnp.where(r + 1 < n_half, north_b[up_n][:, :1], south_b[up_s][:, lat - 1 :])
    down_n = jnp.clip(r - 1, 0, n_half - 1)
    down_s = jnp.clip(n_gy - r, 0, n_half - 1)
    down = jnp.where(r - 1 < n_half, north_b[down_n][:, lat - 1 :], south_b[down_s][:, :1])
    lane_o = iota((plan.k_dev, lat), 1)
    out[:, lat:] = jnp.where(lane_o == 0, up, jnp.where(lane_o == 1, down, 0.0))


def finish_kernel(
    plan, terms, a_table, b_table, fold_v, north_tile, south_tile, edges,
    surface_ref, depth_ref, mask, east_ref, north_ref,
    sal_out, east_out, north_out, height_out, fold, sem,
):
    lon, lat = plan.tile_lon, plan.tile_lat
    c, r = here()
    fetch = pltpu.make_async_copy(fold_v, fold, sem)
    fetch.start()
    split = lon + EDGE
    a_own = a_table[c]
    own_trig = a_own[0:1, :] * b_table[0, :split, :] + a_own[1:2, :] * b_table[1, :split, :]
    fetch.wait()
    a_fold = a_table[fold[c]]
    fold_trig = a_fold[0:1, :] * b_table[0, split:, :] + a_fold[1:2, :] * b_table[1, split:, :]
    trig = jnp.concatenate([own_trig, fold_trig], axis=0)
    sal_all = dot(trig, terms[...])
    sal = sal_all[:lon, :lat]
    sal_out[...] = sal
    is_top = r == plan.n_gy - 1
    sal_n = jnp.where(is_top, sal_all[split:, lat - 1 : lat], sal_all[:lon, lat : lat + 1])
    sal_s = sal_all[:lon, lat + 1 : lat + 2]
    surface, depth = surface_ref[...], depth_ref[...]
    wet = mask[...].astype(F32)
    east, north = east_ref[...], north_ref[...]
    across = edges[EDGE:, :]
    surf_n = jnp.where(is_top, across[:, 2:3], north_tile[:lon, 4:5])
    depth_n = jnp.where(is_top, across[:, 0:1], north_tile[:lon, 5:6])
    wet_n = jnp.where(is_top, across[:, 1:2], north_tile[:lon, 6:7])
    pressure = surface - sal
    row = iota((lon, lat), 0)
    lane = iota((lon, lat), 1)

    def east_of(field, edge):
        return jnp.where(row == lon - 1, edge, pltpu.roll(field, lon - 1, 0))

    def north_of(field, edge):
        return jnp.where(lane == lat - 1, edge, pltpu.roll(field, lat - 1, 1))

    p_e = edges[0:1, :] - sal_all[lon : lon + 1, :lat]
    p_w = edges[3:4, :] - sal_all[lon + 1 : lon + 2, :lat]
    east_next = wet * east_of(wet, edges[2:3, :]) * (
        east - COURANT * (east_of(pressure, p_e) - pressure)
    )
    north_next = wet * north_of(wet, wet_n) * (
        north - COURANT * (north_of(pressure, surf_n - sal_n) - pressure)
    )
    east_out[...] = east_next
    north_out[...] = north_next
    east_flux = 0.5 * (depth + east_of(depth, edges[1:2, :])) * east_next
    north_flux = 0.5 * (depth + north_of(depth, depth_n)) * north_next
    west_face = edges[5:6, :] * wet[:1] * (edges[6:7, :] - COURANT * (pressure[:1] - p_w))
    west_edge = 0.5 * (edges[4:5, :] + depth[:1]) * west_face
    south_face = south_tile[:lon, 2:3] * wet[:, :1] * (
        south_tile[:lon, 3:4] - COURANT * (pressure[:, :1] - (south_tile[:lon, 0:1] - sal_s))
    )
    south_edge = 0.5 * (south_tile[:lon, 1:2] + depth[:, :1]) * south_face
    south_edge = jnp.where(r > 0, south_edge, 0.0)
    west_flux = jnp.where(row == 0, west_edge, pltpu.roll(east_flux, 1, 0))
    south_flux = jnp.where(lane == 0, south_edge, pltpu.roll(north_flux, 1, 1))
    height_out[...] = wet * (
        surface - COURANT * (east_flux - west_flux + north_flux - south_flux)
    )


VMEM = pl.BlockSpec(memory_space=pltpu.VMEM)
HBM = pl.BlockSpec(memory_space=pltpu.HBM)
SLICED_GX = (5, 10)
SLICED_GY = (7,)


def on_device(height, east_speed, north_speed, water_depth, ocean_mask, fold_partner, love_factor):
    lon, lat = height.shape
    n_gx, n_gy = lax.axis_size("gx"), lax.axis_size("gy")
    plan = Plan(lon, lat, n_gx, n_gy, love_factor.shape[0])
    slots, half = plan.n_slots, plan.half
    sent = 2 * lon + EDGE
    sources = (
        height, ocean_mask, water_depth, east_speed, north_speed, plan.u_table, plan.v_table,
        plan.quad, plan.geo, plan.seed_logs, plan.sched, love_factor, fold_partner,
    )
    sources = tuple(
        pltpu.with_memory_space_constraint(jnp.asarray(source), pltpu.HBM) for source in sources
    )
    kept_shapes = [
        source.shape[1:] if k in SLICED_GX + SLICED_GY else source.shape
        for k, source in enumerate(sources)
    ]
    kept = [
        pltpu.VMEM(shape, source.dtype) for shape, source in zip(kept_shapes[1:], sources[1:])
    ]
    packed, surface, *kept = pl.pallas_call(
        lambda *refs: pack_kernel(plan, *refs),
        in_specs=[HBM] * len(sources),
        out_specs=[VMEM] * (len(sources) + 1),
        out_shape=(pltpu.VMEM((sent, lat), F32), pltpu.VMEM((lon, lat), F32), *kept),
        scratch_shapes=[pltpu.VMEM((lon, lat), F32), pltpu.SemaphoreType.DMA((len(sources),))],
        compiler_params=PARAMS,
        name="pack",
    )(*sources)
    mask, depth, east, north, u, v, quad, geo, seed_logs, sched, love, fold = kept
    gathered = lax.all_gather(packed, "gx", axis=0, tiled=False)
    rows = lon + plan.k_dev
    fold_scratch = [pltpu.SMEM((n_gx,), jnp.int32), pltpu.SemaphoreType.DMA]
    mine, edges = pl.pallas_call(
        lambda *refs: fourier_kernel(plan, *refs),
        in_specs=[VMEM] * 9,
        out_specs=[VMEM] * 2,
        out_shape=(pltpu.VMEM((rows, lat), F32), pltpu.VMEM((lon + EDGE, lat), F32)),
        scratch_shapes=fold_scratch,
        compiler_params=PARAMS,
        name="fourier",
    )(gathered, u, v, quad, surface, depth, mask, north, fold)
    blocks = [mine]
    for k in range(1, n_gy):
        ring = [(i, (i + k) % n_gy) for i in range(n_gy)]
        blocks.append(lax.ppermute(mine, "gy", ring))
    sched_scratch = [pltpu.SMEM((1, plan.sched_width), jnp.int32), pltpu.SemaphoreType.DMA]
    basis = pl.pallas_call(
        lambda *refs: basis_kernel(plan, *refs),
        in_specs=[VMEM] * 3,
        out_specs=VMEM,
        out_shape=pltpu.VMEM((plan.n_iter, CHAINS, 2, ROWS, half), BF16),
        scratch_shapes=[
            pltpu.VMEM((slots + 1, GROUP, half), F32),
            pltpu.VMEM((slots + 1, GROUP, half), F32),
            pltpu.VMEM((slots + 1, 2, GROUP, half), F32),
        ]
        + sched_scratch,
        cost_estimate=pl.CostEstimate(flops=60_000_000, bytes_accessed=1_000_000, transcendentals=0),
        compiler_params=PARAMS,
        name="basis",
    )(sched, geo, seed_logs)
    items = plan.n_iter * CHAINS
    split_shape = pltpu.VMEM((n_gy // 2, plan.k_dev, lat), F32)
    terms = pl.pallas_call(
        lambda *refs: legendre_kernel(plan, *refs),
        in_specs=[VMEM] * (n_gy + 3),
        out_specs=VMEM,
        out_shape=pltpu.VMEM((plan.k_dev, 2 * lat), F32),
        scratch_shapes=[
            pltpu.VMEM((n_gy, plan.k_dev, lat), F32),
            pltpu.VMEM((slots + 1, 8 * GROUP, half), BF16),
            pltpu.VMEM((items, 1, ROWS), F32),
            pltpu.VMEM((items, 128), F32),
            pltpu.VMEM((slots + 1, 4 * GROUP, half), F32),
            pltpu.VMEM((plan.n_iter, CHAINS, 8 * GROUP, ROWS), BF16),
            split_shape, split_shape,
        ]
        + sched_scratch,
        compiler_params=PARAMS,
        name="legendre",
    )(*blocks, basis, love, sched)
    everything = lax.all_gather(terms, "gx", axis=0, tiled=True)
    tile = jax.ShapeDtypeStruct((lon, lat), F32)
    a_table, b_table = jnp.asarray(plan.a_table), jnp.asarray(plan.b_table)
    return pl.pallas_call(
        lambda *refs: finish_kernel(plan, *refs),
        in_specs=[VMEM] * 12,
        out_specs=[VMEM] * 4,
        out_shape=(tile,) * 4,
        scratch_shapes=fold_scratch,
        compiler_params=PARAMS,
        name="finish",
    )(
        everything, a_table, b_table, fold, blocks[n_gy - 1], blocks[1], edges,
        surface, depth, mask, east, north,
    )


def solution(mesh):
    spec = P("gx", "gy")
    return jax.shard_map(
        on_device,
        mesh=mesh,
        in_specs=(spec, spec, spec, spec, spec, P(), P()),
        out_specs=(spec,) * 4,
        check_vma=False,
    )
```

```python
import math

import numpy as np

import jax
import jax.numpy as jnp
from jax import lax
from jax.experimental import pallas as pl
from jax.experimental.pallas import tpu as pltpu
from jax.sharding import PartitionSpec as P

COURANT = 0.35
GROUP = 8
STEPS = 32
ROWS = GROUP * STEPS
CHAINS = 2
UNROLL = 3
EDGE = 8
F32 = jnp.float32
BF16 = jnp.bfloat16
HIGHEST = lax.Precision.HIGHEST
PARAMS = pltpu.CompilerParams(vmem_limit_bytes=16 * 1024 * 1024)


class Plan:
    def __init__(self, tile_lon, tile_lat, n_gx, n_gy, degrees):
        self.tile_lon, self.tile_lat = tile_lon, tile_lat
        self.n_gx, self.n_gy, self.degrees = n_gx, n_gy, degrees
        self.nlon, self.nlat = tile_lon * n_gx, tile_lat * n_gy
        self.half = self.nlat // 2
        self.n_groups = -(-degrees // GROUP)
        self.n_slots = -(-self.n_groups // n_gx)
        self.k_dev = 2 * self.n_slots * GROUP
        self.k_all = self.k_dev * n_gx
        self.group_of = np.array(
            [
                [s * n_gx + (c if s % 2 == 0 else n_gx - 1 - c) for s in range(self.n_slots)]
                for c in range(n_gx)
            ],
            np.int32,
        )
        self._schedule()
        self._tables()

    def _schedule(self):
        lists = []
        for c in range(self.n_gx):
            counts = []
            for s in range(self.n_slots):
                left = self.degrees - GROUP * int(self.group_of[c, s])
                counts.append(-(-max(left, 0) // STEPS))
            lists.append(counts)
        longest = max(-(-sum(counts) // CHAINS) for counts in lists)
        longest = max(longest, max(max(counts) for counts in lists))
        self.n_iter = -(-longest // UNROLL) * UNROLL
        per_row = self.n_iter * CHAINS * 2
        self.sched_width = -(-per_row // 128) * 128
        self.sched = np.zeros((self.n_gx, 1, self.sched_width), np.int32)
        for c, counts in enumerate(lists):
            first, second, room = [], [], self.n_iter
            for s, count in enumerate(counts):
                if room >= count:
                    first += [(s, k) for k in range(count)]
                    room -= count
                else:
                    head = count - room
                    second += [(s, k) for k in range(head)]
                    first += [(s, k) for k in range(head, count)]
                    room = 0
            for chain in (first, second):
                while len(chain) < self.n_iter:
                    chain.append((self.n_slots, 0))
            for i in range(self.n_iter):
                for h, chain in enumerate((first, second)):
                    at = (i * CHAINS + h) * 2
                    self.sched[c, 0, at : at + 2] = chain[i]
        top = self.n_gx * (self.n_slots + 1) * GROUP
        self.love_width = -(-(max(top, self.degrees) + 2 * STEPS) // 128) * 128

    def _tables(self):
        rows = np.arange(self.nlat).reshape(2, self.half)
        theta = np.pi * (rows + 0.5) / self.nlat
        self.geo = np.zeros((2, 8, self.half), np.float32)
        self.geo[:, 0] = np.cos(theta)
        self.geo[:, 1] = np.log(np.sin(theta))
        all_theta = np.pi * (np.arange(self.nlat) + 0.5) / self.nlat
        quad = np.pi / self.nlat * (2.0 * np.pi / self.nlon) * np.sin(all_theta)
        self.quad = np.repeat(
            quad.reshape(self.n_gy, 1, self.tile_lat), 8, axis=1
        ).astype(np.float32)
        top = GROUP * (int(self.group_of.max()) + 1)
        factors = np.arange(1, top, dtype=np.float64)
        logs = np.concatenate([[0.0], np.cumsum(0.5 * np.log((2 * factors + 1) / (2 * factors)))])
        orders = self.group_of[:, :, None] * GROUP + np.arange(GROUP)[None, None, :]
        lanes = -(-self.n_gx // 128) * 128
        self.seed_logs = np.zeros((self.n_slots * GROUP, lanes), np.float32)
        self.seed_logs[:, : self.n_gx] = logs[orders].reshape(self.n_gx, -1).T
        lam = 2.0 * np.pi / self.nlon
        cols = np.arange(self.nlon)
        base = (self.group_of[:, :, None] * GROUP * cols[None, None, :]) % self.nlon
        u = np.stack([np.cos(lam * base), np.sin(lam * base)], axis=2)
        pad = -(-2 * self.n_slots // 8) * 8
        self.u_rows = pad
        self.u_table = np.zeros((self.n_gx, pad, self.nlon), np.float32)
        self.u_table[:, : 2 * self.n_slots] = u.reshape(self.n_gx, 2 * self.n_slots, self.nlon)
        small = (np.arange(GROUP)[:, None] * cols[None, :]) % self.nlon
        self.v_table = np.concatenate([np.cos(lam * small), np.sin(lam * small)]).astype(np.float32)
        m = np.concatenate(
            [np.tile(orders[c].reshape(-1), 2) for c in range(self.n_gx)]
        )
        sine = np.tile(np.repeat([0, 1], self.k_dev // 2), self.n_gx)
        nu = np.where(m == 0, 1.0, 2.0) * (m < self.degrees)
        starts = np.arange(self.n_gx) * self.tile_lon
        phase = lam * ((starts[:, None] * m[None, :]) % self.nlon)
        a1 = nu * np.where(sine == 0, np.cos(phase), np.sin(phase))
        a2 = nu * np.where(sine == 0, -np.sin(phase), np.cos(phase))
        self.a_table = np.zeros((self.n_gx, 8, self.k_all), np.float32)
        self.a_table[:, 0] = a1
        self.a_table[:, 1] = a2
        offsets = np.concatenate(
            [
                np.arange(self.tile_lon),
                [self.tile_lon, -1],
                np.zeros(EDGE - 2),
                np.arange(self.tile_lon)[::-1],
            ]
        ).astype(np.int64)
        phase = lam * ((offsets[:, None] * m[None, :]) % self.nlon)
        self.b_table = np.stack([np.cos(phase), np.sin(phase)]).astype(np.float32)
        self.o_rows = offsets.shape[0]


def iota(shape, axis):
    return lax.broadcasted_iota(jnp.int32, shape, axis)


def dot(a, b):
    return lax.dot_general(
        a, b, (((1,), (0,)), ((), ())), precision=HIGHEST, preferred_element_type=F32
    )


def dot3(a, b):
    a_hi, b_hi = a.astype(BF16), b.astype(BF16)
    a_lo = (a - a_hi.astype(F32)).astype(BF16)
    b_lo = (b - b_hi.astype(F32)).astype(BF16)
    n = a.shape[0]
    dims = (((1,), (0,)), ((), ()))
    both = jnp.concatenate([a_hi, a_lo], axis=0)
    big = lax.dot_general(both, b_hi, dims, preferred_element_type=F32)
    small = lax.dot_general(a_hi, b_lo, dims, preferred_element_type=F32)
    return big[:n] + (big[n:] + small)


def rows_of(tile, size):
    height = tile.shape[0]
    tile = jnp.concatenate([tile, jnp.zeros((size - height, size), F32)], axis=0)
    return tile.T[:EDGE, :]


def flip_matrix(size, flipped):
    row = iota((size, size), 0)
    col = iota((size, size), 1)
    target = jnp.where(flipped, size - 1 - col, col)
    return jnp.where(row == target, 1.0, 0.0).astype(F32)


def here():
    return lax.axis_index("gx"), lax.axis_index("gy")


def pack_kernel(plan, *refs):
    count = len(refs) // 2 - 1
    height, mask, depth, east = refs[:4]
    sources = refs[:count]
    out, surface_out = refs[count : count + 2]
    kept = refs[count + 2 : 2 * count + 1]
    height_v, sem = refs[2 * count + 1 :]
    c, r = here()
    targets = (height_v,) + tuple(kept)
    copies = []
    for k, (source, target) in enumerate(zip(sources, targets)):
        if k in SLICED_GX:
            source = source.at[c]
        elif k in SLICED_GY:
            source = source.at[r]
        elif k in SLICED_HALF:
            source = source.at[jnp.where(r < plan.n_gy // 2, 0, 1)]
        copies.append(pltpu.make_async_copy(source, target, sem.at[k]))
    for copy in copies:
        copy.start()
    for copy in copies[:4]:
        copy.wait()
    _, mask_v, depth_v, east_v = targets[:4]
    lon, lat = height_v.shape
    wet = mask_v[...].astype(F32)
    surface = wet * height_v[...]
    surface_out[...] = surface
    out[:lon, :] = surface
    out[lon : lon + 1, :] = depth_v[:1, :]
    out[lon + 1 : lon + 2, :] = wet[:1, :]
    out[lon + 2 : lon + 3, :] = depth_v[lon - 1 :, :]
    out[lon + 3 : lon + 4, :] = wet[lon - 1 :, :]
    out[lon + 4 : lon + 5, :] = east_v[lon - 1 :, :]
    lane = iota((lon, lat), 1)
    tile = jnp.zeros((lon, lat), F32)
    for k, array in enumerate([depth_v, wet, surface]):
        tile = jnp.where(lane == k, array[:, lat - 1 :], tile)
    out[lon + 5 :, :] = rows_of(tile, lat)[: EDGE - 5]
    for copy in copies[4:]:
        copy.wait()


def fourier_kernel(plan, *refs):
    gathered, u, v, quad, surface, depth, mask, north, fold_v = refs[:9]
    n_gx, n_gy, slots = plan.n_gx, plan.n_gy, plan.n_slots
    outs, edges, fold, sem = refs[9 : 9 + n_gy], *refs[9 + n_gy :]
    lon, lat = plan.tile_lon, plan.tile_lat
    c, r = here()
    fetch = pltpu.make_async_copy(fold_v, fold, sem)
    fetch.start()
    field = jnp.concatenate([gathered[d, :lon, :] for d in range(n_gx)], axis=0)
    vc, vs = v[:GROUP, :], v[GROUP:, :]
    cos_rows, sin_rows = [], []
    for s in range(slots):
        uc = u[2 * s : 2 * s + 1, :]
        us = u[2 * s + 1 : 2 * s + 2, :]
        cos_rows.append(uc * vc - us * vs)
        sin_rows.append(us * vc + uc * vs)
    trig = jnp.concatenate(cos_rows + sin_rows, axis=0)
    sums = dot3(trig, field) * quad[:1, :]
    flipped = dot3(sums, flip_matrix(lat, True))
    wet = mask[...].astype(F32)
    lane = iota((lon, lat), 1)
    tile = jnp.zeros((lon, lat), F32)
    for k, array in enumerate([surface, depth, wet, north]):
        tile = jnp.where(lane == k, array[:, lat - 1 :], tile)
    for k, array in enumerate([surface, depth, wet]):
        tile = jnp.where(lane == 4 + k, array[:, :1], tile)
    halo = rows_of(tile, lat)
    for k in range(n_gy):
        target = lax.rem(r + k, n_gy)
        same = (r < n_gy // 2) == (target < n_gy // 2)
        outs[k][:EDGE, :] = halo
        outs[k][EDGE:, :] = jnp.where(same, sums, flipped)
    after = lax.rem(c + 1, n_gx)
    before = lax.rem(c + n_gx - 1, n_gx)
    fetch.wait()
    partner = fold[c]
    edges[0:1, :] = gathered[after, 0:1, :]
    edges[1:3, :] = gathered[after, lon : lon + 2, :]
    edges[3:4, :] = gathered[before, lon - 1 : lon, :]
    edges[4:7, :] = gathered[before, lon + 2 : lon + 5, :]
    edges[7:8, :] = jnp.zeros((1, lat), F32)
    across = jnp.concatenate(
        [gathered[partner, lon + 5 : lon + EDGE, :], jnp.zeros((5, lat), F32)], axis=0
    )
    i, j = iota((lat, lat), 0), iota((lat, lat), 1)
    back = jnp.where((i < lon) & (i + j == lon - 1), 1.0, 0.0).astype(F32)
    edges[EDGE:, :] = dot(across, back)


def scheduled(plan, c, sched, i, h):
    at = (i * CHAINS + h) * 2
    slot, chunk = sched[0, at], sched[0, at + 1]
    even = lax.rem(slot, 2) == 0
    group = slot * plan.n_gx + jnp.where(even, c, plan.n_gx - 1 - c)
    return slot, chunk, group


def basis_kernel(plan, sched_v, geo, seed_logs, p_out, unscale, seeds, state, sched, sem):
    slots, half = plan.n_slots, plan.half
    c, _ = here()
    fetch = pltpu.make_async_copy(sched_v, sched, sem)
    fetch.start()
    log_sin = geo[1:2, :]
    sub = iota((GROUP, half), 0)
    pick = iota(seed_logs.shape, 1) == c
    logs = jnp.sum(jnp.where(pick, seed_logs[...], 0.0), axis=1, keepdims=True)
    for s in range(slots):
        group = s * plan.n_gx + (c if s % 2 == 0 else plan.n_gx - 1 - c)
        order = (sub + group * GROUP).astype(F32)
        exponent = order * log_sin + logs[s * GROUP : (s + 1) * GROUP]
        shift = jnp.clip(-exponent - 80.0, 0.0, 80.0)
        seeds[s] = jnp.exp(exponent + shift) * (1.0 / math.sqrt(4.0 * math.pi))
        unscale[s] = jnp.exp(-shift)
    state[...] = jnp.zeros(state.shape, F32)
    seeds[slots] = jnp.zeros((GROUP, half), F32)
    unscale[slots] = jnp.zeros((GROUP, half), F32)
    x = jnp.broadcast_to(geo[0:1, :], (GROUP, half))
    sub_c = iota((GROUP, 128), 0)
    lane_c = iota((GROUP, 128), 1)
    fetch.wait()

    def coefficients(i, h):
        _, chunk, group = scheduled(plan, c, sched, i, h)
        m0 = group * GROUP
        degree = (m0 + chunk * STEPS + lane_c).astype(F32)
        order = (m0 + sub_c).astype(F32)
        below = degree - 1.0
        growth = jnp.sqrt(
            jnp.maximum(4.0 * degree * degree - 1.0, 1.0)
            / jnp.maximum(degree * degree - order * order, 1.0)
        )
        damping = jnp.sqrt(
            jnp.maximum(below * below - order * order, 0.0)
            / jnp.maximum(4.0 * below * below - 1.0, 1.0)
        )
        return growth, growth * damping

    def begin(i, h):
        slot, chunk, _ = scheduled(plan, c, sched, i, h)
        started = jnp.where(chunk == 0, 0.0, 1.0).astype(F32)
        seed = seeds[slot] * (1.0 - started)
        return slot, seed, state[slot, 0], state[slot, 1]

    def body(i, carry):
        lanes = [begin(i, h) for h in range(CHAINS)]
        ahead = [coefficients(jnp.minimum(i + 1, plan.n_iter - 1), h) for h in range(CHAINS)]
        previous = [lane[2] for lane in lanes]
        before = [lane[3] for lane in lanes]
        pairs = [[] for _ in range(CHAINS)]
        for t in range(STEPS):
            for h, (_, seed, _, _) in enumerate(lanes):
                growth, fall = carry[h]
                a = jnp.broadcast_to(growth[:, t : t + 1], (GROUP, half))
                b = jnp.broadcast_to(fall[:, t : t + 1], (GROUP, half))
                value = (a * x) * previous[h] - b * before[h]
                if t < GROUP:
                    value = value + jnp.where(sub == t, seed, 0.0)
                previous[h], before[h] = value, previous[h]
                pairs[h].append(value)
                if t % 2 == 1:
                    both = jnp.concatenate(pairs[h], axis=0)
                    both_hi = both.astype(BF16)
                    at = (t - 1) * GROUP
                    p_out[i, h, 0, at : at + 2 * GROUP, :] = both_hi
                    p_out[i, h, 1, at : at + 2 * GROUP, :] = (
                        both - both_hi.astype(F32)
                    ).astype(BF16)
                    pairs[h] = []
        for h, lane in enumerate(lanes):
            state[lane[0], 0] = previous[h]
            state[lane[0], 1] = before[h]
        return tuple(ahead)

    lax.fori_loop(0, plan.n_iter, body, tuple(coefficients(0, h) for h in range(CHAINS)))


def legendre_kernel(plan, *refs):
    n_gy, slots, half = plan.n_gy, plan.n_slots, plan.half
    lon, lat, k_half = plan.tile_lon, plan.tile_lat, plan.k_dev // 2
    blocks = refs[:n_gy]
    basis, unscale, love, sched_v, out = refs[n_gy : n_gy + 5]
    (fabs, lhs, weights, acc, coeffs_a, coeffs_b, own_b, mirror_b, sched, sem) = refs[n_gy + 5 :]
    c, r = here()
    fetch = pltpu.make_async_copy(sched_v, sched, sem)
    fetch.start()
    n_half = n_gy // 2
    for k in range(n_gy):
        fabs[lax.rem(r - k + n_gy, n_gy)] = blocks[k][EDGE:, :]
    first_row = jnp.where(r < n_half, 0, n_half)
    sym, anti = [], []
    for b in range(n_half):
        near, far = fabs[first_row + b], fabs[n_gy - 1 - first_row - b]
        sym.append(near + far)
        anti.append(near - far)
    sym = jnp.concatenate(sym, axis=1)
    anti = jnp.concatenate(anti, axis=1)
    for s in range(slots):
        lo, hi = s * GROUP, (s + 1) * GROUP
        rows = jnp.concatenate(
            [sym[lo:hi], anti[lo:hi], sym[k_half + lo : k_half + hi], anti[k_half + lo : k_half + hi]],
            axis=0,
        )
        rows = rows * jnp.concatenate([unscale[s]] * 4, axis=0)
        rows_hi = rows.astype(BF16)
        lhs[s, : 4 * GROUP, :] = rows_hi
        lhs[s, 4 * GROUP :, :] = (rows - rows_hi.astype(F32)).astype(BF16)
    acc[...] = jnp.zeros(acc.shape, F32)
    lhs[slots] = jnp.zeros((8 * GROUP, half), BF16)
    fetch.wait()
    row = iota((4 * GROUP, ROWS), 0)
    lane = iota((4 * GROUP, ROWS), 1)
    i_row, i_lane, t_lane = row % GROUP, lane % GROUP, lane // GROUP
    keep = jnp.where(
        (i_row == i_lane) & ((t_lane + i_row) % 2 == (row // GROUP) % 2), 1.0, 0.0
    ).astype(F32)
    starts = 128 // GROUP
    nt = (((1,), (1,)), ((), ()))
    nn = (((1,), (0,)), ((), ()))
    n = 4 * GROUP

    def products(i, h):
        left = lhs[scheduled(plan, c, sched, i, h)[0]]
        one = lax.dot_general(left, basis[i, h, 0], nt, preferred_element_type=F32)
        two = lax.dot_general(left[:n], basis[i, h, 1], nt, preferred_element_type=F32)
        return one[:n] + one[n:] + two

    def coefficients(i, h, total):
        _, chunk, group = scheduled(plan, c, sched, i, h)
        begin = group + chunk * (STEPS // GROUP)
        at = (begin // starts + 1) * starts - 1 - lax.rem(begin, starts)
        coeff = total * keep * weights[at]
        coeff_hi = coeff.astype(BF16)
        coeff_lo = (coeff - coeff_hi.astype(F32)).astype(BF16)
        return jnp.concatenate([coeff_hi, coeff_lo], axis=0)

    def synthesise(i, h, right):
        three = lax.dot_general(right, basis[i, h, 0], nn, preferred_element_type=F32)
        four = lax.dot_general(right[:n], basis[i, h, 1], nn, preferred_element_type=F32)
        return three[:n] + three[n:] + four

    def analyse_all(k, into):
        for j in range(UNROLL):
            for h in range(CHAINS):
                i = k * UNROLL + j
                into[j, h] = coefficients(i, h, products(i, h))

    def synthesise_all(k, given):
        found = []
        for j in range(UNROLL):
            for h in range(CHAINS):
                i = k * UNROLL + j
                slot = scheduled(plan, c, sched, i, h)[0]
                found.append((slot, synthesise(i, h, given[j, h])))
        for slot, part in found:
            acc[slot] += part

    stages = plan.n_iter // UNROLL
    first = [[products(j, h) for h in range(CHAINS)] for j in range(UNROLL)]
    width = plan.love_width
    padded = jnp.concatenate(
        [love[...].reshape(1, -1), jnp.zeros((1, width - plan.degrees), F32)], axis=1
    )
    shifted = pltpu.roll(
        jnp.broadcast_to(padded, (starts, width)),
        width - GROUP * (starts - 1), 1, stride=GROUP, stride_axis=0,
    )
    shifted = jnp.concatenate(
        [shifted[:, k * 128 : (k + 1) * 128] for k in range(width // 128)], axis=0
    )
    spread = iota((128, ROWS), 1) // GROUP == iota((128, ROWS), 0)
    weights[...] = dot(shifted, jnp.where(spread, 1.0, 0.0).astype(F32)).reshape(
        weights.shape
    )
    for j in range(UNROLL):
        for h in range(CHAINS):
            coeffs_a[j, h] = coefficients(j, h, first[j][h])

    trips = (stages - 1) // 2
    for k in range(trips):
        analyse_all(2 * k + 1, coeffs_b)
        synthesise_all(2 * k, coeffs_a)
        analyse_all(2 * k + 2, coeffs_a)
        synthesise_all(2 * k + 1, coeffs_b)
    if stages % 2 == 0:
        analyse_all(stages - 1, coeffs_b)
    synthesise_all(2 * trips, coeffs_a)
    if stages % 2 == 0:
        synthesise_all(stages - 1, coeffs_b)

    for s in range(slots):
        lo, hi = s * GROUP, (s + 1) * GROUP
        g = acc[s] * jnp.concatenate([unscale[s]] * 4, axis=0)
        for part in range(2):
            even = g[2 * part * GROUP : (2 * part + 1) * GROUP]
            odd = g[(2 * part + 1) * GROUP : (2 * part + 2) * GROUP]
            for b in range(n_half):
                lanes = slice(b * lat, (b + 1) * lat)
                where = slice(part * k_half + lo, part * k_half + hi)
                own_b[b, where, :] = even[:, lanes] + odd[:, lanes]
                mirror_b[b, where, :] = even[:, lanes] - odd[:, lanes]
    k_dev = plan.k_dev
    mine = r - first_row
    out[:k_dev, :] = own_b[mine]
    up = jnp.where(
        r == n_half - 1,
        mirror_b[mine][:, lat - 1 :],
        own_b[jnp.minimum(mine + 1, n_half - 1)][:, :1],
    )
    down = jnp.where(
        r == n_half, mirror_b[mine][:, :1], own_b[jnp.maximum(mine - 1, 0)][:, lat - 1 :]
    )
    lane_o = iota((k_dev, lat), 1)
    columns = jnp.where(lane_o == 0, up, jnp.where(lane_o == 1, down, 0.0))
    out[k_dev:, :] = rows_of(columns, lat)


def finish_kernel(
    plan, terms, a_table, b_table, fold_v, north_tile, south_tile, edges,
    surface_ref, depth_ref, mask, east_ref, north_ref,
    sal_out, east_out, north_out, height_out, fold, sem,
):
    lon, lat = plan.tile_lon, plan.tile_lat
    c, r = here()
    fetch = pltpu.make_async_copy(fold_v, fold, sem)
    fetch.start()
    split = lon + EDGE
    a_own = a_table[c]
    own_trig = a_own[0:1, :] * b_table[0, :split, :] + a_own[1:2, :] * b_table[1, :split, :]
    fetch.wait()
    a_fold = a_table[fold[c]]
    fold_trig = a_fold[0:1, :] * b_table[0, split:, :] + a_fold[1:2, :] * b_table[1, split:, :]
    trig = jnp.concatenate([own_trig, fold_trig], axis=0)
    k_dev, n_gx = plan.k_dev, plan.n_gx
    main = jnp.concatenate([terms[d, :k_dev, :] for d in range(n_gx)], axis=0)
    sal_all = dot3(trig, main)
    up = jnp.concatenate([terms[d, k_dev : k_dev + 1, :k_dev] for d in range(n_gx)], axis=1)
    down = jnp.concatenate([terms[d, k_dev + 1 : k_dev + 2, :k_dev] for d in range(n_gx)], axis=1)
    sal_up = jnp.sum(trig[:lon] * up, axis=1, keepdims=True)
    sal_down = jnp.sum(trig[:lon] * down, axis=1, keepdims=True)
    sal = sal_all[:lon, :lat]
    sal_out[...] = sal
    is_top = r == plan.n_gy - 1
    sal_n = jnp.where(is_top, sal_all[split:, lat - 1 :], sal_up)
    sal_s = sal_down
    surface, depth = surface_ref[...], depth_ref[...]
    wet = mask[...].astype(F32)
    east, north = east_ref[...], north_ref[...]
    turned = jnp.concatenate(
        [north_tile[:EDGE, :], south_tile[:EDGE, :], edges[EDGE:, :],
         jnp.zeros((lat - 3 * EDGE, lat), F32)], axis=0,
    ).T[:lon, :]
    north_tile, south_tile = turned[:, :EDGE], turned[:, EDGE : 2 * EDGE]
    across = turned[:, 2 * EDGE : 3 * EDGE]
    surf_n = jnp.where(is_top, across[:, 2:3], north_tile[:lon, 4:5])
    depth_n = jnp.where(is_top, across[:, 0:1], north_tile[:lon, 5:6])
    wet_n = jnp.where(is_top, across[:, 1:2], north_tile[:lon, 6:7])
    pressure = surface - sal
    row = iota((lon, lat), 0)
    lane = iota((lon, lat), 1)

    def east_of(field, edge):
        return jnp.where(row == lon - 1, edge, pltpu.roll(field, lon - 1, 0))

    def north_of(field, edge):
        return jnp.where(lane == lat - 1, edge, pltpu.roll(field, lat - 1, 1))

    p_e = edges[0:1, :] - sal_all[lon : lon + 1, :lat]
    p_w = edges[3:4, :] - sal_all[lon + 1 : lon + 2, :lat]
    east_next = wet * east_of(wet, edges[2:3, :]) * (
        east - COURANT * (east_of(pressure, p_e) - pressure)
    )
    north_next = wet * north_of(wet, wet_n) * (
        north - COURANT * (north_of(pressure, surf_n - sal_n) - pressure)
    )
    east_out[...] = east_next
    north_out[...] = north_next
    east_flux = 0.5 * (depth + east_of(depth, edges[1:2, :])) * east_next
    north_flux = 0.5 * (depth + north_of(depth, depth_n)) * north_next
    west_face = edges[5:6, :] * wet[:1] * (edges[6:7, :] - COURANT * (pressure[:1] - p_w))
    west_edge = 0.5 * (edges[4:5, :] + depth[:1]) * west_face
    south_face = south_tile[:lon, 2:3] * wet[:, :1] * (
        south_tile[:lon, 3:4] - COURANT * (pressure[:, :1] - (south_tile[:lon, 0:1] - sal_s))
    )
    south_edge = 0.5 * (south_tile[:lon, 1:2] + depth[:, :1]) * south_face
    south_edge = jnp.where(r > 0, south_edge, 0.0)
    west_flux = jnp.where(row == 0, west_edge, pltpu.roll(east_flux, 1, 0))
    south_flux = jnp.where(lane == 0, south_edge, pltpu.roll(north_flux, 1, 1))
    height_out[...] = wet * (
        surface - COURANT * (east_flux - west_flux + north_flux - south_flux)
    )


VMEM = pl.BlockSpec(memory_space=pltpu.VMEM)
HBM = pl.BlockSpec(memory_space=pltpu.HBM)
SLICED_GX = (5, 10)
SLICED_GY = (7,)
SLICED_HALF = (8,)


def on_device(height, east_speed, north_speed, water_depth, ocean_mask, fold_partner, love_factor):
    lon, lat = height.shape
    n_gx, n_gy = lax.axis_size("gx"), lax.axis_size("gy")
    plan = Plan(lon, lat, n_gx, n_gy, love_factor.shape[0])
    slots, half = plan.n_slots, plan.half
    sent = lon + EDGE
    sources = (
        height, ocean_mask, water_depth, east_speed, north_speed, plan.u_table, plan.v_table,
        plan.quad, plan.geo, plan.seed_logs, plan.sched, love_factor, fold_partner,
    )
    sources = tuple(
        pltpu.with_memory_space_constraint(jnp.asarray(source), pltpu.HBM) for source in sources
    )
    kept_shapes = [
        source.shape[1:] if k in SLICED_GX + SLICED_GY + SLICED_HALF else source.shape
        for k, source in enumerate(sources)
    ]
    kept = [
        pltpu.VMEM(shape, source.dtype) for shape, source in zip(kept_shapes[1:], sources[1:])
    ]
    packed, surface, *kept = pl.pallas_call(
        lambda *refs: pack_kernel(plan, *refs),
        in_specs=[HBM] * len(sources),
        out_specs=[VMEM] * (len(sources) + 1),
        out_shape=(pltpu.VMEM((sent, lat), F32), pltpu.VMEM((lon, lat), F32), *kept),
        scratch_shapes=[pltpu.VMEM((lon, lat), F32), pltpu.SemaphoreType.DMA((len(sources),))],
        compiler_params=PARAMS,
        name="pack",
    )(*sources)
    mask, depth, east, north, u, v, quad, geo, seed_logs, sched, love, fold = kept
    gathered = lax.all_gather(packed, "gx", axis=0, tiled=False)
    rows = EDGE + plan.k_dev
    fold_scratch = [pltpu.SMEM((n_gx,), jnp.int32), pltpu.SemaphoreType.DMA]
    *messages, edges = pl.pallas_call(
        lambda *refs: fourier_kernel(plan, *refs),
        in_specs=[VMEM] * 9,
        out_specs=[VMEM] * (n_gy + 1),
        out_shape=(
            *[pltpu.VMEM((rows, lat), F32) for _ in range(n_gy)],
            pltpu.VMEM((2 * EDGE, lat), F32),
        ),
        scratch_shapes=fold_scratch,
        compiler_params=PARAMS,
        name="fourier",
    )(gathered, u, v, quad, surface, depth, mask, north, fold)
    blocks = [messages[0]]
    for k in range(1, n_gy):
        ring = [(i, (i + k) % n_gy) for i in range(n_gy)]
        blocks.append(lax.ppermute(messages[k], "gy", ring))
    sched_scratch = [pltpu.SMEM((1, plan.sched_width), jnp.int32), pltpu.SemaphoreType.DMA]
    basis, unscale = pl.pallas_call(
        lambda *refs: basis_kernel(plan, *refs),
        in_specs=[VMEM] * 3,
        out_specs=[VMEM] * 2,
        out_shape=(
            pltpu.VMEM((plan.n_iter, CHAINS, 2, ROWS, half), BF16),
            pltpu.VMEM((slots + 1, GROUP, half), F32),
        ),
        scratch_shapes=[
            pltpu.VMEM((slots + 1, GROUP, half), F32),
            pltpu.VMEM((slots + 1, 2, GROUP, half), F32),
        ]
        + sched_scratch,
        cost_estimate=pl.CostEstimate(flops=60_000_000, bytes_accessed=1_000_000, transcendentals=0),
        compiler_params=PARAMS,
        name="basis",
    )(sched, geo, seed_logs)
    split_shape = pltpu.VMEM((n_gy // 2, plan.k_dev, lat), F32)
    terms = pl.pallas_call(
        lambda *refs: legendre_kernel(plan, *refs),
        in_specs=[VMEM] * (n_gy + 4),
        out_specs=VMEM,
        out_shape=pltpu.VMEM((plan.k_dev + EDGE, lat), F32),
        scratch_shapes=[
            pltpu.VMEM((n_gy, plan.k_dev, lat), F32),
            pltpu.VMEM((slots + 1, 8 * GROUP, half), BF16),
            pltpu.VMEM((plan.love_width // GROUP, 1, ROWS), F32),
            pltpu.VMEM((slots + 1, 4 * GROUP, half), F32),
            pltpu.VMEM((UNROLL, CHAINS, 8 * GROUP, ROWS), BF16),
            pltpu.VMEM((UNROLL, CHAINS, 8 * GROUP, ROWS), BF16),
            split_shape, split_shape,
        ]
        + sched_scratch,
        compiler_params=PARAMS,
        name="legendre",
    )(*blocks, basis, unscale, love, sched)
    everything = lax.all_gather(terms, "gx", axis=0, tiled=False)
    tile = jax.ShapeDtypeStruct((lon, lat), F32)
    a_table, b_table = jnp.asarray(plan.a_table), jnp.asarray(plan.b_table)
    return pl.pallas_call(
        lambda *refs: finish_kernel(plan, *refs),
        in_specs=[VMEM] * 12,
        out_specs=[VMEM] * 4,
        out_shape=(tile,) * 4,
        scratch_shapes=fold_scratch,
        compiler_params=PARAMS,
        name="finish",
    )(
        everything, a_table, b_table, fold, blocks[n_gy - 1], blocks[1], edges,
        surface, depth, mask, east, north,
    )


def solution(mesh):
    spec = P("gx", "gy")
    return jax.shard_map(
        on_device,
        mesh=mesh,
        in_specs=(spec, spec, spec, spec, spec, P(), P()),
        out_specs=(spec,) * 4,
        check_vma=False,
    )
```

```python
import math

import numpy as np

import jax
import jax.numpy as jnp
from jax import lax
from jax.experimental import pallas as pl
from jax.experimental.pallas import tpu as pltpu
from jax.sharding import PartitionSpec as P

COURANT = 0.35
GROUP = 8
STEPS = 32
ROWS = GROUP * STEPS
CHAINS = 3
UNROLL = 2
EDGE = 8
F32 = jnp.float32
BF16 = jnp.bfloat16
HIGHEST = lax.Precision.HIGHEST
PARAMS = pltpu.CompilerParams(vmem_limit_bytes=16 * 1024 * 1024)


class Plan:
    def __init__(self, tile_lon, tile_lat, n_gx, n_gy, degrees):
        self.tile_lon, self.tile_lat = tile_lon, tile_lat
        self.n_gx, self.n_gy, self.degrees = n_gx, n_gy, degrees
        self.nlon, self.nlat = tile_lon * n_gx, tile_lat * n_gy
        self.half = self.nlat // 2
        self.n_groups = -(-degrees // GROUP)
        self.n_slots = -(-self.n_groups // n_gx)
        self.k_dev = 2 * self.n_slots * GROUP
        self.k_all = self.k_dev * n_gx
        self.group_of = np.array(
            [
                [s * n_gx + (c if s % 2 == 0 else n_gx - 1 - c) for s in range(self.n_slots)]
                for c in range(n_gx)
            ],
            np.int32,
        )
        self._schedule()
        self._tables()

    def _schedule(self):
        lists = []
        for c in range(self.n_gx):
            counts = []
            for s in range(self.n_slots):
                left = self.degrees - GROUP * int(self.group_of[c, s])
                counts.append(-(-max(left, 0) // STEPS))
            lists.append(counts)
        longest = max(-(-sum(counts) // CHAINS) for counts in lists)
        longest = max(longest, max(max(counts) for counts in lists))
        self.n_iter = -(-longest // UNROLL) * UNROLL
        per_row = self.n_iter * CHAINS * 2
        self.sched_width = -(-per_row // 128) * 128
        self.sched = np.zeros((self.n_gx, 1, self.sched_width), np.int32)
        for c, counts in enumerate(lists):
            chains, room = [[]], self.n_iter
            for s, count in enumerate(counts):
                if room >= count:
                    chains[-1] += [(s, k) for k in range(count)]
                    room -= count
                else:
                    head = count - room
                    chains[-1] += [(s, k) for k in range(head, count)]
                    chains.append([(s, k) for k in range(head)])
                    room = self.n_iter - head
            chains += [[] for _ in range(CHAINS - len(chains))]
            for h, chain in enumerate(chains):
                chain += [(self.n_slots, 0)] * (self.n_iter - len(chain))
                for i, item in enumerate(chain):
                    at = (i * CHAINS + h) * 2
                    self.sched[c, 0, at : at + 2] = item
        top = self.n_gx * (self.n_slots + 1) * GROUP
        self.love_width = -(-(max(top, self.degrees) + 2 * STEPS) // 128) * 128

    def _tables(self):
        rows = np.arange(self.nlat).reshape(2, self.half)
        theta = np.pi * (rows + 0.5) / self.nlat
        self.geo = np.zeros((2, 8, self.half), np.float32)
        self.geo[:, 0] = np.cos(theta)
        self.geo[:, 1] = np.log(np.sin(theta))
        all_theta = np.pi * (np.arange(self.nlat) + 0.5) / self.nlat
        quad = np.pi / self.nlat * (2.0 * np.pi / self.nlon) * np.sin(all_theta)
        self.quad = np.repeat(
            quad.reshape(self.n_gy, 1, self.tile_lat), 8, axis=1
        ).astype(np.float32)
        top = GROUP * (int(self.group_of.max()) + 1)
        factors = np.arange(1, top, dtype=np.float64)
        logs = np.concatenate([[0.0], np.cumsum(0.5 * np.log((2 * factors + 1) / (2 * factors)))])
        orders = self.group_of[:, :, None] * GROUP + np.arange(GROUP)[None, None, :]
        lanes = -(-self.n_gx // 128) * 128
        self.seed_logs = np.zeros((self.n_slots * GROUP, lanes), np.float32)
        self.seed_logs[:, : self.n_gx] = logs[orders].reshape(self.n_gx, -1).T
        lam = 2.0 * np.pi / self.nlon
        cols = np.arange(self.nlon)
        base = (self.group_of[:, :, None] * GROUP * cols[None, None, :]) % self.nlon
        u = np.stack([np.cos(lam * base), np.sin(lam * base)], axis=2)
        pad = -(-2 * self.n_slots // 8) * 8
        self.u_rows = pad
        self.u_table = np.zeros((self.n_gx, pad, self.nlon), np.float32)
        self.u_table[:, : 2 * self.n_slots] = u.reshape(self.n_gx, 2 * self.n_slots, self.nlon)
        small = (np.arange(GROUP)[:, None] * cols[None, :]) % self.nlon
        self.v_table = np.concatenate([np.cos(lam * small), np.sin(lam * small)]).astype(np.float32)
        m = np.concatenate(
            [np.tile(orders[c].reshape(-1), 2) for c in range(self.n_gx)]
        )
        sine = np.tile(np.repeat([0, 1], self.k_dev // 2), self.n_gx)
        nu = np.where(m == 0, 1.0, 2.0) * (m < self.degrees)
        starts = np.arange(self.n_gx) * self.tile_lon
        phase = lam * ((starts[:, None] * m[None, :]) % self.nlon)
        a1 = nu * np.where(sine == 0, np.cos(phase), np.sin(phase))
        a2 = nu * np.where(sine == 0, -np.sin(phase), np.cos(phase))
        self.a_table = np.zeros((self.n_gx, 8, self.k_all), np.float32)
        self.a_table[:, 0] = a1
        self.a_table[:, 1] = a2
        offsets = np.concatenate(
            [
                np.arange(self.tile_lon),
                [self.tile_lon, -1],
                np.zeros(EDGE - 2),
                np.arange(self.tile_lon)[::-1],
            ]
        ).astype(np.int64)
        phase = lam * ((offsets[:, None] * m[None, :]) % self.nlon)
        self.b_table = np.stack([np.cos(phase), np.sin(phase)]).astype(np.float32)
        self.o_rows = offsets.shape[0]


def iota(shape, axis):
    return lax.broadcasted_iota(jnp.int32, shape, axis)


def dot(a, b):
    return lax.dot_general(
        a, b, (((1,), (0,)), ((), ())), precision=HIGHEST, preferred_element_type=F32
    )


def dot3(a, b):
    a_hi, b_hi = a.astype(BF16), b.astype(BF16)
    a_lo = (a - a_hi.astype(F32)).astype(BF16)
    b_lo = (b - b_hi.astype(F32)).astype(BF16)
    n = a.shape[0]
    dims = (((1,), (0,)), ((), ()))
    both = jnp.concatenate([a_hi, a_lo], axis=0)
    big = lax.dot_general(both, b_hi, dims, preferred_element_type=F32)
    small = lax.dot_general(a_hi, b_lo, dims, preferred_element_type=F32)
    return big[:n] + (big[n:] + small)


def rows_of(tile, size):
    height = tile.shape[0]
    tile = jnp.concatenate([tile, jnp.zeros((size - height, size), F32)], axis=0)
    return tile.T[:EDGE, :]


def flip_matrix(size, flipped):
    row = iota((size, size), 0)
    col = iota((size, size), 1)
    target = jnp.where(flipped, size - 1 - col, col)
    return jnp.where(row == target, 1.0, 0.0).astype(F32)


def here():
    return lax.axis_index("gx"), lax.axis_index("gy")


def pack_kernel(plan, *refs):
    count = len(refs) // 2 - 1
    height, mask, depth, east = refs[:4]
    sources = refs[:count]
    out, surface_out = refs[count : count + 2]
    kept = refs[count + 2 : 2 * count + 1]
    height_v, sem = refs[2 * count + 1 :]
    c, r = here()
    targets = (height_v,) + tuple(kept)
    copies = []
    for k, (source, target) in enumerate(zip(sources, targets)):
        if k in SLICED_GX:
            source = source.at[c]
        elif k in SLICED_GY:
            source = source.at[r]
        elif k in SLICED_HALF:
            source = source.at[jnp.where(r < plan.n_gy // 2, 0, 1)]
        copies.append(pltpu.make_async_copy(source, target, sem.at[k]))
    for copy in copies:
        copy.start()
    for copy in copies[:4]:
        copy.wait()
    _, mask_v, depth_v, east_v = targets[:4]
    lon, lat = height_v.shape
    wet = mask_v[...].astype(F32)
    surface = wet * height_v[...]
    surface_out[...] = surface
    out[:lon, :] = surface
    out[lon : lon + 1, :] = depth_v[:1, :]
    out[lon + 1 : lon + 2, :] = wet[:1, :]
    out[lon + 2 : lon + 3, :] = depth_v[lon - 1 :, :]
    out[lon + 3 : lon + 4, :] = wet[lon - 1 :, :]
    out[lon + 4 : lon + 5, :] = east_v[lon - 1 :, :]
    lane = iota((lon, lat), 1)
    tile = jnp.zeros((lon, lat), F32)
    for k, array in enumerate([depth_v, wet, surface]):
        tile = jnp.where(lane == k, array[:, lat - 1 :], tile)
    out[lon + 5 :, :] = rows_of(tile, lat)[: EDGE - 5]
    for copy in copies[4:]:
        copy.wait()


def fourier_kernel(plan, *refs):
    gathered, u, v, quad, surface, depth, mask, north, fold_v = refs[:9]
    n_gx, n_gy, slots = plan.n_gx, plan.n_gy, plan.n_slots
    outs, edges, fold, sem = refs[9 : 9 + n_gy], *refs[9 + n_gy :]
    lon, lat = plan.tile_lon, plan.tile_lat
    c, r = here()
    fetch = pltpu.make_async_copy(fold_v, fold, sem)
    fetch.start()
    field = jnp.concatenate([gathered[d, :lon, :] for d in range(n_gx)], axis=0)
    vc, vs = v[:GROUP, :], v[GROUP:, :]
    cos_rows, sin_rows = [], []
    for s in range(slots):
        uc = u[2 * s : 2 * s + 1, :]
        us = u[2 * s + 1 : 2 * s + 2, :]
        cos_rows.append(uc * vc - us * vs)
        sin_rows.append(us * vc + uc * vs)
    trig = jnp.concatenate(cos_rows + sin_rows, axis=0)
    sums = dot3(trig, field) * quad[:1, :]
    flipped = dot3(sums, flip_matrix(lat, True))
    wet = mask[...].astype(F32)
    lane = iota((lon, lat), 1)
    tile = jnp.zeros((lon, lat), F32)
    for k, array in enumerate([surface, depth, wet, north]):
        tile = jnp.where(lane == k, array[:, lat - 1 :], tile)
    for k, array in enumerate([surface, depth, wet]):
        tile = jnp.where(lane == 4 + k, array[:, :1], tile)
    halo = rows_of(tile, lat)
    for k in range(n_gy):
        target = lax.rem(r + k, n_gy)
        same = (r < n_gy // 2) == (target < n_gy // 2)
        outs[k][:EDGE, :] = halo
        outs[k][EDGE:, :] = jnp.where(same, sums, flipped)
    after = lax.rem(c + 1, n_gx)
    before = lax.rem(c + n_gx - 1, n_gx)
    fetch.wait()
    partner = fold[c]
    edges[0:1, :] = gathered[after, 0:1, :]
    edges[1:3, :] = gathered[after, lon : lon + 2, :]
    edges[3:4, :] = gathered[before, lon - 1 : lon, :]
    edges[4:7, :] = gathered[before, lon + 2 : lon + 5, :]
    edges[7:8, :] = jnp.zeros((1, lat), F32)
    across = jnp.concatenate(
        [gathered[partner, lon + 5 : lon + EDGE, :], jnp.zeros((5, lat), F32)], axis=0
    )
    i, j = iota((lat, lat), 0), iota((lat, lat), 1)
    back = jnp.where((i < lon) & (i + j == lon - 1), 1.0, 0.0).astype(F32)
    edges[EDGE:, :] = dot(across, back)


def scheduled(plan, c, sched, i, h):
    at = (i * CHAINS + h) * 2
    slot, chunk = sched[0, at], sched[0, at + 1]
    even = lax.rem(slot, 2) == 0
    group = slot * plan.n_gx + jnp.where(even, c, plan.n_gx - 1 - c)
    return slot, chunk, group


def basis_kernel(
    plan, sched_v, geo, seed_logs, fold_v, a_table, p_out, unscale, a_own, a_fold,
    seeds, state, sched, fold, sem,
):
    slots, half = plan.n_slots, plan.half
    c, _ = here()
    fetch = pltpu.make_async_copy(sched_v, sched, sem.at[0])
    fetch.start()
    fetch_fold = pltpu.make_async_copy(fold_v, fold, sem.at[1])
    fetch_fold.start()
    fetch_own = pltpu.make_async_copy(a_table.at[c], a_own, sem.at[2])
    fetch_own.start()
    log_sin = geo[1:2, :]
    sub = iota((GROUP, half), 0)
    pick = iota(seed_logs.shape, 1) == c
    logs = jnp.sum(jnp.where(pick, seed_logs[...], 0.0), axis=1, keepdims=True)
    for s in range(slots):
        group = s * plan.n_gx + (c if s % 2 == 0 else plan.n_gx - 1 - c)
        order = (sub + group * GROUP).astype(F32)
        exponent = order * log_sin + logs[s * GROUP : (s + 1) * GROUP]
        shift = jnp.clip(-exponent - 80.0, 0.0, 80.0)
        seeds[s] = jnp.exp(exponent + shift) * (1.0 / math.sqrt(4.0 * math.pi))
        unscale[s] = jnp.exp(-shift)
    state[...] = jnp.zeros(state.shape, F32)
    seeds[slots] = jnp.zeros((GROUP, half), F32)
    unscale[slots] = jnp.zeros((GROUP, half), F32)
    x = jnp.broadcast_to(geo[0:1, :], (GROUP, half))
    sub_c = iota((GROUP, 128), 0)
    lane_c = iota((GROUP, 128), 1)
    fetch.wait()
    fetch_fold.wait()
    fetch_across = pltpu.make_async_copy(a_table.at[fold[c]], a_fold, sem.at[1])
    fetch_across.start()

    def coefficients(i, h):
        _, chunk, group = scheduled(plan, c, sched, i, h)
        m0 = group * GROUP
        degree = (m0 + chunk * STEPS + lane_c).astype(F32)
        order = (m0 + sub_c).astype(F32)
        below = degree - 1.0
        growth = jnp.sqrt(
            jnp.maximum(4.0 * degree * degree - 1.0, 1.0)
            / jnp.maximum(degree * degree - order * order, 1.0)
        )
        damping = jnp.sqrt(
            jnp.maximum(below * below - order * order, 0.0)
            / jnp.maximum(4.0 * below * below - 1.0, 1.0)
        )
        return growth, growth * damping

    def begin(i, h):
        slot, chunk, _ = scheduled(plan, c, sched, i, h)
        started = jnp.where(chunk == 0, 0.0, 1.0).astype(F32)
        seed = seeds[slot] * (1.0 - started)
        return slot, seed, state[slot, 0], state[slot, 1]

    def body(i, carry):
        lanes = [begin(i, h) for h in range(CHAINS)]
        ahead = [coefficients(jnp.minimum(i + 1, plan.n_iter - 1), h) for h in range(CHAINS)]
        previous = [lane[2] for lane in lanes]
        before = [lane[3] for lane in lanes]
        pairs = [[] for _ in range(CHAINS)]
        for t in range(STEPS):
            for h, (_, seed, _, _) in enumerate(lanes):
                growth, fall = carry[h]
                a = jnp.broadcast_to(growth[:, t : t + 1], (GROUP, half))
                b = jnp.broadcast_to(fall[:, t : t + 1], (GROUP, half))
                value = (a * x) * previous[h] - b * before[h]
                if t < GROUP:
                    value = value + jnp.where(sub == t, seed, 0.0)
                previous[h], before[h] = value, previous[h]
                pairs[h].append(value)
                if t % 2 == 1:
                    both = jnp.concatenate(pairs[h], axis=0)
                    both_hi = both.astype(BF16)
                    at = (t - 1) * GROUP
                    both_lo = (both - both_hi.astype(F32)).astype(BF16)
                    for k in range(half // 128):
                        lanes_k = slice(k * 128, (k + 1) * 128)
                        p_out[i, h, 0, k, at : at + 2 * GROUP, :] = both_hi[:, lanes_k]
                        p_out[i, h, 1, k, at : at + 2 * GROUP, :] = both_lo[:, lanes_k]
                    pairs[h] = []
        for h, lane in enumerate(lanes):
            state[lane[0], 0] = previous[h]
            state[lane[0], 1] = before[h]
        return tuple(ahead)

    lax.fori_loop(0, plan.n_iter, body, tuple(coefficients(0, h) for h in range(CHAINS)))
    fetch_own.wait()
    fetch_across.wait()


def legendre_kernel(plan, *refs):
    n_gy, slots, half = plan.n_gy, plan.n_slots, plan.half
    lon, lat, k_half = plan.tile_lon, plan.tile_lat, plan.k_dev // 2
    blocks = refs[:n_gy]
    basis, unscale, love, sched_v, out = refs[n_gy : n_gy + 5]
    (fabs, lhs, weights, acc, coeffs_a, coeffs_b, own_b, mirror_b, turned, sched, sem) = refs[n_gy + 5 :]
    c, r = here()
    fetch = pltpu.make_async_copy(sched_v, sched, sem)
    fetch.start()
    n_half = n_gy // 2
    for k in range(n_gy):
        fabs[lax.rem(r - k + n_gy, n_gy)] = blocks[k][EDGE:, :]
    first_row = jnp.where(r < n_half, 0, n_half)
    sym, anti = [], []
    for b in range(n_half):
        near, far = fabs[first_row + b], fabs[n_gy - 1 - first_row - b]
        sym.append(near + far)
        anti.append(near - far)
    sym = jnp.concatenate(sym, axis=1)
    anti = jnp.concatenate(anti, axis=1)
    for s in range(slots):
        lo, hi = s * GROUP, (s + 1) * GROUP
        rows = jnp.concatenate(
            [sym[lo:hi], anti[lo:hi], sym[k_half + lo : k_half + hi], anti[k_half + lo : k_half + hi]],
            axis=0,
        )
        rows = rows * jnp.concatenate([unscale[s]] * 4, axis=0)
        rows_hi = rows.astype(BF16)
        lhs[s, : 4 * GROUP, :] = rows_hi
        lhs[s, 4 * GROUP :, :] = (rows - rows_hi.astype(F32)).astype(BF16)
    acc[...] = jnp.zeros(acc.shape, F32)
    lhs[slots] = jnp.zeros((8 * GROUP, half), BF16)
    fetch.wait()
    row = iota((4 * GROUP, ROWS), 0)
    lane = iota((4 * GROUP, ROWS), 1)
    i_row, i_lane, t_lane = row % GROUP, lane % GROUP, lane // GROUP
    keep = jnp.where(
        (i_row == i_lane) & ((t_lane + i_row) % 2 == (row // GROUP) % 2), 1.0, 0.0
    ).astype(F32)
    starts = 128 // GROUP
    nt = (((1,), (1,)), ((), ()))
    nn = (((1,), (0,)), ((), ()))
    n = 4 * GROUP

    def matrix(i, h, part):
        return jnp.concatenate([basis[i, h, part, k] for k in range(half // 128)], axis=1)

    def products(i, h):
        left = lhs[scheduled(plan, c, sched, i, h)[0]]
        at = (i % (2 * UNROLL)) * CHAINS + h
        turned[at, 0] = matrix(i, h, 0).T
        one = lax.dot_general(left, turned[at, 0], nn, preferred_element_type=F32)
        if i < UNROLL:
            two = lax.dot_general(left[:n], matrix(i, h, 1), nt, preferred_element_type=F32)
        else:
            turned[at, 1] = matrix(i, h, 1).T
            two = lax.dot_general(left[:n], turned[at, 1], nn, preferred_element_type=F32)
        return one[:n] + one[n:] + two

    def coefficients(i, h, total):
        _, chunk, group = scheduled(plan, c, sched, i, h)
        begin = group + chunk * (STEPS // GROUP)
        at = (begin // starts + 1) * starts - 1 - lax.rem(begin, starts)
        coeff = total * keep * weights[at]
        coeff_hi = coeff.astype(BF16)
        coeff_lo = (coeff - coeff_hi.astype(F32)).astype(BF16)
        return jnp.concatenate([coeff_hi, coeff_lo], axis=0)

    def synthesise(i, h, right):
        three = lax.dot_general(right, matrix(i, h, 0), nn, preferred_element_type=F32)
        four = lax.dot_general(right[:n], matrix(i, h, 1), nn, preferred_element_type=F32)
        return three[:n] + three[n:] + four

    def analyse_all(k, into):
        for j in range(UNROLL):
            for h in range(CHAINS):
                i = k * UNROLL + j
                into[j, h] = coefficients(i, h, products(i, h))

    def synthesise_all(k, given):
        found = []
        for j in range(UNROLL):
            for h in range(CHAINS):
                i = k * UNROLL + j
                slot = scheduled(plan, c, sched, i, h)[0]
                found.append((slot, synthesise(i, h, given[j, h])))
        for slot, part in found:
            acc[slot] += part

    stages = plan.n_iter // UNROLL
    first = [[products(j, h) for h in range(CHAINS)] for j in range(UNROLL)]
    width = plan.love_width
    padded = jnp.concatenate(
        [love[...].reshape(1, -1), jnp.zeros((1, width - plan.degrees), F32)], axis=1
    )
    shifted = pltpu.roll(
        jnp.broadcast_to(padded, (starts, width)),
        width - GROUP * (starts - 1), 1, stride=GROUP, stride_axis=0,
    )
    shifted = jnp.concatenate(
        [shifted[:, k * 128 : (k + 1) * 128] for k in range(width // 128)], axis=0
    )
    spread = iota((128, ROWS), 1) // GROUP == iota((128, ROWS), 0)
    weights[...] = dot(shifted, jnp.where(spread, 1.0, 0.0).astype(F32)).reshape(
        weights.shape
    )
    for j in range(UNROLL):
        for h in range(CHAINS):
            coeffs_a[j, h] = coefficients(j, h, first[j][h])

    trips = (stages - 1) // 2
    for k in range(trips):
        analyse_all(2 * k + 1, coeffs_b)
        synthesise_all(2 * k, coeffs_a)
        analyse_all(2 * k + 2, coeffs_a)
        synthesise_all(2 * k + 1, coeffs_b)
    if stages % 2 == 0:
        analyse_all(stages - 1, coeffs_b)
    synthesise_all(2 * trips, coeffs_a)
    if stages % 2 == 0:
        synthesise_all(stages - 1, coeffs_b)

    for s in range(slots):
        lo, hi = s * GROUP, (s + 1) * GROUP
        g = acc[s] * jnp.concatenate([unscale[s]] * 4, axis=0)
        for part in range(2):
            even = g[2 * part * GROUP : (2 * part + 1) * GROUP]
            odd = g[(2 * part + 1) * GROUP : (2 * part + 2) * GROUP]
            for b in range(n_half):
                lanes = slice(b * lat, (b + 1) * lat)
                where = slice(part * k_half + lo, part * k_half + hi)
                own_b[b, where, :] = even[:, lanes] + odd[:, lanes]
                mirror_b[b, where, :] = even[:, lanes] - odd[:, lanes]
    k_dev = plan.k_dev
    mine = r - first_row
    out[:k_dev, :] = own_b[mine]
    up = jnp.where(
        r == n_half - 1,
        mirror_b[mine][:, lat - 1 :],
        own_b[jnp.minimum(mine + 1, n_half - 1)][:, :1],
    )
    down = jnp.where(
        r == n_half, mirror_b[mine][:, :1], own_b[jnp.maximum(mine - 1, 0)][:, lat - 1 :]
    )
    lane_o = iota((k_dev, lat), 1)
    columns = jnp.where(lane_o == 0, up, jnp.where(lane_o == 1, down, 0.0))
    out[k_dev:, :] = rows_of(columns, lat)


def finish_kernel(
    plan, terms, a_own, a_fold, b_table, north_tile, south_tile, edges,
    surface_ref, depth_ref, mask, east_ref, north_ref,
    sal_out, east_out, north_out, height_out,
):
    lon, lat = plan.tile_lon, plan.tile_lat
    _, r = here()
    split = lon + EDGE
    own_trig = a_own[0:1, :] * b_table[0, :split, :] + a_own[1:2, :] * b_table[1, :split, :]
    fold_trig = a_fold[0:1, :] * b_table[0, split:, :] + a_fold[1:2, :] * b_table[1, split:, :]
    trig = jnp.concatenate([own_trig, fold_trig], axis=0)
    k_dev, n_gx = plan.k_dev, plan.n_gx
    main = jnp.concatenate([terms[d, :k_dev, :] for d in range(n_gx)], axis=0)
    sal_all = dot3(trig, main)
    up = jnp.concatenate([terms[d, k_dev : k_dev + 1, :k_dev] for d in range(n_gx)], axis=1)
    down = jnp.concatenate([terms[d, k_dev + 1 : k_dev + 2, :k_dev] for d in range(n_gx)], axis=1)
    sal_up = jnp.sum(trig[:lon] * up, axis=1, keepdims=True)
    sal_down = jnp.sum(trig[:lon] * down, axis=1, keepdims=True)
    sal = sal_all[:lon, :lat]
    sal_out[...] = sal
    is_top = r == plan.n_gy - 1
    sal_n = jnp.where(is_top, sal_all[split:, lat - 1 :], sal_up)
    sal_s = sal_down
    surface, depth = surface_ref[...], depth_ref[...]
    wet = mask[...].astype(F32)
    east, north = east_ref[...], north_ref[...]
    turned = jnp.concatenate(
        [north_tile[:EDGE, :], south_tile[:EDGE, :], edges[EDGE:, :],
         jnp.zeros((lat - 3 * EDGE, lat), F32)], axis=0,
    ).T[:lon, :]
    north_tile, south_tile = turned[:, :EDGE], turned[:, EDGE : 2 * EDGE]
    across = turned[:, 2 * EDGE : 3 * EDGE]
    surf_n = jnp.where(is_top, across[:, 2:3], north_tile[:lon, 4:5])
    depth_n = jnp.where(is_top, across[:, 0:1], north_tile[:lon, 5:6])
    wet_n = jnp.where(is_top, across[:, 1:2], north_tile[:lon, 6:7])
    pressure = surface - sal
    row = iota((lon, lat), 0)
    lane = iota((lon, lat), 1)

    def east_of(field, edge):
        return jnp.where(row == lon - 1, edge, pltpu.roll(field, lon - 1, 0))

    def north_of(field, edge):
        return jnp.where(lane == lat - 1, edge, pltpu.roll(field, lat - 1, 1))

    p_e = edges[0:1, :] - sal_all[lon : lon + 1, :lat]
    p_w = edges[3:4, :] - sal_all[lon + 1 : lon + 2, :lat]
    east_next = wet * east_of(wet, edges[2:3, :]) * (
        east - COURANT * (east_of(pressure, p_e) - pressure)
    )
    north_next = wet * north_of(wet, wet_n) * (
        north - COURANT * (north_of(pressure, surf_n - sal_n) - pressure)
    )
    east_out[...] = east_next
    north_out[...] = north_next
    east_flux = 0.5 * (depth + east_of(depth, edges[1:2, :])) * east_next
    north_flux = 0.5 * (depth + north_of(depth, depth_n)) * north_next
    west_face = edges[5:6, :] * wet[:1] * (edges[6:7, :] - COURANT * (pressure[:1] - p_w))
    west_edge = 0.5 * (edges[4:5, :] + depth[:1]) * west_face
    south_face = south_tile[:lon, 2:3] * wet[:, :1] * (
        south_tile[:lon, 3:4] - COURANT * (pressure[:, :1] - (south_tile[:lon, 0:1] - sal_s))
    )
    south_edge = 0.5 * (south_tile[:lon, 1:2] + depth[:, :1]) * south_face
    south_edge = jnp.where(r > 0, south_edge, 0.0)
    west_flux = jnp.where(row == 0, west_edge, pltpu.roll(east_flux, 1, 0))
    south_flux = jnp.where(lane == 0, south_edge, pltpu.roll(north_flux, 1, 1))
    height_out[...] = wet * (
        surface - COURANT * (east_flux - west_flux + north_flux - south_flux)
    )


VMEM = pl.BlockSpec(memory_space=pltpu.VMEM)
HBM = pl.BlockSpec(memory_space=pltpu.HBM)
SLICED_GX = (5, 10)
SLICED_GY = (7,)
SLICED_HALF = (8,)


def on_device(height, east_speed, north_speed, water_depth, ocean_mask, fold_partner, love_factor):
    lon, lat = height.shape
    n_gx, n_gy = lax.axis_size("gx"), lax.axis_size("gy")
    plan = Plan(lon, lat, n_gx, n_gy, love_factor.shape[0])
    slots, half = plan.n_slots, plan.half
    sent = lon + EDGE
    sources = (
        height, ocean_mask, water_depth, east_speed, north_speed, plan.u_table, plan.v_table,
        plan.quad, plan.geo, plan.seed_logs, plan.sched, love_factor, fold_partner,
    )
    sources = tuple(
        pltpu.with_memory_space_constraint(jnp.asarray(source), pltpu.HBM) for source in sources
    )
    kept_shapes = [
        source.shape[1:] if k in SLICED_GX + SLICED_GY + SLICED_HALF else source.shape
        for k, source in enumerate(sources)
    ]
    kept = [
        pltpu.VMEM(shape, source.dtype) for shape, source in zip(kept_shapes[1:], sources[1:])
    ]
    packed, surface, *kept = pl.pallas_call(
        lambda *refs: pack_kernel(plan, *refs),
        in_specs=[HBM] * len(sources),
        out_specs=[VMEM] * (len(sources) + 1),
        out_shape=(pltpu.VMEM((sent, lat), F32), pltpu.VMEM((lon, lat), F32), *kept),
        scratch_shapes=[pltpu.VMEM((lon, lat), F32), pltpu.SemaphoreType.DMA((len(sources),))],
        compiler_params=PARAMS,
        name="pack",
    )(*sources)
    mask, depth, east, north, u, v, quad, geo, seed_logs, sched, love, fold = kept
    gathered = lax.all_gather(packed, "gx", axis=0, tiled=False)
    rows = EDGE + plan.k_dev
    fold_scratch = [pltpu.SMEM((n_gx,), jnp.int32), pltpu.SemaphoreType.DMA]
    *messages, edges = pl.pallas_call(
        lambda *refs: fourier_kernel(plan, *refs),
        in_specs=[VMEM] * 9,
        out_specs=[VMEM] * (n_gy + 1),
        out_shape=(
            *[pltpu.VMEM((rows, lat), F32) for _ in range(n_gy)],
            pltpu.VMEM((2 * EDGE, lat), F32),
        ),
        scratch_shapes=fold_scratch,
        compiler_params=PARAMS,
        name="fourier",
    )(gathered, u, v, quad, surface, depth, mask, north, fold)
    blocks = [messages[0]]
    for k in range(1, n_gy):
        ring = [(i, (i + k) % n_gy) for i in range(n_gy)]
        blocks.append(lax.ppermute(messages[k], "gy", ring))
    sched_scratch = [pltpu.SMEM((1, plan.sched_width), jnp.int32), pltpu.SemaphoreType.DMA]
    a_table = pltpu.with_memory_space_constraint(jnp.asarray(plan.a_table), pltpu.HBM)
    basis, unscale, a_own, a_fold = pl.pallas_call(
        lambda *refs: basis_kernel(plan, *refs),
        in_specs=[VMEM] * 4 + [HBM],
        out_specs=[VMEM] * 4,
        out_shape=(
            pltpu.VMEM((plan.n_iter, CHAINS, 2, half // 128, ROWS, 128), BF16),
            pltpu.VMEM((slots + 1, GROUP, half), F32),
            pltpu.VMEM((8, plan.k_all), F32),
            pltpu.VMEM((8, plan.k_all), F32),
        ),
        scratch_shapes=[
            pltpu.VMEM((slots + 1, GROUP, half), F32),
            pltpu.VMEM((slots + 1, 2, GROUP, half), F32),
            pltpu.SMEM((1, plan.sched_width), jnp.int32),
            pltpu.SMEM((n_gx,), jnp.int32),
            pltpu.SemaphoreType.DMA((3,)),
        ],
        cost_estimate=pl.CostEstimate(flops=60_000_000, bytes_accessed=1_000_000, transcendentals=0),
        compiler_params=PARAMS,
        name="basis",
    )(sched, geo, seed_logs, fold, a_table)
    split_shape = pltpu.VMEM((n_gy // 2, plan.k_dev, lat), F32)
    terms = pl.pallas_call(
        lambda *refs: legendre_kernel(plan, *refs),
        in_specs=[VMEM] * (n_gy + 4),
        out_specs=VMEM,
        out_shape=pltpu.VMEM((plan.k_dev + EDGE, lat), F32),
        scratch_shapes=[
            pltpu.VMEM((n_gy, plan.k_dev, lat), F32),
            pltpu.VMEM((slots + 1, 8 * GROUP, half), BF16),
            pltpu.VMEM((plan.love_width // GROUP, 1, ROWS), F32),
            pltpu.VMEM((slots + 1, 4 * GROUP, half), F32),
            pltpu.VMEM((UNROLL, CHAINS, 8 * GROUP, ROWS), BF16),
            pltpu.VMEM((UNROLL, CHAINS, 8 * GROUP, ROWS), BF16),
            split_shape, split_shape,
            pltpu.VMEM((2 * UNROLL * CHAINS, 2, half, ROWS), BF16),
        ]
        + sched_scratch,
        compiler_params=PARAMS,
        name="legendre",
    )(*blocks, basis, unscale, love, sched)
    everything = lax.all_gather(terms, "gx", axis=0, tiled=False)
    tile = jax.ShapeDtypeStruct((lon, lat), F32)
    b_table = jnp.asarray(plan.b_table)
    return pl.pallas_call(
        lambda *refs: finish_kernel(plan, *refs),
        in_specs=[VMEM] * 12,
        out_specs=[VMEM] * 4,
        out_shape=(tile,) * 4,
        compiler_params=PARAMS,
        name="finish",
    )(
        everything, a_own, a_fold, b_table, blocks[n_gy - 1], blocks[1], edges,
        surface, depth, mask, east, north,
    )


def solution(mesh):
    spec = P("gx", "gy")
    return jax.shard_map(
        on_device,
        mesh=mesh,
        in_specs=(spec, spec, spec, spec, spec, P(), P()),
        out_specs=(spec,) * 4,
        check_vma=False,
    )
```

```python
import math

import numpy as np

import jax
import jax.numpy as jnp
from jax import lax
from jax.experimental import pallas as pl
from jax.experimental.pallas import tpu as pltpu
from jax.sharding import PartitionSpec as P

COURANT = 0.35
GROUP = 8
STEPS = 32
ROWS = GROUP * STEPS
CHAINS = 3
UNROLL = 2
EDGE = 8
F32 = jnp.float32
BF16 = jnp.bfloat16
HIGHEST = lax.Precision.HIGHEST
PARAMS = pltpu.CompilerParams(vmem_limit_bytes=16 * 1024 * 1024)


class Plan:
    def __init__(self, tile_lon, tile_lat, n_gx, n_gy, degrees):
        self.tile_lon, self.tile_lat = tile_lon, tile_lat
        self.n_gx, self.n_gy, self.degrees = n_gx, n_gy, degrees
        self.nlon, self.nlat = tile_lon * n_gx, tile_lat * n_gy
        self.half = self.nlat // 2
        self.n_groups = -(-degrees // GROUP)
        self.n_slots = -(-self.n_groups // n_gx)
        self.k_dev = 2 * self.n_slots * GROUP
        self.k_all = self.k_dev * n_gx
        self.group_of = np.array(
            [
                [s * n_gx + (c if s % 2 == 0 else n_gx - 1 - c) for s in range(self.n_slots)]
                for c in range(n_gx)
            ],
            np.int32,
        )
        self._schedule()
        self._tables()

    def _schedule(self):
        lists = []
        for c in range(self.n_gx):
            counts = []
            for s in range(self.n_slots):
                left = self.degrees - GROUP * int(self.group_of[c, s])
                counts.append(-(-max(left, 0) // STEPS))
            lists.append(counts)
        longest = max(-(-sum(counts) // CHAINS) for counts in lists)
        longest = max(longest, max(max(counts) for counts in lists))
        self.n_iter = -(-longest // UNROLL) * UNROLL
        per_row = self.n_iter * CHAINS * 2
        self.sched_width = -(-per_row // 128) * 128
        self.sched = np.zeros((self.n_gx, 1, self.sched_width), np.int32)
        for c, counts in enumerate(lists):
            chains, room = [[]], self.n_iter
            for s, count in enumerate(counts):
                if room >= count:
                    chains[-1] += [(s, k) for k in range(count)]
                    room -= count
                else:
                    head = count - room
                    chains[-1] += [(s, k) for k in range(head, count)]
                    chains.append([(s, k) for k in range(head)])
                    room = self.n_iter - head
            chains += [[] for _ in range(CHAINS - len(chains))]
            for h, chain in enumerate(chains):
                chain += [(self.n_slots, 0)] * (self.n_iter - len(chain))
                for i, item in enumerate(chain):
                    at = (i * CHAINS + h) * 2
                    self.sched[c, 0, at : at + 2] = item
        top = self.n_gx * (self.n_slots + 1) * GROUP
        self.love_width = -(-(max(top, self.degrees) + 2 * STEPS) // 128) * 128

    def _tables(self):
        rows = np.arange(self.nlat).reshape(2, self.half)
        theta = np.pi * (rows + 0.5) / self.nlat
        self.geo = np.zeros((2, 8, self.half), np.float32)
        self.geo[:, 0] = np.cos(theta)
        self.geo[:, 1] = np.log(np.sin(theta))
        all_theta = np.pi * (np.arange(self.nlat) + 0.5) / self.nlat
        quad = np.pi / self.nlat * (2.0 * np.pi / self.nlon) * np.sin(all_theta)
        self.quad = np.repeat(
            quad.reshape(self.n_gy, 1, self.tile_lat), 8, axis=1
        ).astype(np.float32)
        top = GROUP * (int(self.group_of.max()) + 1)
        factors = np.arange(1, top, dtype=np.float64)
        logs = np.concatenate([[0.0], np.cumsum(0.5 * np.log((2 * factors + 1) / (2 * factors)))])
        orders = self.group_of[:, :, None] * GROUP + np.arange(GROUP)[None, None, :]
        lanes = -(-self.n_gx // 128) * 128
        self.seed_logs = np.zeros((self.n_slots * GROUP, lanes), np.float32)
        self.seed_logs[:, : self.n_gx] = logs[orders].reshape(self.n_gx, -1).T
        lam = 2.0 * np.pi / self.nlon
        cols = np.arange(self.nlon)
        base = (self.group_of[:, :, None] * GROUP * cols[None, None, :]) % self.nlon
        u = np.stack([np.cos(lam * base), np.sin(lam * base)], axis=2)
        pad = -(-2 * self.n_slots // 8) * 8
        self.u_rows = pad
        self.u_table = np.zeros((self.n_gx, pad, self.nlon), np.float32)
        self.u_table[:, : 2 * self.n_slots] = u.reshape(self.n_gx, 2 * self.n_slots, self.nlon)
        small = (np.arange(GROUP)[:, None] * cols[None, :]) % self.nlon
        self.v_table = np.concatenate([np.cos(lam * small), np.sin(lam * small)]).astype(np.float32)
        m = np.concatenate(
            [np.tile(orders[c].reshape(-1), 2) for c in range(self.n_gx)]
        )
        sine = np.tile(np.repeat([0, 1], self.k_dev // 2), self.n_gx)
        nu = np.where(m == 0, 1.0, 2.0) * (m < self.degrees)
        starts = np.arange(self.n_gx) * self.tile_lon
        phase = lam * ((starts[:, None] * m[None, :]) % self.nlon)
        a1 = nu * np.where(sine == 0, np.cos(phase), np.sin(phase))
        a2 = nu * np.where(sine == 0, -np.sin(phase), np.cos(phase))
        self.a_table = np.zeros((self.n_gx, 8, self.k_all), np.float32)
        self.a_table[:, 0] = a1
        self.a_table[:, 1] = a2
        offsets = np.concatenate(
            [
                np.arange(self.tile_lon),
                [self.tile_lon, -1],
                np.zeros(EDGE - 2),
                np.arange(self.tile_lon)[::-1],
            ]
        ).astype(np.int64)
        phase = lam * ((offsets[:, None] * m[None, :]) % self.nlon)
        self.b_table = np.stack([np.cos(phase), np.sin(phase)]).astype(np.float32)
        self.o_rows = offsets.shape[0]


def iota(shape, axis):
    return lax.broadcasted_iota(jnp.int32, shape, axis)


def dot(a, b):
    return lax.dot_general(
        a, b, (((1,), (0,)), ((), ())), precision=HIGHEST, preferred_element_type=F32
    )


def dot3(a, b):
    a_hi, b_hi = a.astype(BF16), b.astype(BF16)
    a_lo = (a - a_hi.astype(F32)).astype(BF16)
    b_lo = (b - b_hi.astype(F32)).astype(BF16)
    n = a.shape[0]
    dims = (((1,), (0,)), ((), ()))
    both = jnp.concatenate([a_hi, a_lo], axis=0)
    big = lax.dot_general(both, b_hi, dims, preferred_element_type=F32)
    small = lax.dot_general(a_hi, b_lo, dims, preferred_element_type=F32)
    return big[:n] + (big[n:] + small)


def rows_of(tile, size):
    height = tile.shape[0]
    tile = jnp.concatenate([tile, jnp.zeros((size - height, size), F32)], axis=0)
    return tile.T[:EDGE, :]


def flip_matrix(size, flipped):
    row = iota((size, size), 0)
    col = iota((size, size), 1)
    target = jnp.where(flipped, size - 1 - col, col)
    return jnp.where(row == target, 1.0, 0.0).astype(F32)


def here():
    return lax.axis_index("gx"), lax.axis_index("gy")


def pack_kernel(plan, *refs):
    count = len(refs) // 2 - 1
    height, mask, depth, east = refs[:4]
    sources = refs[:count]
    out, surface_out = refs[count : count + 2]
    kept = refs[count + 2 : 2 * count + 1]
    height_v, sem = refs[2 * count + 1 :]
    c, r = here()
    targets = (height_v,) + tuple(kept)
    copies = []
    for k, (source, target) in enumerate(zip(sources, targets)):
        if k in SLICED_GX:
            source = source.at[c]
        elif k in SLICED_GY:
            source = source.at[r]
        elif k in SLICED_HALF:
            source = source.at[jnp.where(r < plan.n_gy // 2, 0, 1)]
        copies.append(pltpu.make_async_copy(source, target, sem.at[k]))
    for copy in copies:
        copy.start()
    for copy in copies[:4]:
        copy.wait()
    _, mask_v, depth_v, east_v = targets[:4]
    lon, lat = height_v.shape
    wet = mask_v[...].astype(F32)
    surface = wet * height_v[...]
    surface_out[...] = surface
    out[:lon, :] = surface
    out[lon : lon + 1, :] = depth_v[:1, :]
    out[lon + 1 : lon + 2, :] = wet[:1, :]
    out[lon + 2 : lon + 3, :] = depth_v[lon - 1 :, :]
    out[lon + 3 : lon + 4, :] = wet[lon - 1 :, :]
    out[lon + 4 : lon + 5, :] = east_v[lon - 1 :, :]
    lane = iota((lon, lat), 1)
    tile = jnp.zeros((lon, lat), F32)
    for k, array in enumerate([depth_v, wet, surface]):
        tile = jnp.where(lane == k, array[:, lat - 1 :], tile)
    out[lon + 5 :, :] = rows_of(tile, lat)[: EDGE - 5]
    for copy in copies[4:]:
        copy.wait()


def fourier_kernel(plan, *refs):
    n_gx, n_gy, slots = plan.n_gx, plan.n_gy, plan.n_slots
    tiles, refs = refs[:n_gx], refs[n_gx:]
    u, v, quad, surface, depth, mask, north, fold_v = refs[:8]
    outs, edges, gathered, fold, sem = refs[8 : 8 + n_gy], *refs[8 + n_gy :]
    lon, lat = plan.tile_lon, plan.tile_lat
    c, r = here()
    fetch = pltpu.make_async_copy(fold_v, fold, sem)
    fetch.start()
    for k in range(n_gx):
        gathered[c ^ k] = tiles[k][...]
    field = jnp.concatenate([gathered[d, :lon, :] for d in range(n_gx)], axis=0)
    vc, vs = v[:GROUP, :], v[GROUP:, :]
    cos_rows, sin_rows = [], []
    for s in range(slots):
        uc = u[2 * s : 2 * s + 1, :]
        us = u[2 * s + 1 : 2 * s + 2, :]
        cos_rows.append(uc * vc - us * vs)
        sin_rows.append(us * vc + uc * vs)
    trig = jnp.concatenate(cos_rows + sin_rows, axis=0)
    sums = dot3(trig, field) * quad[:1, :]
    flipped = dot3(sums, flip_matrix(lat, True))
    wet = mask[...].astype(F32)
    lane = iota((lon, lat), 1)
    tile = jnp.zeros((lon, lat), F32)
    for k, array in enumerate([surface, depth, wet, north]):
        tile = jnp.where(lane == k, array[:, lat - 1 :], tile)
    for k, array in enumerate([surface, depth, wet]):
        tile = jnp.where(lane == 4 + k, array[:, :1], tile)
    halo = rows_of(tile, lat)
    for k in range(n_gy):
        target = lax.rem(r + k, n_gy)
        same = (r < n_gy // 2) == (target < n_gy // 2)
        outs[k][:EDGE, :] = halo
        outs[k][EDGE:, :] = jnp.where(same, sums, flipped)
    after = lax.rem(c + 1, n_gx)
    before = lax.rem(c + n_gx - 1, n_gx)
    fetch.wait()
    partner = fold[c]
    edges[0:1, :] = gathered[after, 0:1, :]
    edges[1:3, :] = gathered[after, lon : lon + 2, :]
    edges[3:4, :] = gathered[before, lon - 1 : lon, :]
    edges[4:7, :] = gathered[before, lon + 2 : lon + 5, :]
    edges[7:8, :] = jnp.zeros((1, lat), F32)
    across = jnp.concatenate(
        [gathered[partner, lon + 5 : lon + EDGE, :], jnp.zeros((5, lat), F32)], axis=0
    )
    i, j = iota((lat, lat), 0), iota((lat, lat), 1)
    back = jnp.where((i < lon) & (i + j == lon - 1), 1.0, 0.0).astype(F32)
    edges[EDGE:, :] = dot(across, back)


def scheduled(plan, c, sched, i, h):
    at = (i * CHAINS + h) * 2
    slot, chunk = sched[0, at], sched[0, at + 1]
    even = lax.rem(slot, 2) == 0
    group = slot * plan.n_gx + jnp.where(even, c, plan.n_gx - 1 - c)
    return slot, chunk, group


def basis_kernel(
    plan, sched_v, geo, seed_logs, fold_v, a_table, p_out, unscale, a_own, a_fold,
    seeds, state, sched, fold, sem,
):
    slots, half = plan.n_slots, plan.half
    c, _ = here()
    fetch = pltpu.make_async_copy(sched_v, sched, sem.at[0])
    fetch.start()
    fetch_fold = pltpu.make_async_copy(fold_v, fold, sem.at[1])
    fetch_fold.start()
    fetch_own = pltpu.make_async_copy(a_table.at[c], a_own, sem.at[2])
    fetch_own.start()
    log_sin = geo[1:2, :]
    sub = iota((GROUP, half), 0)
    pick = iota(seed_logs.shape, 1) == c
    logs = jnp.sum(jnp.where(pick, seed_logs[...], 0.0), axis=1, keepdims=True)
    for s in range(slots):
        group = s * plan.n_gx + (c if s % 2 == 0 else plan.n_gx - 1 - c)
        order = (sub + group * GROUP).astype(F32)
        exponent = order * log_sin + logs[s * GROUP : (s + 1) * GROUP]
        shift = jnp.clip(-exponent - 80.0, 0.0, 80.0)
        seeds[s] = jnp.exp(exponent + shift) * (1.0 / math.sqrt(4.0 * math.pi))
        unscale[s] = jnp.exp(-shift)
    state[...] = jnp.zeros(state.shape, F32)
    seeds[slots] = jnp.zeros((GROUP, half), F32)
    unscale[slots] = jnp.zeros((GROUP, half), F32)
    x = jnp.broadcast_to(geo[0:1, :], (GROUP, half))
    sub_c = iota((GROUP, 128), 0)
    lane_c = iota((GROUP, 128), 1)
    fetch.wait()
    fetch_fold.wait()
    fetch_across = pltpu.make_async_copy(a_table.at[fold[c]], a_fold, sem.at[1])
    fetch_across.start()

    def coefficients(i, h):
        _, chunk, group = scheduled(plan, c, sched, i, h)
        m0 = group * GROUP
        degree = (m0 + chunk * STEPS + lane_c).astype(F32)
        order = (m0 + sub_c).astype(F32)
        below = degree - 1.0
        growth = jnp.sqrt(
            jnp.maximum(4.0 * degree * degree - 1.0, 1.0)
            / jnp.maximum(degree * degree - order * order, 1.0)
        )
        damping = jnp.sqrt(
            jnp.maximum(below * below - order * order, 0.0)
            / jnp.maximum(4.0 * below * below - 1.0, 1.0)
        )
        return growth, growth * damping

    def begin(i, h):
        slot, chunk, _ = scheduled(plan, c, sched, i, h)
        started = jnp.where(chunk == 0, 0.0, 1.0).astype(F32)
        seed = seeds[slot] * (1.0 - started)
        return slot, seed, state[slot, 0], state[slot, 1]

    def body(i, carry):
        lanes = [begin(i, h) for h in range(CHAINS)]
        ahead = [coefficients(jnp.minimum(i + 1, plan.n_iter - 1), h) for h in range(CHAINS)]
        previous = [lane[2] for lane in lanes]
        before = [lane[3] for lane in lanes]
        pairs = [[] for _ in range(CHAINS)]
        for t in range(STEPS):
            for h, (_, seed, _, _) in enumerate(lanes):
                growth, fall = carry[h]
                a = jnp.broadcast_to(growth[:, t : t + 1], (GROUP, half))
                b = jnp.broadcast_to(fall[:, t : t + 1], (GROUP, half))
                value = (a * x) * previous[h] - b * before[h]
                if t < GROUP:
                    value = value + jnp.where(sub == t, seed, 0.0)
                previous[h], before[h] = value, previous[h]
                pairs[h].append(value)
                if t % 2 == 1:
                    both = jnp.concatenate(pairs[h], axis=0)
                    both_hi = both.astype(BF16)
                    at = (t - 1) * GROUP
                    both_lo = (both - both_hi.astype(F32)).astype(BF16)
                    for k in range(half // 128):
                        lanes_k = slice(k * 128, (k + 1) * 128)
                        p_out[i, h, 0, k, at : at + 2 * GROUP, :] = both_hi[:, lanes_k]
                        p_out[i, h, 1, k, at : at + 2 * GROUP, :] = both_lo[:, lanes_k]
                    pairs[h] = []
        for h, lane in enumerate(lanes):
            state[lane[0], 0] = previous[h]
            state[lane[0], 1] = before[h]
        return tuple(ahead)

    lax.fori_loop(0, plan.n_iter, body, tuple(coefficients(0, h) for h in range(CHAINS)))
    fetch_own.wait()
    fetch_across.wait()


def legendre_kernel(plan, *refs):
    n_gy, slots, half = plan.n_gy, plan.n_slots, plan.half
    lon, lat, k_half = plan.tile_lon, plan.tile_lat, plan.k_dev // 2
    blocks = refs[:n_gy]
    basis, unscale, love, sched_v, out = refs[n_gy : n_gy + 5]
    (fabs, lhs, weights, acc, coeffs_a, coeffs_b, own_b, mirror_b, turned, sched, sem) = refs[n_gy + 5 :]
    c, r = here()
    fetch = pltpu.make_async_copy(sched_v, sched, sem)
    fetch.start()
    n_half = n_gy // 2
    for k in range(n_gy):
        fabs[lax.rem(r - k + n_gy, n_gy)] = blocks[k][EDGE:, :]
    first_row = jnp.where(r < n_half, 0, n_half)
    sym, anti = [], []
    for b in range(n_half):
        near, far = fabs[first_row + b], fabs[n_gy - 1 - first_row - b]
        sym.append(near + far)
        anti.append(near - far)
    sym = jnp.concatenate(sym, axis=1)
    anti = jnp.concatenate(anti, axis=1)
    for s in range(slots):
        lo, hi = s * GROUP, (s + 1) * GROUP
        rows = jnp.concatenate(
            [sym[lo:hi], anti[lo:hi], sym[k_half + lo : k_half + hi], anti[k_half + lo : k_half + hi]],
            axis=0,
        )
        rows = rows * jnp.concatenate([unscale[s]] * 4, axis=0)
        rows_hi = rows.astype(BF16)
        lhs[s, : 4 * GROUP, :] = rows_hi
        lhs[s, 4 * GROUP :, :] = (rows - rows_hi.astype(F32)).astype(BF16)
    acc[...] = jnp.zeros(acc.shape, F32)
    lhs[slots] = jnp.zeros((8 * GROUP, half), BF16)
    fetch.wait()
    row = iota((4 * GROUP, ROWS), 0)
    lane = iota((4 * GROUP, ROWS), 1)
    i_row, i_lane, t_lane = row % GROUP, lane % GROUP, lane // GROUP
    keep = jnp.where(
        (i_row == i_lane) & ((t_lane + i_row) % 2 == (row // GROUP) % 2), 1.0, 0.0
    ).astype(F32)
    starts = 128 // GROUP
    nt = (((1,), (1,)), ((), ()))
    nn = (((1,), (0,)), ((), ()))
    n = 4 * GROUP

    def matrix(i, h, part):
        return jnp.concatenate([basis[i, h, part, k] for k in range(half // 128)], axis=1)

    def products(i, h):
        left = lhs[scheduled(plan, c, sched, i, h)[0]]
        at = (i % (2 * UNROLL)) * CHAINS + h
        turned[at, 0] = matrix(i, h, 0).T
        one = lax.dot_general(left, turned[at, 0], nn, preferred_element_type=F32)
        if i < UNROLL:
            two = lax.dot_general(left[:n], matrix(i, h, 1), nt, preferred_element_type=F32)
        else:
            turned[at, 1] = matrix(i, h, 1).T
            two = lax.dot_general(left[:n], turned[at, 1], nn, preferred_element_type=F32)
        return one[:n] + one[n:] + two

    def coefficients(i, h, total):
        _, chunk, group = scheduled(plan, c, sched, i, h)
        begin = group + chunk * (STEPS // GROUP)
        at = (begin // starts + 1) * starts - 1 - lax.rem(begin, starts)
        coeff = total * keep * weights[at]
        coeff_hi = coeff.astype(BF16)
        coeff_lo = (coeff - coeff_hi.astype(F32)).astype(BF16)
        return jnp.concatenate([coeff_hi, coeff_lo], axis=0)

    def synthesise(i, h, right):
        three = lax.dot_general(right, matrix(i, h, 0), nn, preferred_element_type=F32)
        four = lax.dot_general(right[:n], matrix(i, h, 1), nn, preferred_element_type=F32)
        return three[:n] + three[n:] + four

    def analyse_all(k, into):
        for j in range(UNROLL):
            for h in range(CHAINS):
                i = k * UNROLL + j
                into[j, h] = coefficients(i, h, products(i, h))

    def synthesise_all(k, given):
        found = []
        for j in range(UNROLL):
            for h in range(CHAINS):
                i = k * UNROLL + j
                slot = scheduled(plan, c, sched, i, h)[0]
                found.append((slot, synthesise(i, h, given[j, h])))
        for slot, part in found:
            acc[slot] += part

    stages = plan.n_iter // UNROLL
    first = [[products(j, h) for h in range(CHAINS)] for j in range(UNROLL)]
    width = plan.love_width
    padded = jnp.concatenate(
        [love[...].reshape(1, -1), jnp.zeros((1, width - plan.degrees), F32)], axis=1
    )
    shifted = pltpu.roll(
        jnp.broadcast_to(padded, (starts, width)),
        width - GROUP * (starts - 1), 1, stride=GROUP, stride_axis=0,
    )
    shifted = jnp.concatenate(
        [shifted[:, k * 128 : (k + 1) * 128] for k in range(width // 128)], axis=0
    )
    spread = iota((128, ROWS), 1) // GROUP == iota((128, ROWS), 0)
    weights[...] = dot(shifted, jnp.where(spread, 1.0, 0.0).astype(F32)).reshape(
        weights.shape
    )
    for j in range(UNROLL):
        for h in range(CHAINS):
            coeffs_a[j, h] = coefficients(j, h, first[j][h])

    trips = (stages - 1) // 2
    for k in range(trips):
        analyse_all(2 * k + 1, coeffs_b)
        synthesise_all(2 * k, coeffs_a)
        analyse_all(2 * k + 2, coeffs_a)
        synthesise_all(2 * k + 1, coeffs_b)
    if stages % 2 == 0:
        analyse_all(stages - 1, coeffs_b)
    synthesise_all(2 * trips, coeffs_a)
    if stages % 2 == 0:
        synthesise_all(stages - 1, coeffs_b)

    for s in range(slots):
        lo, hi = s * GROUP, (s + 1) * GROUP
        g = acc[s] * jnp.concatenate([unscale[s]] * 4, axis=0)
        for part in range(2):
            even = g[2 * part * GROUP : (2 * part + 1) * GROUP]
            odd = g[(2 * part + 1) * GROUP : (2 * part + 2) * GROUP]
            for b in range(n_half):
                lanes = slice(b * lat, (b + 1) * lat)
                where = slice(part * k_half + lo, part * k_half + hi)
                own_b[b, where, :] = even[:, lanes] + odd[:, lanes]
                mirror_b[b, where, :] = even[:, lanes] - odd[:, lanes]
    k_dev = plan.k_dev
    mine = r - first_row
    out[:k_dev, :] = own_b[mine]
    up = jnp.where(
        r == n_half - 1,
        mirror_b[mine][:, lat - 1 :],
        own_b[jnp.minimum(mine + 1, n_half - 1)][:, :1],
    )
    down = jnp.where(
        r == n_half, mirror_b[mine][:, :1], own_b[jnp.maximum(mine - 1, 0)][:, lat - 1 :]
    )
    lane_o = iota((k_dev, lat), 1)
    columns = jnp.where(lane_o == 0, up, jnp.where(lane_o == 1, down, 0.0))
    out[k_dev:, :] = rows_of(columns, lat)


def finish_kernel(plan, *refs):
    n_gx = plan.n_gx
    received, refs = refs[:n_gx], refs[n_gx:]
    a_own, a_fold, b_table, north_tile, south_tile, edges, surface_ref, depth_ref = refs[:8]
    mask, east_ref, north_ref, sal_out, east_out, north_out, height_out, terms = refs[8:]
    c, r = here()
    for k in range(n_gx):
        terms[c ^ k] = received[k][...]
    lon, lat = plan.tile_lon, plan.tile_lat
    split = lon + EDGE
    own_trig = a_own[0:1, :] * b_table[0, :split, :] + a_own[1:2, :] * b_table[1, :split, :]
    fold_trig = a_fold[0:1, :] * b_table[0, split:, :] + a_fold[1:2, :] * b_table[1, split:, :]
    trig = jnp.concatenate([own_trig, fold_trig], axis=0)
    k_dev = plan.k_dev
    main = jnp.concatenate([terms[d, :k_dev, :] for d in range(n_gx)], axis=0)
    sal_all = dot3(trig, main)
    up = jnp.concatenate([terms[d, k_dev : k_dev + 1, :k_dev] for d in range(n_gx)], axis=1)
    down = jnp.concatenate([terms[d, k_dev + 1 : k_dev + 2, :k_dev] for d in range(n_gx)], axis=1)
    sal_up = jnp.sum(trig[:lon] * up, axis=1, keepdims=True)
    sal_down = jnp.sum(trig[:lon] * down, axis=1, keepdims=True)
    sal = sal_all[:lon, :lat]
    sal_out[...] = sal
    is_top = r == plan.n_gy - 1
    sal_n = jnp.where(is_top, sal_all[split:, lat - 1 :], sal_up)
    sal_s = sal_down
    surface, depth = surface_ref[...], depth_ref[...]
    wet = mask[...].astype(F32)
    east, north = east_ref[...], north_ref[...]
    turned = jnp.concatenate(
        [north_tile[:EDGE, :], south_tile[:EDGE, :], edges[EDGE:, :],
         jnp.zeros((lat - 3 * EDGE, lat), F32)], axis=0,
    ).T[:lon, :]
    north_tile, south_tile = turned[:, :EDGE], turned[:, EDGE : 2 * EDGE]
    across = turned[:, 2 * EDGE : 3 * EDGE]
    surf_n = jnp.where(is_top, across[:, 2:3], north_tile[:lon, 4:5])
    depth_n = jnp.where(is_top, across[:, 0:1], north_tile[:lon, 5:6])
    wet_n = jnp.where(is_top, across[:, 1:2], north_tile[:lon, 6:7])
    pressure = surface - sal
    row = iota((lon, lat), 0)
    lane = iota((lon, lat), 1)

    def east_of(field, edge):
        return jnp.where(row == lon - 1, edge, pltpu.roll(field, lon - 1, 0))

    def north_of(field, edge):
        return jnp.where(lane == lat - 1, edge, pltpu.roll(field, lat - 1, 1))

    p_e = edges[0:1, :] - sal_all[lon : lon + 1, :lat]
    p_w = edges[3:4, :] - sal_all[lon + 1 : lon + 2, :lat]
    east_next = wet * east_of(wet, edges[2:3, :]) * (
        east - COURANT * (east_of(pressure, p_e) - pressure)
    )
    north_next = wet * north_of(wet, wet_n) * (
        north - COURANT * (north_of(pressure, surf_n - sal_n) - pressure)
    )
    east_out[...] = east_next
    north_out[...] = north_next
    east_flux = 0.5 * (depth + east_of(depth, edges[1:2, :])) * east_next
    north_flux = 0.5 * (depth + north_of(depth, depth_n)) * north_next
    west_face = edges[5:6, :] * wet[:1] * (edges[6:7, :] - COURANT * (pressure[:1] - p_w))
    west_edge = 0.5 * (edges[4:5, :] + depth[:1]) * west_face
    south_face = south_tile[:lon, 2:3] * wet[:, :1] * (
        south_tile[:lon, 3:4] - COURANT * (pressure[:, :1] - (south_tile[:lon, 0:1] - sal_s))
    )
    south_edge = 0.5 * (south_tile[:lon, 1:2] + depth[:, :1]) * south_face
    south_edge = jnp.where(r > 0, south_edge, 0.0)
    west_flux = jnp.where(row == 0, west_edge, pltpu.roll(east_flux, 1, 0))
    south_flux = jnp.where(lane == 0, south_edge, pltpu.roll(north_flux, 1, 1))
    height_out[...] = wet * (
        surface - COURANT * (east_flux - west_flux + north_flux - south_flux)
    )


def spread_gx(x):
    size = lax.axis_size("gx")

    def swap(value, k):
        return lax.ppermute(value, "gx", [(i, i ^ k) for i in range(size)])

    parts = [x] + [None] * (size - 1)
    for k in sorted(range(2, size, 2), key=lambda k: -bin(k).count("1")):
        parts[k] = swap(x, k)
    for k in range(0, size, 2):
        parts[k + 1] = swap(parts[k], 1)
    return parts


VMEM = pl.BlockSpec(memory_space=pltpu.VMEM)
HBM = pl.BlockSpec(memory_space=pltpu.HBM)
SLICED_GX = (5, 10)
SLICED_GY = (7,)
SLICED_HALF = (8,)


def on_device(height, east_speed, north_speed, water_depth, ocean_mask, fold_partner, love_factor):
    lon, lat = height.shape
    n_gx, n_gy = lax.axis_size("gx"), lax.axis_size("gy")
    plan = Plan(lon, lat, n_gx, n_gy, love_factor.shape[0])
    slots, half = plan.n_slots, plan.half
    sent = lon + EDGE
    sources = (
        height, ocean_mask, water_depth, east_speed, north_speed, plan.u_table, plan.v_table,
        plan.quad, plan.geo, plan.seed_logs, plan.sched, love_factor, fold_partner,
    )
    sources = tuple(
        pltpu.with_memory_space_constraint(jnp.asarray(source), pltpu.HBM) for source in sources
    )
    kept_shapes = [
        source.shape[1:] if k in SLICED_GX + SLICED_GY + SLICED_HALF else source.shape
        for k, source in enumerate(sources)
    ]
    kept = [
        pltpu.VMEM(shape, source.dtype) for shape, source in zip(kept_shapes[1:], sources[1:])
    ]
    packed, surface, *kept = pl.pallas_call(
        lambda *refs: pack_kernel(plan, *refs),
        in_specs=[HBM] * len(sources),
        out_specs=[VMEM] * (len(sources) + 1),
        out_shape=(pltpu.VMEM((sent, lat), F32), pltpu.VMEM((lon, lat), F32), *kept),
        scratch_shapes=[pltpu.VMEM((lon, lat), F32), pltpu.SemaphoreType.DMA((len(sources),))],
        compiler_params=PARAMS,
        name="pack",
    )(*sources)
    mask, depth, east, north, u, v, quad, geo, seed_logs, sched, love, fold = kept
    tiles = spread_gx(packed)
    rows = EDGE + plan.k_dev
    fold_scratch = [pltpu.SMEM((n_gx,), jnp.int32), pltpu.SemaphoreType.DMA]
    *messages, edges = pl.pallas_call(
        lambda *refs: fourier_kernel(plan, *refs),
        in_specs=[VMEM] * (n_gx + 8),
        out_specs=[VMEM] * (n_gy + 1),
        out_shape=(
            *[pltpu.VMEM((rows, lat), F32) for _ in range(n_gy)],
            pltpu.VMEM((2 * EDGE, lat), F32),
        ),
        scratch_shapes=[pltpu.VMEM((n_gx, sent, lat), F32)] + fold_scratch,
        compiler_params=PARAMS,
        name="fourier",
    )(*tiles, u, v, quad, surface, depth, mask, north, fold)
    blocks = [messages[0]]
    for k in range(1, n_gy):
        ring = [(i, (i + k) % n_gy) for i in range(n_gy)]
        blocks.append(lax.ppermute(messages[k], "gy", ring))
    sched_scratch = [pltpu.SMEM((1, plan.sched_width), jnp.int32), pltpu.SemaphoreType.DMA]
    a_table = pltpu.with_memory_space_constraint(jnp.asarray(plan.a_table), pltpu.HBM)
    basis, unscale, a_own, a_fold = pl.pallas_call(
        lambda *refs: basis_kernel(plan, *refs),
        in_specs=[VMEM] * 4 + [HBM],
        out_specs=[VMEM] * 4,
        out_shape=(
            pltpu.VMEM((plan.n_iter, CHAINS, 2, half // 128, ROWS, 128), BF16),
            pltpu.VMEM((slots + 1, GROUP, half), F32),
            pltpu.VMEM((8, plan.k_all), F32),
            pltpu.VMEM((8, plan.k_all), F32),
        ),
        scratch_shapes=[
            pltpu.VMEM((slots + 1, GROUP, half), F32),
            pltpu.VMEM((slots + 1, 2, GROUP, half), F32),
            pltpu.SMEM((1, plan.sched_width), jnp.int32),
            pltpu.SMEM((n_gx,), jnp.int32),
            pltpu.SemaphoreType.DMA((3,)),
        ],
        cost_estimate=pl.CostEstimate(flops=60_000_000, bytes_accessed=1_000_000, transcendentals=0),
        compiler_params=PARAMS,
        name="basis",
    )(sched, geo, seed_logs, fold, a_table)
    split_shape = pltpu.VMEM((n_gy // 2, plan.k_dev, lat), F32)
    terms = pl.pallas_call(
        lambda *refs: legendre_kernel(plan, *refs),
        in_specs=[VMEM] * (n_gy + 4),
        out_specs=VMEM,
        out_shape=pltpu.VMEM((plan.k_dev + EDGE, lat), F32),
        scratch_shapes=[
            pltpu.VMEM((n_gy, plan.k_dev, lat), F32),
            pltpu.VMEM((slots + 1, 8 * GROUP, half), BF16),
            pltpu.VMEM((plan.love_width // GROUP, 1, ROWS), F32),
            pltpu.VMEM((slots + 1, 4 * GROUP, half), F32),
            pltpu.VMEM((UNROLL, CHAINS, 8 * GROUP, ROWS), BF16),
            pltpu.VMEM((UNROLL, CHAINS, 8 * GROUP, ROWS), BF16),
            split_shape, split_shape,
            pltpu.VMEM((2 * UNROLL * CHAINS, 2, half, ROWS), BF16),
        ]
        + sched_scratch,
        compiler_params=PARAMS,
        name="legendre",
    )(*blocks, basis, unscale, love, sched)
    everything = spread_gx(terms)
    tile = jax.ShapeDtypeStruct((lon, lat), F32)
    b_table = jnp.asarray(plan.b_table)
    return pl.pallas_call(
        lambda *refs: finish_kernel(plan, *refs),
        in_specs=[VMEM] * (n_gx + 11),
        out_specs=[VMEM] * 4,
        out_shape=(tile,) * 4,
        scratch_shapes=[pltpu.VMEM((n_gx, plan.k_dev + EDGE, lat), F32)],
        compiler_params=PARAMS,
        name="finish",
    )(
        *everything, a_own, a_fold, b_table, blocks[n_gy - 1], blocks[1], edges,
        surface, depth, mask, east, north,
    )


def solution(mesh):
    spec = P("gx", "gy")
    return jax.shard_map(
        on_device,
        mesh=mesh,
        in_specs=(spec, spec, spec, spec, spec, P(), P()),
        out_specs=(spec,) * 4,
        check_vma=False,
    )
```

```python
import math

import numpy as np

import jax
import jax.numpy as jnp
from jax import lax
from jax.experimental import pallas as pl
from jax.experimental.pallas import tpu as pltpu
from jax.sharding import PartitionSpec as P

COURANT = 0.35
GROUP = 8
STEPS = 32
ROWS = GROUP * STEPS
CHAINS = 3
UNROLL = 2
EDGE = 8
EARLY = (5, 12)
F32 = jnp.float32
BF16 = jnp.bfloat16
HIGHEST = lax.Precision.HIGHEST
PARAMS = pltpu.CompilerParams(vmem_limit_bytes=16 * 1024 * 1024)


class Plan:
    def __init__(self, tile_lon, tile_lat, n_gx, n_gy, degrees):
        self.tile_lon, self.tile_lat = tile_lon, tile_lat
        self.n_gx, self.n_gy, self.degrees = n_gx, n_gy, degrees
        self.nlon, self.nlat = tile_lon * n_gx, tile_lat * n_gy
        self.half = self.nlat // 2
        self.n_groups = -(-degrees // GROUP)
        self.n_slots = -(-self.n_groups // n_gx)
        self.k_dev = 2 * self.n_slots * GROUP
        self.k_all = self.k_dev * n_gx
        self.group_of = np.array(
            [
                [s * n_gx + (c if s % 2 == 0 else n_gx - 1 - c) for s in range(self.n_slots)]
                for c in range(n_gx)
            ],
            np.int32,
        )
        self._schedule()
        self._tables()

    def _schedule(self):
        lists = []
        for c in range(self.n_gx):
            counts = []
            for s in range(self.n_slots):
                left = self.degrees - GROUP * int(self.group_of[c, s])
                counts.append(-(-max(left, 0) // STEPS))
            lists.append(counts)
        longest = max(-(-sum(counts) // CHAINS) for counts in lists)
        longest = max(longest, max(max(counts) for counts in lists))
        self.n_iter = -(-longest // UNROLL) * UNROLL
        per_row = self.n_iter * CHAINS * 2
        self.sched_width = -(-per_row // 128) * 128
        self.n_early = self.n_iter * EARLY[0] // EARLY[1]
        self.sched = np.zeros((self.n_gx, 1, self.sched_width), np.int32)
        for c, counts in enumerate(lists):
            chains, room = [[]], self.n_iter
            for s, count in enumerate(counts):
                if room >= count:
                    chains[-1] += [(s, k) for k in range(count)]
                    room -= count
                else:
                    head = count - room
                    chains[-1] += [(s, k) for k in range(head, count)]
                    chains.append([(s, k) for k in range(head)])
                    room = self.n_iter - head
            chains += [[] for _ in range(CHAINS - len(chains))]
            for h, chain in enumerate(chains):
                chain += [(self.n_slots, 0)] * (self.n_iter - len(chain))
                for i, item in enumerate(chain):
                    at = (i * CHAINS + h) * 2
                    self.sched[c, 0, at : at + 2] = item
        top = self.n_gx * (self.n_slots + 1) * GROUP
        self.love_width = -(-(max(top, self.degrees) + 2 * STEPS) // 128) * 128

    def _tables(self):
        rows = np.arange(self.nlat).reshape(2, self.half)
        theta = np.pi * (rows + 0.5) / self.nlat
        self.geo = np.zeros((2, 8, self.half), np.float32)
        self.geo[:, 0] = np.cos(theta)
        self.geo[:, 1] = np.log(np.sin(theta))
        all_theta = np.pi * (np.arange(self.nlat) + 0.5) / self.nlat
        quad = np.pi / self.nlat * (2.0 * np.pi / self.nlon) * np.sin(all_theta)
        self.quad = np.repeat(
            quad.reshape(self.n_gy, 1, self.tile_lat), 8, axis=1
        ).astype(np.float32)
        top = GROUP * (int(self.group_of.max()) + 1)
        factors = np.arange(1, top, dtype=np.float64)
        logs = np.concatenate([[0.0], np.cumsum(0.5 * np.log((2 * factors + 1) / (2 * factors)))])
        orders = self.group_of[:, :, None] * GROUP + np.arange(GROUP)[None, None, :]
        lanes = -(-self.n_gx // 128) * 128
        self.seed_logs = np.zeros((self.n_slots * GROUP, lanes), np.float32)
        self.seed_logs[:, : self.n_gx] = logs[orders].reshape(self.n_gx, -1).T
        lam = 2.0 * np.pi / self.nlon
        cols = np.arange(self.nlon)
        base = (self.group_of[:, :, None] * GROUP * cols[None, None, :]) % self.nlon
        u = np.stack([np.cos(lam * base), np.sin(lam * base)], axis=2)
        pad = -(-2 * self.n_slots // 8) * 8
        self.u_rows = pad
        self.u_table = np.zeros((self.n_gx, pad, self.nlon), np.float32)
        self.u_table[:, : 2 * self.n_slots] = u.reshape(self.n_gx, 2 * self.n_slots, self.nlon)
        small = (np.arange(GROUP)[:, None] * cols[None, :]) % self.nlon
        self.v_table = np.concatenate([np.cos(lam * small), np.sin(lam * small)]).astype(np.float32)
        m = np.concatenate(
            [np.tile(orders[c].reshape(-1), 2) for c in range(self.n_gx)]
        )
        sine = np.tile(np.repeat([0, 1], self.k_dev // 2), self.n_gx)
        nu = np.where(m == 0, 1.0, 2.0) * (m < self.degrees)
        starts = np.arange(self.n_gx) * self.tile_lon
        phase = lam * ((starts[:, None] * m[None, :]) % self.nlon)
        a1 = nu * np.where(sine == 0, np.cos(phase), np.sin(phase))
        a2 = nu * np.where(sine == 0, -np.sin(phase), np.cos(phase))
        self.a_table = np.zeros((self.n_gx, 8, self.k_all), np.float32)
        self.a_table[:, 0] = a1
        self.a_table[:, 1] = a2
        offsets = np.concatenate(
            [
                np.arange(self.tile_lon),
                [self.tile_lon, -1],
                np.zeros(EDGE - 2),
                np.arange(self.tile_lon)[::-1],
            ]
        ).astype(np.int64)
        phase = lam * ((offsets[:, None] * m[None, :]) % self.nlon)
        self.b_table = np.stack([np.cos(phase), np.sin(phase)]).astype(np.float32)
        self.o_rows = offsets.shape[0]


def iota(shape, axis):
    return lax.broadcasted_iota(jnp.int32, shape, axis)


def dot(a, b):
    return lax.dot_general(
        a, b, (((1,), (0,)), ((), ())), precision=HIGHEST, preferred_element_type=F32
    )


def dot3(a, b):
    a_hi, b_hi = a.astype(BF16), b.astype(BF16)
    a_lo = (a - a_hi.astype(F32)).astype(BF16)
    b_lo = (b - b_hi.astype(F32)).astype(BF16)
    n = a.shape[0]
    dims = (((1,), (0,)), ((), ()))
    both = jnp.concatenate([a_hi, a_lo], axis=0)
    big = lax.dot_general(both, b_hi, dims, preferred_element_type=F32)
    small = lax.dot_general(a_hi, b_lo, dims, preferred_element_type=F32)
    return big[:n] + (big[n:] + small)


def rows_of(tile, size):
    height = tile.shape[0]
    tile = jnp.concatenate([tile, jnp.zeros((size - height, size), F32)], axis=0)
    return tile.T[:EDGE, :]


def flip_matrix(size, flipped):
    row = iota((size, size), 0)
    col = iota((size, size), 1)
    target = jnp.where(flipped, size - 1 - col, col)
    return jnp.where(row == target, 1.0, 0.0).astype(F32)


def here():
    return lax.axis_index("gx"), lax.axis_index("gy")


def pack_kernel(plan, *refs):
    count = len(refs) // 2 - 1
    height, mask, depth, east = refs[:4]
    sources = refs[:count]
    out, surface_out = refs[count : count + 2]
    kept = refs[count + 2 : 2 * count + 1]
    height_v, sem = refs[2 * count + 1 :]
    c, r = here()
    targets = (height_v,) + tuple(kept)
    copies = []
    for k, (source, target) in enumerate(zip(sources, targets)):
        if k in SLICED_GX:
            source = source.at[c]
        elif k in SLICED_GY:
            source = source.at[r]
        elif k in SLICED_HALF:
            source = source.at[jnp.where(r < plan.n_gy // 2, 0, 1)]
        copies.append(pltpu.make_async_copy(source, target, sem.at[k]))
    for copy in copies:
        copy.start()
    for copy in copies[:4]:
        copy.wait()
    _, mask_v, depth_v, east_v = targets[:4]
    lon, lat = height_v.shape
    wet = mask_v[...].astype(F32)
    surface = wet * height_v[...]
    surface_out[...] = surface
    out[:lon, :] = surface
    out[lon : lon + 1, :] = depth_v[:1, :]
    out[lon + 1 : lon + 2, :] = wet[:1, :]
    out[lon + 2 : lon + 3, :] = depth_v[lon - 1 :, :]
    out[lon + 3 : lon + 4, :] = wet[lon - 1 :, :]
    out[lon + 4 : lon + 5, :] = east_v[lon - 1 :, :]
    lane = iota((lon, lat), 1)
    tile = jnp.zeros((lon, lat), F32)
    for k, array in enumerate([depth_v, wet, surface]):
        tile = jnp.where(lane == k, array[:, lat - 1 :], tile)
    out[lon + 5 :, :] = rows_of(tile, lat)[: EDGE - 5]
    for copy in copies[4:]:
        copy.wait()


def fourier_kernel(plan, *refs):
    n_gx, n_gy, slots = plan.n_gx, plan.n_gy, plan.n_slots
    tiles, refs = refs[: n_gx // 2], refs[n_gx // 2 :]
    u, v, quad, surface, depth, mask, north, fold_v = refs[:8]
    outs, edges, gathered, fold, sem = refs[9 : 9 + n_gy], *refs[9 + n_gy :]
    lon, lat = plan.tile_lon, plan.tile_lat
    c, r = here()
    fetch = pltpu.make_async_copy(fold_v, fold, sem)
    fetch.start()
    for k in range(n_gx):
        half_rows = slice((k % 2) * (lon + EDGE), (k % 2 + 1) * (lon + EDGE))
        gathered[c ^ k] = tiles[k // 2][half_rows, :]
    field = jnp.concatenate([gathered[d, :lon, :] for d in range(n_gx)], axis=0)
    vc, vs = v[:GROUP, :], v[GROUP:, :]
    cos_rows, sin_rows = [], []
    for s in range(slots):
        uc = u[2 * s : 2 * s + 1, :]
        us = u[2 * s + 1 : 2 * s + 2, :]
        cos_rows.append(uc * vc - us * vs)
        sin_rows.append(us * vc + uc * vs)
    trig = jnp.concatenate(cos_rows + sin_rows, axis=0)
    sums = dot3(trig, field) * quad[:1, :]
    flipped = dot3(sums, flip_matrix(lat, True))
    wet = mask[...].astype(F32)
    lane = iota((lon, lat), 1)
    tile = jnp.zeros((lon, lat), F32)
    for k, array in enumerate([surface, depth, wet, north]):
        tile = jnp.where(lane == k, array[:, lat - 1 :], tile)
    for k, array in enumerate([surface, depth, wet]):
        tile = jnp.where(lane == 4 + k, array[:, :1], tile)
    halo = rows_of(tile, lat)
    for k in range(n_gy):
        target = lax.rem(r + k, n_gy)
        same = (r < n_gy // 2) == (target < n_gy // 2)
        outs[k][:EDGE, :] = halo
        outs[k][EDGE:, :] = jnp.where(same, sums, flipped)
    after = lax.rem(c + 1, n_gx)
    before = lax.rem(c + n_gx - 1, n_gx)
    fetch.wait()
    partner = fold[c]
    edges[0:1, :] = gathered[after, 0:1, :]
    edges[1:3, :] = gathered[after, lon : lon + 2, :]
    edges[3:4, :] = gathered[before, lon - 1 : lon, :]
    edges[4:7, :] = gathered[before, lon + 2 : lon + 5, :]
    edges[7:8, :] = jnp.zeros((1, lat), F32)
    across = jnp.concatenate(
        [gathered[partner, lon + 5 : lon + EDGE, :], jnp.zeros((5, lat), F32)], axis=0
    )
    i, j = iota((lat, lat), 0), iota((lat, lat), 1)
    back = jnp.where((i < lon) & (i + j == lon - 1), 1.0, 0.0).astype(F32)
    edges[EDGE:, :] = dot(across, back)


def scheduled(plan, c, sched, i, h):
    at = (i * CHAINS + h) * 2
    slot, chunk = sched[0, at], sched[0, at + 1]
    even = lax.rem(slot, 2) == 0
    group = slot * plan.n_gx + jnp.where(even, c, plan.n_gx - 1 - c)
    return slot, chunk, group


def basis_early_kernel(
    plan, sched_v, geo, seed_logs, fold_v, a_table, p_out, seeds, unscale, state, a_own, a_fold,
    sched, fold, sem,
):
    slots, half = plan.n_slots, plan.half
    c, _ = here()
    fetch = pltpu.make_async_copy(sched_v, sched, sem.at[0])
    fetch.start()
    fetch_fold = pltpu.make_async_copy(fold_v, fold, sem.at[1])
    fetch_fold.start()
    fetch_own = pltpu.make_async_copy(a_table.at[c], a_own, sem.at[2])
    fetch_own.start()
    log_sin = geo[1:2, :]
    sub = iota((GROUP, half), 0)
    pick = iota(seed_logs.shape, 1) == c
    logs = jnp.sum(jnp.where(pick, seed_logs[...], 0.0), axis=1, keepdims=True)
    for s in range(slots):
        group = s * plan.n_gx + (c if s % 2 == 0 else plan.n_gx - 1 - c)
        order = (sub + group * GROUP).astype(F32)
        exponent = order * log_sin + logs[s * GROUP : (s + 1) * GROUP]
        shift = jnp.clip(-exponent - 80.0, 0.0, 80.0)
        seeds[s] = jnp.exp(exponent + shift) * (1.0 / math.sqrt(4.0 * math.pi))
        unscale[s] = jnp.exp(-shift)
    state[...] = jnp.zeros(state.shape, F32)
    seeds[slots] = jnp.zeros((GROUP, half), F32)
    unscale[slots] = jnp.zeros((GROUP, half), F32)
    fetch.wait()
    fetch_fold.wait()
    fetch_across = pltpu.make_async_copy(a_table.at[fold[c]], a_fold, sem.at[1])
    fetch_across.start()
    recurrence(plan, c, 0, plan.n_early, sched, geo, seeds, state, p_out)
    fetch_own.wait()
    fetch_across.wait()


def basis_late_kernel(plan, sched_v, geo, seeds, state_in, _, p_out, state, sched, sem):
    c, _ = here()
    fetch = pltpu.make_async_copy(sched_v, sched, sem)
    fetch.start()
    state[...] = state_in[...]
    fetch.wait()
    recurrence(plan, c, plan.n_early, plan.n_iter, sched, geo, seeds, state, p_out)


def recurrence(plan, c, start, stop, sched, geo, seeds, state, p_out):
    slots, half = plan.n_slots, plan.half
    sub = iota((GROUP, half), 0)
    x = jnp.broadcast_to(geo[0:1, :], (GROUP, half))
    sub_c = iota((GROUP, 128), 0)
    lane_c = iota((GROUP, 128), 1)

    def coefficients(i, h):
        _, chunk, group = scheduled(plan, c, sched, i, h)
        m0 = group * GROUP
        degree = (m0 + chunk * STEPS + lane_c).astype(F32)
        order = (m0 + sub_c).astype(F32)
        below = degree - 1.0
        growth = jnp.sqrt(
            jnp.maximum(4.0 * degree * degree - 1.0, 1.0)
            / jnp.maximum(degree * degree - order * order, 1.0)
        )
        damping = jnp.sqrt(
            jnp.maximum(below * below - order * order, 0.0)
            / jnp.maximum(4.0 * below * below - 1.0, 1.0)
        )
        return growth, growth * damping

    def begin(i, h):
        slot, chunk, _ = scheduled(plan, c, sched, i, h)
        started = jnp.where(chunk == 0, 0.0, 1.0).astype(F32)
        seed = seeds[slot] * (1.0 - started)
        return slot, seed, state[slot, 0], state[slot, 1]

    def body(i, carry):
        lanes = [begin(i, h) for h in range(CHAINS)]
        ahead = [coefficients(jnp.minimum(i + 1, stop - 1), h) for h in range(CHAINS)]
        previous = [lane[2] for lane in lanes]
        before = [lane[3] for lane in lanes]
        pairs = [[] for _ in range(CHAINS)]
        for t in range(STEPS):
            for h, (_, seed, _, _) in enumerate(lanes):
                growth, fall = carry[h]
                a = jnp.broadcast_to(growth[:, t : t + 1], (GROUP, half))
                b = jnp.broadcast_to(fall[:, t : t + 1], (GROUP, half))
                value = (a * x) * previous[h] - b * before[h]
                if t < GROUP:
                    value = value + jnp.where(sub == t, seed, 0.0)
                previous[h], before[h] = value, previous[h]
                pairs[h].append(value)
                if t % 2 == 1:
                    both = jnp.concatenate(pairs[h], axis=0)
                    both_hi = both.astype(BF16)
                    at = (t - 1) * GROUP
                    both_lo = (both - both_hi.astype(F32)).astype(BF16)
                    for k in range(half // 128):
                        lanes_k = slice(k * 128, (k + 1) * 128)
                        p_out[i - start, h, 0, k, at : at + 2 * GROUP, :] = both_hi[:, lanes_k]
                        p_out[i - start, h, 1, k, at : at + 2 * GROUP, :] = both_lo[:, lanes_k]
                    pairs[h] = []
        for h, lane in enumerate(lanes):
            state[lane[0], 0] = previous[h]
            state[lane[0], 1] = before[h]
        return tuple(ahead)

    lax.fori_loop(start, stop, body, tuple(coefficients(start, h) for h in range(CHAINS)))


def legendre_kernel(plan, *refs):
    n_gy, slots, half = plan.n_gy, plan.n_slots, plan.half
    lon, lat, k_half = plan.tile_lon, plan.tile_lat, plan.k_dev // 2
    blocks = refs[:n_gy]
    early, late, unscale, love, sched_v, out = refs[n_gy : n_gy + 6]
    (fabs, lhs, weights, acc, coeffs_a, coeffs_b, own_b, mirror_b, turned, sched, sem) = refs[n_gy + 6 :]
    c, r = here()
    fetch = pltpu.make_async_copy(sched_v, sched, sem)
    fetch.start()
    n_half = n_gy // 2
    for k in range(n_gy):
        fabs[lax.rem(r - k + n_gy, n_gy)] = blocks[k][EDGE:, :]
    first_row = jnp.where(r < n_half, 0, n_half)
    sym, anti = [], []
    for b in range(n_half):
        near, far = fabs[first_row + b], fabs[n_gy - 1 - first_row - b]
        sym.append(near + far)
        anti.append(near - far)
    sym = jnp.concatenate(sym, axis=1)
    anti = jnp.concatenate(anti, axis=1)
    for s in range(slots):
        lo, hi = s * GROUP, (s + 1) * GROUP
        rows = jnp.concatenate(
            [sym[lo:hi], anti[lo:hi], sym[k_half + lo : k_half + hi], anti[k_half + lo : k_half + hi]],
            axis=0,
        )
        rows = rows * jnp.concatenate([unscale[s]] * 4, axis=0)
        rows_hi = rows.astype(BF16)
        lhs[s, : 4 * GROUP, :] = rows_hi
        lhs[s, 4 * GROUP :, :] = (rows - rows_hi.astype(F32)).astype(BF16)
    acc[...] = jnp.zeros(acc.shape, F32)
    lhs[slots] = jnp.zeros((8 * GROUP, half), BF16)
    fetch.wait()
    row = iota((4 * GROUP, ROWS), 0)
    lane = iota((4 * GROUP, ROWS), 1)
    i_row, i_lane, t_lane = row % GROUP, lane % GROUP, lane // GROUP
    keep = jnp.where(
        (i_row == i_lane) & ((t_lane + i_row) % 2 == (row // GROUP) % 2), 1.0, 0.0
    ).astype(F32)
    starts = 128 // GROUP
    nt = (((1,), (1,)), ((), ()))
    nn = (((1,), (0,)), ((), ()))
    n = 4 * GROUP

    def matrix(i, h, part):
        basis, at = (early, i) if i < plan.n_early else (late, i - plan.n_early)
        return jnp.concatenate([basis[at, h, part, k] for k in range(half // 128)], axis=1)

    def products(i, h):
        left = lhs[scheduled(plan, c, sched, i, h)[0]]
        at = (i % (2 * UNROLL)) * CHAINS + h
        turned[at, 0] = matrix(i, h, 0).T
        one = lax.dot_general(left, turned[at, 0], nn, preferred_element_type=F32)
        if i < UNROLL:
            two = lax.dot_general(left[:n], matrix(i, h, 1), nt, preferred_element_type=F32)
        else:
            turned[at, 1] = matrix(i, h, 1).T
            two = lax.dot_general(left[:n], turned[at, 1], nn, preferred_element_type=F32)
        return one[:n] + one[n:] + two

    def coefficients(i, h, total):
        _, chunk, group = scheduled(plan, c, sched, i, h)
        begin = group + chunk * (STEPS // GROUP)
        at = (begin // starts + 1) * starts - 1 - lax.rem(begin, starts)
        coeff = total * keep * weights[at]
        coeff_hi = coeff.astype(BF16)
        coeff_lo = (coeff - coeff_hi.astype(F32)).astype(BF16)
        return jnp.concatenate([coeff_hi, coeff_lo], axis=0)

    def synthesise(i, h, right):
        three = lax.dot_general(right, matrix(i, h, 0), nn, preferred_element_type=F32)
        four = lax.dot_general(right[:n], matrix(i, h, 1), nn, preferred_element_type=F32)
        return three[:n] + three[n:] + four

    def analyse_all(k, into):
        for j in range(UNROLL):
            for h in range(CHAINS):
                i = k * UNROLL + j
                into[j, h] = coefficients(i, h, products(i, h))

    def synthesise_all(k, given):
        found = []
        for j in range(UNROLL):
            for h in range(CHAINS):
                i = k * UNROLL + j
                slot = scheduled(plan, c, sched, i, h)[0]
                found.append((slot, synthesise(i, h, given[j, h])))
        for slot, part in found:
            acc[slot] += part

    stages = plan.n_iter // UNROLL
    first = [[products(j, h) for h in range(CHAINS)] for j in range(UNROLL)]
    width = plan.love_width
    padded = jnp.concatenate(
        [love[...].reshape(1, -1), jnp.zeros((1, width - plan.degrees), F32)], axis=1
    )
    shifted = pltpu.roll(
        jnp.broadcast_to(padded, (starts, width)),
        width - GROUP * (starts - 1), 1, stride=GROUP, stride_axis=0,
    )
    shifted = jnp.concatenate(
        [shifted[:, k * 128 : (k + 1) * 128] for k in range(width // 128)], axis=0
    )
    spread = iota((128, ROWS), 1) // GROUP == iota((128, ROWS), 0)
    weights[...] = dot(shifted, jnp.where(spread, 1.0, 0.0).astype(F32)).reshape(
        weights.shape
    )
    for j in range(UNROLL):
        for h in range(CHAINS):
            coeffs_a[j, h] = coefficients(j, h, first[j][h])

    trips = (stages - 1) // 2
    for k in range(trips):
        analyse_all(2 * k + 1, coeffs_b)
        synthesise_all(2 * k, coeffs_a)
        analyse_all(2 * k + 2, coeffs_a)
        synthesise_all(2 * k + 1, coeffs_b)
    if stages % 2 == 0:
        analyse_all(stages - 1, coeffs_b)
    synthesise_all(2 * trips, coeffs_a)
    if stages % 2 == 0:
        synthesise_all(stages - 1, coeffs_b)

    for s in range(slots):
        lo, hi = s * GROUP, (s + 1) * GROUP
        g = acc[s] * jnp.concatenate([unscale[s]] * 4, axis=0)
        for part in range(2):
            even = g[2 * part * GROUP : (2 * part + 1) * GROUP]
            odd = g[(2 * part + 1) * GROUP : (2 * part + 2) * GROUP]
            for b in range(n_half):
                lanes = slice(b * lat, (b + 1) * lat)
                where = slice(part * k_half + lo, part * k_half + hi)
                own_b[b, where, :] = even[:, lanes] + odd[:, lanes]
                mirror_b[b, where, :] = even[:, lanes] - odd[:, lanes]
    k_dev = plan.k_dev
    mine = r - first_row
    out[:k_dev, :] = own_b[mine]
    up = jnp.where(
        r == n_half - 1,
        mirror_b[mine][:, lat - 1 :],
        own_b[jnp.minimum(mine + 1, n_half - 1)][:, :1],
    )
    down = jnp.where(
        r == n_half, mirror_b[mine][:, :1], own_b[jnp.maximum(mine - 1, 0)][:, lat - 1 :]
    )
    lane_o = iota((k_dev, lat), 1)
    columns = jnp.where(lane_o == 0, up, jnp.where(lane_o == 1, down, 0.0))
    out[k_dev:, :] = rows_of(columns, lat)


def finish_kernel(plan, *refs):
    n_gx = plan.n_gx
    received, refs = refs[:n_gx], refs[n_gx:]
    a_own, a_fold, b_table, north_tile, south_tile, edges, surface_ref, depth_ref = refs[:8]
    mask, east_ref, north_ref, sal_out, east_out, north_out, height_out, terms = refs[8:]
    c, r = here()
    for k in range(n_gx):
        terms[c ^ k] = received[k][...]
    lon, lat = plan.tile_lon, plan.tile_lat
    split = lon + EDGE
    own_trig = a_own[0:1, :] * b_table[0, :split, :] + a_own[1:2, :] * b_table[1, :split, :]
    fold_trig = a_fold[0:1, :] * b_table[0, split:, :] + a_fold[1:2, :] * b_table[1, split:, :]
    trig = jnp.concatenate([own_trig, fold_trig], axis=0)
    k_dev = plan.k_dev
    main = jnp.concatenate([terms[d, :k_dev, :] for d in range(n_gx)], axis=0)
    sal_all = dot3(trig, main)
    up = jnp.concatenate([terms[d, k_dev : k_dev + 1, :k_dev] for d in range(n_gx)], axis=1)
    down = jnp.concatenate([terms[d, k_dev + 1 : k_dev + 2, :k_dev] for d in range(n_gx)], axis=1)
    sal_up = jnp.sum(trig[:lon] * up, axis=1, keepdims=True)
    sal_down = jnp.sum(trig[:lon] * down, axis=1, keepdims=True)
    sal = sal_all[:lon, :lat]
    sal_out[...] = sal
    is_top = r == plan.n_gy - 1
    sal_n = jnp.where(is_top, sal_all[split:, lat - 1 :], sal_up)
    sal_s = sal_down
    surface, depth = surface_ref[...], depth_ref[...]
    wet = mask[...].astype(F32)
    east, north = east_ref[...], north_ref[...]
    turned = jnp.concatenate(
        [north_tile[:EDGE, :], south_tile[:EDGE, :], edges[EDGE:, :],
         jnp.zeros((lat - 3 * EDGE, lat), F32)], axis=0,
    ).T[:lon, :]
    north_tile, south_tile = turned[:, :EDGE], turned[:, EDGE : 2 * EDGE]
    across = turned[:, 2 * EDGE : 3 * EDGE]
    surf_n = jnp.where(is_top, across[:, 2:3], north_tile[:lon, 4:5])
    depth_n = jnp.where(is_top, across[:, 0:1], north_tile[:lon, 5:6])
    wet_n = jnp.where(is_top, across[:, 1:2], north_tile[:lon, 6:7])
    pressure = surface - sal
    row = iota((lon, lat), 0)
    lane = iota((lon, lat), 1)

    def east_of(field, edge):
        return jnp.where(row == lon - 1, edge, pltpu.roll(field, lon - 1, 0))

    def north_of(field, edge):
        return jnp.where(lane == lat - 1, edge, pltpu.roll(field, lat - 1, 1))

    p_e = edges[0:1, :] - sal_all[lon : lon + 1, :lat]
    p_w = edges[3:4, :] - sal_all[lon + 1 : lon + 2, :lat]
    east_next = wet * east_of(wet, edges[2:3, :]) * (
        east - COURANT * (east_of(pressure, p_e) - pressure)
    )
    north_next = wet * north_of(wet, wet_n) * (
        north - COURANT * (north_of(pressure, surf_n - sal_n) - pressure)
    )
    east_out[...] = east_next
    north_out[...] = north_next
    east_flux = 0.5 * (depth + east_of(depth, edges[1:2, :])) * east_next
    north_flux = 0.5 * (depth + north_of(depth, depth_n)) * north_next
    west_face = edges[5:6, :] * wet[:1] * (edges[6:7, :] - COURANT * (pressure[:1] - p_w))
    west_edge = 0.5 * (edges[4:5, :] + depth[:1]) * west_face
    south_face = south_tile[:lon, 2:3] * wet[:, :1] * (
        south_tile[:lon, 3:4] - COURANT * (pressure[:, :1] - (south_tile[:lon, 0:1] - sal_s))
    )
    south_edge = 0.5 * (south_tile[:lon, 1:2] + depth[:, :1]) * south_face
    south_edge = jnp.where(r > 0, south_edge, 0.0)
    west_flux = jnp.where(row == 0, west_edge, pltpu.roll(east_flux, 1, 0))
    south_flux = jnp.where(lane == 0, south_edge, pltpu.roll(north_flux, 1, 1))
    height_out[...] = wet * (
        surface - COURANT * (east_flux - west_flux + north_flux - south_flux)
    )


def spread_gx(x):
    size = lax.axis_size("gx")

    def swap(value, k):
        return lax.ppermute(value, "gx", [(i, i ^ k) for i in range(size)])

    parts = [x] + [None] * (size - 1)
    for k in sorted(range(2, size, 2), key=lambda k: -bin(k).count("1")):
        parts[k] = swap(x, k)
    for k in range(0, size, 2):
        parts[k + 1] = swap(parts[k], 1)
    return parts


def pairs_gx(x):
    size = lax.axis_size("gx")

    def swap(value, k):
        return lax.ppermute(value, "gx", [(i, i ^ k) for i in range(size)])

    both = jnp.concatenate([x, swap(x, 1)], axis=0)
    parts = [both] + [None] * (size // 2 - 1)
    for k in sorted(range(2, size, 2), key=lambda k: -bin(k).count("1")):
        parts[k // 2] = swap(both, k)
    return parts


VMEM = pl.BlockSpec(memory_space=pltpu.VMEM)
HBM = pl.BlockSpec(memory_space=pltpu.HBM)
SLICED_GX = (5, 10)
SLICED_GY = (7,)
SLICED_HALF = (8,)


def on_device(height, east_speed, north_speed, water_depth, ocean_mask, fold_partner, love_factor):
    lon, lat = height.shape
    n_gx, n_gy = lax.axis_size("gx"), lax.axis_size("gy")
    plan = Plan(lon, lat, n_gx, n_gy, love_factor.shape[0])
    slots, half = plan.n_slots, plan.half
    sent = lon + EDGE
    sources = (
        height, ocean_mask, water_depth, east_speed, north_speed, plan.u_table, plan.v_table,
        plan.quad, plan.geo, plan.seed_logs, plan.sched, love_factor, fold_partner,
    )
    sources = tuple(
        pltpu.with_memory_space_constraint(jnp.asarray(source), pltpu.HBM) for source in sources
    )
    kept_shapes = [
        source.shape[1:] if k in SLICED_GX + SLICED_GY + SLICED_HALF else source.shape
        for k, source in enumerate(sources)
    ]
    kept = [
        pltpu.VMEM(shape, source.dtype) for shape, source in zip(kept_shapes[1:], sources[1:])
    ]
    packed, surface, *kept = pl.pallas_call(
        lambda *refs: pack_kernel(plan, *refs),
        in_specs=[HBM] * len(sources),
        out_specs=[VMEM] * (len(sources) + 1),
        out_shape=(pltpu.VMEM((sent, lat), F32), pltpu.VMEM((lon, lat), F32), *kept),
        scratch_shapes=[pltpu.VMEM((lon, lat), F32), pltpu.SemaphoreType.DMA((len(sources),))],
        compiler_params=PARAMS,
        name="pack",
    )(*sources)
    mask, depth, east, north, u, v, quad, geo, seed_logs, sched, love, fold = kept
    tiles = pairs_gx(packed)
    a_table = pltpu.with_memory_space_constraint(jnp.asarray(plan.a_table), pltpu.HBM)
    table_shape = pltpu.VMEM((slots + 1, GROUP, half), F32)
    state_shape = pltpu.VMEM((slots + 1, 2, GROUP, half), F32)

    def basis_shape(count):
        return pltpu.VMEM((count, CHAINS, 2, half // 128, ROWS, 128), BF16)

    def basis_cost(count):
        return pl.CostEstimate(
            flops=5_000_000 * count, bytes_accessed=1_000_000, transcendentals=0
        )

    n_early, n_late = plan.n_early, plan.n_iter - plan.n_early
    early, seeds, unscale, state, a_own, a_fold = pl.pallas_call(
        lambda *refs: basis_early_kernel(plan, *refs),
        in_specs=[VMEM] * 4 + [HBM],
        out_specs=[VMEM] * 6,
        out_shape=(
            basis_shape(n_early), table_shape, table_shape, state_shape,
            pltpu.VMEM((8, plan.k_all), F32),
            pltpu.VMEM((8, plan.k_all), F32),
        ),
        scratch_shapes=[
            pltpu.SMEM((1, plan.sched_width), jnp.int32),
            pltpu.SMEM((n_gx,), jnp.int32),
            pltpu.SemaphoreType.DMA((3,)),
        ],
        cost_estimate=basis_cost(n_early),
        compiler_params=PARAMS,
        name="basis_early",
    )(sched, geo, seed_logs, fold, a_table)
    rows = EDGE + plan.k_dev
    fold_scratch = [pltpu.SMEM((n_gx,), jnp.int32), pltpu.SemaphoreType.DMA]
    *messages, edges = pl.pallas_call(
        lambda *refs: fourier_kernel(plan, *refs),
        in_specs=[VMEM] * (n_gx // 2 + 9),
        out_specs=[VMEM] * (n_gy + 1),
        out_shape=(
            *[pltpu.VMEM((rows, lat), F32) for _ in range(n_gy)],
            pltpu.VMEM((2 * EDGE, lat), F32),
        ),
        scratch_shapes=[pltpu.VMEM((n_gx, sent, lat), F32)] + fold_scratch,
        compiler_params=PARAMS,
        name="fourier",
    )(*tiles, u, v, quad, surface, depth, mask, north, fold, state)
    blocks = [messages[0]]
    for k in range(1, n_gy):
        ring = [(i, (i + k) % n_gy) for i in range(n_gy)]
        blocks.append(lax.ppermute(messages[k], "gy", ring))
    sched_scratch = [pltpu.SMEM((1, plan.sched_width), jnp.int32), pltpu.SemaphoreType.DMA]
    late = pl.pallas_call(
        lambda *refs: basis_late_kernel(plan, *refs),
        in_specs=[VMEM] * 5,
        out_specs=VMEM,
        out_shape=basis_shape(n_late),
        scratch_shapes=[
            state_shape,
            pltpu.SMEM((1, plan.sched_width), jnp.int32),
            pltpu.SemaphoreType.DMA,
        ],
        cost_estimate=basis_cost(n_late),
        compiler_params=PARAMS,
        name="basis_late",
    )(sched, geo, seeds, state, edges)
    split_shape = pltpu.VMEM((n_gy // 2, plan.k_dev, lat), F32)
    terms = pl.pallas_call(
        lambda *refs: legendre_kernel(plan, *refs),
        in_specs=[VMEM] * (n_gy + 5),
        out_specs=VMEM,
        out_shape=pltpu.VMEM((plan.k_dev + EDGE, lat), F32),
        scratch_shapes=[
            pltpu.VMEM((n_gy, plan.k_dev, lat), F32),
            pltpu.VMEM((slots + 1, 8 * GROUP, half), BF16),
            pltpu.VMEM((plan.love_width // GROUP, 1, ROWS), F32),
            pltpu.VMEM((slots + 1, 4 * GROUP, half), F32),
            pltpu.VMEM((UNROLL, CHAINS, 8 * GROUP, ROWS), BF16),
            pltpu.VMEM((UNROLL, CHAINS, 8 * GROUP, ROWS), BF16),
            split_shape, split_shape,
            pltpu.VMEM((2 * UNROLL * CHAINS, 2, half, ROWS), BF16),
        ]
        + sched_scratch,
        compiler_params=PARAMS,
        name="legendre",
    )(*blocks, early, late, unscale, love, sched)
    everything = spread_gx(terms)
    tile = jax.ShapeDtypeStruct((lon, lat), F32)
    b_table = jnp.asarray(plan.b_table)
    return pl.pallas_call(
        lambda *refs: finish_kernel(plan, *refs),
        in_specs=[VMEM] * (n_gx + 11),
        out_specs=[VMEM] * 4,
        out_shape=(tile,) * 4,
        scratch_shapes=[pltpu.VMEM((n_gx, plan.k_dev + EDGE, lat), F32)],
        compiler_params=PARAMS,
        name="finish",
    )(
        *everything, a_own, a_fold, b_table, blocks[n_gy - 1], blocks[1], edges,
        surface, depth, mask, east, north,
    )


def solution(mesh):
    spec = P("gx", "gy")
    return jax.shard_map(
        on_device,
        mesh=mesh,
        in_specs=(spec, spec, spec, spec, spec, P(), P()),
        out_specs=(spec,) * 4,
        check_vma=False,
    )
```

```python
import math

import numpy as np

import jax
import jax.numpy as jnp
from jax import lax
from jax.experimental import pallas as pl
from jax.experimental.pallas import tpu as pltpu
from jax.sharding import PartitionSpec as P

COURANT = 0.35
GROUP = 8
STEPS = 32
ROWS = GROUP * STEPS
CHAINS = 3
UNROLL = 2
EDGE = 8
EARLY = (6, 12)
F32 = jnp.float32
BF16 = jnp.bfloat16
HIGHEST = lax.Precision.HIGHEST
PARAMS = pltpu.CompilerParams(vmem_limit_bytes=16 * 1024 * 1024)


class Plan:
    def __init__(self, tile_lon, tile_lat, n_gx, n_gy, degrees):
        self.tile_lon, self.tile_lat = tile_lon, tile_lat
        self.n_gx, self.n_gy, self.degrees = n_gx, n_gy, degrees
        self.nlon, self.nlat = tile_lon * n_gx, tile_lat * n_gy
        self.half = self.nlat // 2
        self.n_groups = -(-degrees // GROUP)
        self.n_slots = -(-self.n_groups // n_gx)
        self.k_dev = 2 * self.n_slots * GROUP
        self.k_all = self.k_dev * n_gx
        self.group_of = np.array(
            [
                [s * n_gx + (c if s % 2 == 0 else n_gx - 1 - c) for s in range(self.n_slots)]
                for c in range(n_gx)
            ],
            np.int32,
        )
        self._schedule()
        self._tables()

    def _schedule(self):
        lists = []
        for c in range(self.n_gx):
            counts = []
            for s in range(self.n_slots):
                left = self.degrees - GROUP * int(self.group_of[c, s])
                counts.append(-(-max(left, 0) // STEPS))
            lists.append(counts)
        longest = max(-(-sum(counts) // CHAINS) for counts in lists)
        longest = max(longest, max(max(counts) for counts in lists))
        self.n_iter = -(-longest // UNROLL) * UNROLL
        per_row = self.n_iter * CHAINS * 2
        self.sched_width = -(-per_row // 128) * 128
        self.n_early = self.n_iter * EARLY[0] // EARLY[1]
        self.sched = np.zeros((self.n_gx, 1, self.sched_width), np.int32)
        for c, counts in enumerate(lists):
            chains, room = [[]], self.n_iter
            for s, count in enumerate(counts):
                if room >= count:
                    chains[-1] += [(s, k) for k in range(count)]
                    room -= count
                else:
                    head = count - room
                    chains[-1] += [(s, k) for k in range(head, count)]
                    chains.append([(s, k) for k in range(head)])
                    room = self.n_iter - head
            chains += [[] for _ in range(CHAINS - len(chains))]
            for h, chain in enumerate(chains):
                chain += [(self.n_slots, 0)] * (self.n_iter - len(chain))
                for i, item in enumerate(chain):
                    at = (i * CHAINS + h) * 2
                    self.sched[c, 0, at : at + 2] = item
        top = self.n_gx * (self.n_slots + 1) * GROUP
        self.love_width = -(-(max(top, self.degrees) + 2 * STEPS) // 128) * 128

    def _tables(self):
        rows = np.arange(self.nlat).reshape(2, self.half)
        theta = np.pi * (rows + 0.5) / self.nlat
        self.geo = np.zeros((2, 8, self.half), np.float32)
        self.geo[:, 0] = np.cos(theta)
        self.geo[:, 1] = np.log(np.sin(theta))
        all_theta = np.pi * (np.arange(self.nlat) + 0.5) / self.nlat
        quad = np.pi / self.nlat * (2.0 * np.pi / self.nlon) * np.sin(all_theta)
        self.quad = np.repeat(
            quad.reshape(self.n_gy, 1, self.tile_lat), 8, axis=1
        ).astype(np.float32)
        top = GROUP * (int(self.group_of.max()) + 1)
        factors = np.arange(1, top, dtype=np.float64)
        logs = np.concatenate([[0.0], np.cumsum(0.5 * np.log((2 * factors + 1) / (2 * factors)))])
        orders = self.group_of[:, :, None] * GROUP + np.arange(GROUP)[None, None, :]
        lanes = -(-self.n_gx // 128) * 128
        self.seed_logs = np.zeros((self.n_slots * GROUP, lanes), np.float32)
        self.seed_logs[:, : self.n_gx] = logs[orders].reshape(self.n_gx, -1).T
        lam = 2.0 * np.pi / self.nlon
        cols = np.arange(self.nlon)
        base = (self.group_of[:, :, None] * GROUP * cols[None, None, :]) % self.nlon
        u = np.stack([np.cos(lam * base), np.sin(lam * base)], axis=2)
        pad = -(-2 * self.n_slots // 8) * 8
        self.u_rows = pad
        self.u_table = np.zeros((self.n_gx, pad, self.nlon), np.float32)
        self.u_table[:, : 2 * self.n_slots] = u.reshape(self.n_gx, 2 * self.n_slots, self.nlon)
        small = (np.arange(GROUP)[:, None] * cols[None, :]) % self.nlon
        self.v_table = np.concatenate([np.cos(lam * small), np.sin(lam * small)]).astype(np.float32)
        m = np.concatenate(
            [np.tile(orders[c].reshape(-1), 2) for c in range(self.n_gx)]
        )
        sine = np.tile(np.repeat([0, 1], self.k_dev // 2), self.n_gx)
        nu = np.where(m == 0, 1.0, 2.0) * (m < self.degrees)
        starts = np.arange(self.n_gx) * self.tile_lon
        phase = lam * ((starts[:, None] * m[None, :]) % self.nlon)
        a1 = nu * np.where(sine == 0, np.cos(phase), np.sin(phase))
        a2 = nu * np.where(sine == 0, -np.sin(phase), np.cos(phase))
        self.a_table = np.zeros((self.n_gx, 8, self.k_all), np.float32)
        self.a_table[:, 0] = a1
        self.a_table[:, 1] = a2
        offsets = np.concatenate(
            [
                np.arange(self.tile_lon),
                [self.tile_lon, -1],
                np.zeros(EDGE - 2),
                np.arange(self.tile_lon)[::-1],
            ]
        ).astype(np.int64)
        phase = lam * ((offsets[:, None] * m[None, :]) % self.nlon)
        self.b_table = np.stack([np.cos(phase), np.sin(phase)]).astype(np.float32)
        self.o_rows = offsets.shape[0]


def iota(shape, axis):
    return lax.broadcasted_iota(jnp.int32, shape, axis)


def dot(a, b):
    return lax.dot_general(
        a, b, (((1,), (0,)), ((), ())), precision=HIGHEST, preferred_element_type=F32
    )


def dot3(a, b):
    a_hi, b_hi = a.astype(BF16), b.astype(BF16)
    a_lo = (a - a_hi.astype(F32)).astype(BF16)
    b_lo = (b - b_hi.astype(F32)).astype(BF16)
    n = a.shape[0]
    dims = (((1,), (0,)), ((), ()))
    both = jnp.concatenate([a_hi, a_lo], axis=0)
    big = lax.dot_general(both, b_hi, dims, preferred_element_type=F32)
    small = lax.dot_general(a_hi, b_lo, dims, preferred_element_type=F32)
    return big[:n] + (big[n:] + small)


def rows_of(columns, size):
    height = columns[0].shape[0]
    diagonal = iota((height, size), 0) == iota((height, size), 1)
    rows = [jnp.sum(jnp.where(diagonal, x, 0.0), axis=0, keepdims=True) for x in columns]
    rows.append(jnp.zeros((EDGE - len(columns), size), F32))
    return jnp.concatenate(rows, axis=0)


def flip_matrix(size, flipped):
    row = iota((size, size), 0)
    col = iota((size, size), 1)
    target = jnp.where(flipped, size - 1 - col, col)
    return jnp.where(row == target, 1.0, 0.0).astype(F32)


def here():
    return lax.axis_index("gx"), lax.axis_index("gy")


def pack_kernel(plan, *refs):
    count = len(refs) // 2 - 1
    height, mask, depth, east = refs[:4]
    sources = refs[:count]
    out, surface_out = refs[count : count + 2]
    kept = refs[count + 2 : 2 * count + 1]
    height_v, sem = refs[2 * count + 1 :]
    c, r = here()
    targets = (height_v,) + tuple(kept)
    copies = []
    for k, (source, target) in enumerate(zip(sources, targets)):
        if k in SLICED_GX:
            source = source.at[c]
        elif k in SLICED_GY:
            source = source.at[r]
        elif k in SLICED_HALF:
            source = source.at[jnp.where(r < plan.n_gy // 2, 0, 1)]
        copies.append(pltpu.make_async_copy(source, target, sem.at[k]))
    for copy in copies:
        copy.start()
    for copy in copies[:4]:
        copy.wait()
    _, mask_v, depth_v, east_v = targets[:4]
    lon, lat = height_v.shape
    wet = mask_v[...].astype(F32)
    surface = wet * height_v[...]
    surface_out[...] = surface
    out[:lon, :] = surface
    out[lon : lon + 1, :] = depth_v[:1, :]
    out[lon + 1 : lon + 2, :] = wet[:1, :]
    out[lon + 2 : lon + 3, :] = depth_v[lon - 1 :, :]
    out[lon + 3 : lon + 4, :] = wet[lon - 1 :, :]
    out[lon + 4 : lon + 5, :] = east_v[lon - 1 :, :]
    columns = [array[:, lat - 1 :] for array in (depth_v, wet, surface)]
    out[lon + 5 :, :] = rows_of(columns, lat)[: EDGE - 5]
    for copy in copies[4:]:
        copy.wait()


def fourier_kernel(plan, *refs):
    n_gx, n_gy, slots = plan.n_gx, plan.n_gy, plan.n_slots
    tiles, refs = refs[: n_gx // 2], refs[n_gx // 2 :]
    u, v, quad, surface, depth, mask, north, fold_v = refs[:8]
    outs, edges, gathered, fold, sem = refs[9 : 9 + n_gy], *refs[9 + n_gy :]
    lon, lat = plan.tile_lon, plan.tile_lat
    c, r = here()
    fetch = pltpu.make_async_copy(fold_v, fold, sem)
    fetch.start()
    for k in range(n_gx):
        half_rows = slice((k % 2) * (lon + EDGE), (k % 2 + 1) * (lon + EDGE))
        gathered[c ^ k] = tiles[k // 2][half_rows, :]
    field = jnp.concatenate([gathered[d, :lon, :] for d in range(n_gx)], axis=0)
    vc, vs = v[:GROUP, :], v[GROUP:, :]
    cos_rows, sin_rows = [], []
    for s in range(slots):
        uc = u[2 * s : 2 * s + 1, :]
        us = u[2 * s + 1 : 2 * s + 2, :]
        cos_rows.append(uc * vc - us * vs)
        sin_rows.append(us * vc + uc * vs)
    trig = jnp.concatenate(cos_rows + sin_rows, axis=0)
    sums = dot3(trig, field) * quad[:1, :]
    flipped = dot3(sums, flip_matrix(lat, True))
    wet = mask[...].astype(F32)
    columns = [array[:, lat - 1 :] for array in (surface, depth, wet, north)]
    columns += [array[:, :1] for array in (surface, depth, wet)]
    halo = rows_of(columns, lat)
    for k in range(n_gy):
        target = lax.rem(r + k, n_gy)
        same = (r < n_gy // 2) == (target < n_gy // 2)
        outs[k][:EDGE, :] = halo
        outs[k][EDGE:, :] = jnp.where(same, sums, flipped)
    after = lax.rem(c + 1, n_gx)
    before = lax.rem(c + n_gx - 1, n_gx)
    fetch.wait()
    partner = fold[c]
    edges[0:1, :] = gathered[after, 0:1, :]
    edges[1:3, :] = gathered[after, lon : lon + 2, :]
    edges[3:4, :] = gathered[before, lon - 1 : lon, :]
    edges[4:7, :] = gathered[before, lon + 2 : lon + 5, :]
    edges[7:8, :] = jnp.zeros((1, lat), F32)
    edges[EDGE : EDGE + 3, :] = gathered[partner, lon + 5 : lon + EDGE, :]
    edges[EDGE + 3 :, :] = jnp.zeros((EDGE - 3, lat), F32)


def scheduled(plan, c, sched, i, h):
    at = (i * CHAINS + h) * 2
    slot, chunk = sched[0, at], sched[0, at + 1]
    even = lax.rem(slot, 2) == 0
    group = slot * plan.n_gx + jnp.where(even, c, plan.n_gx - 1 - c)
    return slot, chunk, group


def basis_early_kernel(
    plan, sched_v, geo, seed_logs, fold_v, a_table, p_out, seeds, unscale, state, a_own, a_fold,
    sched, fold, sem,
):
    slots, half = plan.n_slots, plan.half
    c, _ = here()
    fetch = pltpu.make_async_copy(sched_v, sched, sem.at[0])
    fetch.start()
    fetch_fold = pltpu.make_async_copy(fold_v, fold, sem.at[1])
    fetch_fold.start()
    fetch_own = pltpu.make_async_copy(a_table.at[c], a_own, sem.at[2])
    fetch_own.start()
    log_sin = geo[1:2, :]
    sub = iota((GROUP, half), 0)
    pick = iota(seed_logs.shape, 1) == c
    logs = jnp.sum(jnp.where(pick, seed_logs[...], 0.0), axis=1, keepdims=True)
    for s in range(slots):
        group = s * plan.n_gx + (c if s % 2 == 0 else plan.n_gx - 1 - c)
        order = (sub + group * GROUP).astype(F32)
        exponent = order * log_sin + logs[s * GROUP : (s + 1) * GROUP]
        shift = jnp.clip(-exponent - 80.0, 0.0, 80.0)
        seeds[s] = jnp.exp(exponent + shift) * (1.0 / math.sqrt(4.0 * math.pi))
        unscale[s] = jnp.exp(-shift)
    state[...] = jnp.zeros(state.shape, F32)
    seeds[slots] = jnp.zeros((GROUP, half), F32)
    unscale[slots] = jnp.zeros((GROUP, half), F32)
    fetch.wait()
    fetch_fold.wait()
    fetch_across = pltpu.make_async_copy(a_table.at[fold[c]], a_fold, sem.at[1])
    fetch_across.start()
    recurrence(plan, c, 0, plan.n_early, sched, geo, seeds, state, p_out)
    fetch_own.wait()
    fetch_across.wait()


def basis_late_kernel(plan, sched_v, geo, seeds, state_in, _, p_out, state, sched, sem):
    c, _ = here()
    fetch = pltpu.make_async_copy(sched_v, sched, sem)
    fetch.start()
    state[...] = state_in[...]
    fetch.wait()
    recurrence(plan, c, plan.n_early, plan.n_iter, sched, geo, seeds, state, p_out)


def recurrence(plan, c, start, stop, sched, geo, seeds, state, p_out):
    slots, half = plan.n_slots, plan.half
    sub = iota((GROUP, half), 0)
    x = jnp.broadcast_to(geo[0:1, :], (GROUP, half))
    sub_c = iota((GROUP, 128), 0)
    lane_c = iota((GROUP, 128), 1)

    def coefficients(i, h):
        _, chunk, group = scheduled(plan, c, sched, i, h)
        m0 = group * GROUP
        degree = (m0 + chunk * STEPS + lane_c).astype(F32)
        order = (m0 + sub_c).astype(F32)
        below = degree - 1.0
        growth = jnp.sqrt(
            jnp.maximum(4.0 * degree * degree - 1.0, 1.0)
            / jnp.maximum(degree * degree - order * order, 1.0)
        )
        damping = jnp.sqrt(
            jnp.maximum(below * below - order * order, 0.0)
            / jnp.maximum(4.0 * below * below - 1.0, 1.0)
        )
        return growth, growth * damping

    def begin(i, h):
        slot, chunk, _ = scheduled(plan, c, sched, i, h)
        started = jnp.where(chunk == 0, 0.0, 1.0).astype(F32)
        seed = seeds[slot] * (1.0 - started)
        return slot, seed, state[slot, 0], state[slot, 1]

    def body(i, carry):
        lanes = [begin(i, h) for h in range(CHAINS)]
        ahead = [coefficients(jnp.minimum(i + 1, stop - 1), h) for h in range(CHAINS)]
        previous = [lane[2] for lane in lanes]
        before = [lane[3] for lane in lanes]
        pairs = [[] for _ in range(CHAINS)]
        for t in range(STEPS):
            for h, (_, seed, _, _) in enumerate(lanes):
                growth, fall = carry[h]
                a = jnp.broadcast_to(growth[:, t : t + 1], (GROUP, half))
                b = jnp.broadcast_to(fall[:, t : t + 1], (GROUP, half))
                value = (a * x) * previous[h] - b * before[h]
                if t < GROUP:
                    value = value + jnp.where(sub == t, seed, 0.0)
                previous[h], before[h] = value, previous[h]
                pairs[h].append(value)
                if t % 2 == 1:
                    both = jnp.concatenate(pairs[h], axis=0)
                    both_hi = both.astype(BF16)
                    at = (t - 1) * GROUP
                    both_lo = (both - both_hi.astype(F32)).astype(BF16)
                    for k in range(half // 128):
                        lanes_k = slice(k * 128, (k + 1) * 128)
                        p_out[i - start, h, 0, k, at : at + 2 * GROUP, :] = both_hi[:, lanes_k]
                        p_out[i - start, h, 1, k, at : at + 2 * GROUP, :] = both_lo[:, lanes_k]
                    pairs[h] = []
        for h, lane in enumerate(lanes):
            state[lane[0], 0] = previous[h]
            state[lane[0], 1] = before[h]
        return tuple(ahead)

    lax.fori_loop(start, stop, body, tuple(coefficients(start, h) for h in range(CHAINS)))


def legendre_kernel(plan, *refs):
    n_gy, slots, half = plan.n_gy, plan.n_slots, plan.half
    lon, lat, k_half = plan.tile_lon, plan.tile_lat, plan.k_dev // 2
    blocks = refs[:n_gy]
    early, late, unscale, love, sched_v, out = refs[n_gy : n_gy + 6]
    (fabs, lhs, weights, acc, coeffs_a, coeffs_b, own_b, mirror_b, turned, sched, sem) = refs[n_gy + 6 :]
    c, r = here()
    fetch = pltpu.make_async_copy(sched_v, sched, sem)
    fetch.start()
    n_half = n_gy // 2
    for k in range(n_gy):
        fabs[lax.rem(r - k + n_gy, n_gy)] = blocks[k][EDGE:, :]
    first_row = jnp.where(r < n_half, 0, n_half)
    sym, anti = [], []
    for b in range(n_half):
        near, far = fabs[first_row + b], fabs[n_gy - 1 - first_row - b]
        sym.append(near + far)
        anti.append(near - far)
    sym = jnp.concatenate(sym, axis=1)
    anti = jnp.concatenate(anti, axis=1)
    for s in range(slots):
        lo, hi = s * GROUP, (s + 1) * GROUP
        rows = jnp.concatenate(
            [sym[lo:hi], anti[lo:hi], sym[k_half + lo : k_half + hi], anti[k_half + lo : k_half + hi]],
            axis=0,
        )
        rows = rows * jnp.concatenate([unscale[s]] * 4, axis=0)
        rows_hi = rows.astype(BF16)
        lhs[s, : 4 * GROUP, :] = rows_hi
        lhs[s, 4 * GROUP :, :] = (rows - rows_hi.astype(F32)).astype(BF16)
    acc[...] = jnp.zeros(acc.shape, F32)
    lhs[slots] = jnp.zeros((8 * GROUP, half), BF16)
    fetch.wait()
    row = iota((4 * GROUP, ROWS), 0)
    lane = iota((4 * GROUP, ROWS), 1)
    i_row, i_lane, t_lane = row % GROUP, lane % GROUP, lane // GROUP
    keep = jnp.where(
        (i_row == i_lane) & ((t_lane + i_row) % 2 == (row // GROUP) % 2), 1.0, 0.0
    ).astype(F32)
    starts = 128 // GROUP
    nt = (((1,), (1,)), ((), ()))
    nn = (((1,), (0,)), ((), ()))
    n = 4 * GROUP

    def matrix(i, h, part):
        basis, at = (early, i) if i < plan.n_early else (late, i - plan.n_early)
        return jnp.concatenate([basis[at, h, part, k] for k in range(half // 128)], axis=1)

    def products(i, h):
        left = lhs[scheduled(plan, c, sched, i, h)[0]]
        at = (i % (2 * UNROLL)) * CHAINS + h
        turned[at, 0] = matrix(i, h, 0).T
        one = lax.dot_general(left, turned[at, 0], nn, preferred_element_type=F32)
        if i < UNROLL:
            two = lax.dot_general(left[:n], matrix(i, h, 1), nt, preferred_element_type=F32)
        else:
            turned[at, 1] = matrix(i, h, 1).T
            two = lax.dot_general(left[:n], turned[at, 1], nn, preferred_element_type=F32)
        return one[:n] + one[n:] + two

    def coefficients(i, h, total):
        _, chunk, group = scheduled(plan, c, sched, i, h)
        begin = group + chunk * (STEPS // GROUP)
        at = (begin // starts + 1) * starts - 1 - lax.rem(begin, starts)
        coeff = total * keep * weights[at]
        coeff_hi = coeff.astype(BF16)
        coeff_lo = (coeff - coeff_hi.astype(F32)).astype(BF16)
        return jnp.concatenate([coeff_hi, coeff_lo], axis=0)

    def synthesise(i, h, right):
        three = lax.dot_general(right, matrix(i, h, 0), nn, preferred_element_type=F32)
        four = lax.dot_general(right[:n], matrix(i, h, 1), nn, preferred_element_type=F32)
        return three[:n] + three[n:] + four

    def analyse_all(k, into):
        for j in range(UNROLL):
            for h in range(CHAINS):
                i = k * UNROLL + j
                into[j, h] = coefficients(i, h, products(i, h))

    def synthesise_all(k, given):
        found = []
        for j in range(UNROLL):
            for h in range(CHAINS):
                i = k * UNROLL + j
                slot = scheduled(plan, c, sched, i, h)[0]
                found.append((slot, synthesise(i, h, given[j, h])))
        for slot, part in found:
            acc[slot] += part

    stages = plan.n_iter // UNROLL
    first = [[products(j, h) for h in range(CHAINS)] for j in range(UNROLL)]
    width = plan.love_width
    padded = jnp.concatenate(
        [love[...].reshape(1, -1), jnp.zeros((1, width - plan.degrees), F32)], axis=1
    )
    shifted = pltpu.roll(
        jnp.broadcast_to(padded, (starts, width)),
        width - GROUP * (starts - 1), 1, stride=GROUP, stride_axis=0,
    )
    shifted = jnp.concatenate(
        [shifted[:, k * 128 : (k + 1) * 128] for k in range(width // 128)], axis=0
    )
    spread = iota((128, ROWS), 1) // GROUP == iota((128, ROWS), 0)
    weights[...] = dot(shifted, jnp.where(spread, 1.0, 0.0).astype(F32)).reshape(
        weights.shape
    )
    for j in range(UNROLL):
        for h in range(CHAINS):
            coeffs_a[j, h] = coefficients(j, h, first[j][h])

    trips = (stages - 1) // 2
    for k in range(trips):
        analyse_all(2 * k + 1, coeffs_b)
        synthesise_all(2 * k, coeffs_a)
        analyse_all(2 * k + 2, coeffs_a)
        synthesise_all(2 * k + 1, coeffs_b)
    if stages % 2 == 0:
        analyse_all(stages - 1, coeffs_b)
    synthesise_all(2 * trips, coeffs_a)
    if stages % 2 == 0:
        synthesise_all(stages - 1, coeffs_b)

    for s in range(slots):
        lo, hi = s * GROUP, (s + 1) * GROUP
        g = acc[s] * jnp.concatenate([unscale[s]] * 4, axis=0)
        for part in range(2):
            even = g[2 * part * GROUP : (2 * part + 1) * GROUP]
            odd = g[(2 * part + 1) * GROUP : (2 * part + 2) * GROUP]
            for b in range(n_half):
                lanes = slice(b * lat, (b + 1) * lat)
                where = slice(part * k_half + lo, part * k_half + hi)
                own_b[b, where, :] = even[:, lanes] + odd[:, lanes]
                mirror_b[b, where, :] = even[:, lanes] - odd[:, lanes]
    k_dev = plan.k_dev
    mine = r - first_row
    out[:k_dev, :] = own_b[mine]
    up = jnp.where(
        r == n_half - 1,
        mirror_b[mine][:, lat - 1 :],
        own_b[jnp.minimum(mine + 1, n_half - 1)][:, :1],
    )
    down = jnp.where(
        r == n_half, mirror_b[mine][:, :1], own_b[jnp.maximum(mine - 1, 0)][:, lat - 1 :]
    )
    out[k_dev:, :] = rows_of([up, down], lat)


def finish_kernel(plan, *refs):
    n_gx = plan.n_gx
    received, refs = refs[:n_gx], refs[n_gx:]
    a_own, a_fold, b_table, north_tile, south_tile, edges, surface_ref, depth_ref = refs[:8]
    mask, east_ref, north_ref, sal_out, east_out, north_out, height_out, terms = refs[8:]
    c, r = here()
    for k in range(n_gx):
        terms[c ^ k] = received[k][...]
    lon, lat = plan.tile_lon, plan.tile_lat
    split = lon + EDGE
    own_trig = a_own[0:1, :] * b_table[0, :split, :] + a_own[1:2, :] * b_table[1, :split, :]
    fold_trig = a_fold[0:1, :] * b_table[0, split:, :] + a_fold[1:2, :] * b_table[1, split:, :]
    trig = jnp.concatenate([own_trig, fold_trig], axis=0)
    k_dev = plan.k_dev
    main = jnp.concatenate([terms[d, :k_dev, :] for d in range(n_gx)], axis=0)
    sal_all = dot3(trig, main)
    up = jnp.concatenate([terms[d, k_dev : k_dev + 1, :k_dev] for d in range(n_gx)], axis=1)
    down = jnp.concatenate([terms[d, k_dev + 1 : k_dev + 2, :k_dev] for d in range(n_gx)], axis=1)
    sal_up = jnp.sum(trig[:lon] * up, axis=1, keepdims=True)
    sal_down = jnp.sum(trig[:lon] * down, axis=1, keepdims=True)
    sal = sal_all[:lon, :lat]
    sal_out[...] = sal
    is_top = r == plan.n_gy - 1
    sal_n = jnp.where(is_top, sal_all[split:, lat - 1 :], sal_up)
    sal_s = sal_down
    surface, depth = surface_ref[...], depth_ref[...]
    wet = mask[...].astype(F32)
    east, north = east_ref[...], north_ref[...]
    i, j = iota((lon, lat), 0), iota((lon, lat), 1)

    def column(row, picked):
        return jnp.sum(jnp.where(picked, row, 0.0), axis=1, keepdims=True)

    def beside(tile, k):
        return column(tile[k : k + 1, :], i == j)

    def fold_value(k):
        return column(edges[EDGE + k : EDGE + k + 1, :], i + j == lon - 1)

    surf_n = jnp.where(is_top, fold_value(2), beside(north_tile, 4))
    depth_n = jnp.where(is_top, fold_value(0), beside(north_tile, 5))
    wet_n = jnp.where(is_top, fold_value(1), beside(north_tile, 6))
    pressure = surface - sal
    row = iota((lon, lat), 0)
    lane = iota((lon, lat), 1)

    def east_of(field, edge):
        return jnp.where(row == lon - 1, edge, pltpu.roll(field, lon - 1, 0))

    def north_of(field, edge):
        return jnp.where(lane == lat - 1, edge, pltpu.roll(field, lat - 1, 1))

    p_e = edges[0:1, :] - sal_all[lon : lon + 1, :lat]
    p_w = edges[3:4, :] - sal_all[lon + 1 : lon + 2, :lat]
    east_next = wet * east_of(wet, edges[2:3, :]) * (
        east - COURANT * (east_of(pressure, p_e) - pressure)
    )
    north_next = wet * north_of(wet, wet_n) * (
        north - COURANT * (north_of(pressure, surf_n - sal_n) - pressure)
    )
    east_out[...] = east_next
    north_out[...] = north_next
    east_flux = 0.5 * (depth + east_of(depth, edges[1:2, :])) * east_next
    north_flux = 0.5 * (depth + north_of(depth, depth_n)) * north_next
    west_face = edges[5:6, :] * wet[:1] * (edges[6:7, :] - COURANT * (pressure[:1] - p_w))
    west_edge = 0.5 * (edges[4:5, :] + depth[:1]) * west_face
    south_face = beside(south_tile, 2) * wet[:, :1] * (
        beside(south_tile, 3) - COURANT * (pressure[:, :1] - (beside(south_tile, 0) - sal_s))
    )
    south_edge = 0.5 * (beside(south_tile, 1) + depth[:, :1]) * south_face
    south_edge = jnp.where(r > 0, south_edge, 0.0)
    west_flux = jnp.where(row == 0, west_edge, pltpu.roll(east_flux, 1, 0))
    south_flux = jnp.where(lane == 0, south_edge, pltpu.roll(north_flux, 1, 1))
    height_out[...] = wet * (
        surface - COURANT * (east_flux - west_flux + north_flux - south_flux)
    )


def spread_gx(x):
    size = lax.axis_size("gx")

    def swap(value, k):
        return lax.ppermute(value, "gx", [(i, i ^ k) for i in range(size)])

    parts = [x] + [None] * (size - 1)
    for k in sorted(range(2, size, 2), key=lambda k: -bin(k).count("1")):
        parts[k] = swap(x, k)
    for k in range(0, size, 2):
        parts[k + 1] = swap(parts[k], 1)
    return parts


def pairs_gx(x):
    size = lax.axis_size("gx")

    def swap(value, k):
        return lax.ppermute(value, "gx", [(i, i ^ k) for i in range(size)])

    both = jnp.concatenate([x, swap(x, 1)], axis=0)
    parts = [both] + [None] * (size // 2 - 1)
    for k in sorted(range(2, size, 2), key=lambda k: -bin(k).count("1")):
        parts[k // 2] = swap(both, k)
    return parts


VMEM = pl.BlockSpec(memory_space=pltpu.VMEM)
HBM = pl.BlockSpec(memory_space=pltpu.HBM)
SLICED_GX = (5, 10)
SLICED_GY = (7,)
SLICED_HALF = (8,)


def on_device(height, east_speed, north_speed, water_depth, ocean_mask, fold_partner, love_factor):
    lon, lat = height.shape
    n_gx, n_gy = lax.axis_size("gx"), lax.axis_size("gy")
    plan = Plan(lon, lat, n_gx, n_gy, love_factor.shape[0])
    slots, half = plan.n_slots, plan.half
    sent = lon + EDGE
    sources = (
        height, ocean_mask, water_depth, east_speed, north_speed, plan.u_table, plan.v_table,
        plan.quad, plan.geo, plan.seed_logs, plan.sched, love_factor, fold_partner,
    )
    sources = tuple(
        pltpu.with_memory_space_constraint(jnp.asarray(source), pltpu.HBM) for source in sources
    )
    kept_shapes = [
        source.shape[1:] if k in SLICED_GX + SLICED_GY + SLICED_HALF else source.shape
        for k, source in enumerate(sources)
    ]
    kept = [
        pltpu.VMEM(shape, source.dtype) for shape, source in zip(kept_shapes[1:], sources[1:])
    ]
    packed, surface, *kept = pl.pallas_call(
        lambda *refs: pack_kernel(plan, *refs),
        in_specs=[HBM] * len(sources),
        out_specs=[VMEM] * (len(sources) + 1),
        out_shape=(pltpu.VMEM((sent, lat), F32), pltpu.VMEM((lon, lat), F32), *kept),
        scratch_shapes=[pltpu.VMEM((lon, lat), F32), pltpu.SemaphoreType.DMA((len(sources),))],
        compiler_params=PARAMS,
        name="pack",
    )(*sources)
    mask, depth, east, north, u, v, quad, geo, seed_logs, sched, love, fold = kept
    tiles = pairs_gx(packed)
    a_table = pltpu.with_memory_space_constraint(jnp.asarray(plan.a_table), pltpu.HBM)
    table_shape = pltpu.VMEM((slots + 1, GROUP, half), F32)
    state_shape = pltpu.VMEM((slots + 1, 2, GROUP, half), F32)

    def basis_shape(count):
        return pltpu.VMEM((count, CHAINS, 2, half // 128, ROWS, 128), BF16)

    def basis_cost(count):
        return pl.CostEstimate(
            flops=5_000_000 * count, bytes_accessed=1_000_000, transcendentals=0
        )

    n_early, n_late = plan.n_early, plan.n_iter - plan.n_early
    early, seeds, unscale, state, a_own, a_fold = pl.pallas_call(
        lambda *refs: basis_early_kernel(plan, *refs),
        in_specs=[VMEM] * 4 + [HBM],
        out_specs=[VMEM] * 6,
        out_shape=(
            basis_shape(n_early), table_shape, table_shape, state_shape,
            pltpu.VMEM((8, plan.k_all), F32),
            pltpu.VMEM((8, plan.k_all), F32),
        ),
        scratch_shapes=[
            pltpu.SMEM((1, plan.sched_width), jnp.int32),
            pltpu.SMEM((n_gx,), jnp.int32),
            pltpu.SemaphoreType.DMA((3,)),
        ],
        cost_estimate=basis_cost(n_early),
        compiler_params=PARAMS,
        name="basis_early",
    )(sched, geo, seed_logs, fold, a_table)
    rows = EDGE + plan.k_dev
    fold_scratch = [pltpu.SMEM((n_gx,), jnp.int32), pltpu.SemaphoreType.DMA]
    *messages, edges = pl.pallas_call(
        lambda *refs: fourier_kernel(plan, *refs),
        in_specs=[VMEM] * (n_gx // 2 + 9),
        out_specs=[VMEM] * (n_gy + 1),
        out_shape=(
            *[pltpu.VMEM((rows, lat), F32) for _ in range(n_gy)],
            pltpu.VMEM((2 * EDGE, lat), F32),
        ),
        scratch_shapes=[pltpu.VMEM((n_gx, sent, lat), F32)] + fold_scratch,
        compiler_params=PARAMS,
        name="fourier",
    )(*tiles, u, v, quad, surface, depth, mask, north, fold, state)
    blocks = [messages[0]]
    for k in range(1, n_gy):
        ring = [(i, (i + k) % n_gy) for i in range(n_gy)]
        blocks.append(lax.ppermute(messages[k], "gy", ring))
    sched_scratch = [pltpu.SMEM((1, plan.sched_width), jnp.int32), pltpu.SemaphoreType.DMA]
    late = pl.pallas_call(
        lambda *refs: basis_late_kernel(plan, *refs),
        in_specs=[VMEM] * 5,
        out_specs=VMEM,
        out_shape=basis_shape(n_late),
        scratch_shapes=[
            state_shape,
            pltpu.SMEM((1, plan.sched_width), jnp.int32),
            pltpu.SemaphoreType.DMA,
        ],
        cost_estimate=basis_cost(n_late),
        compiler_params=PARAMS,
        name="basis_late",
    )(sched, geo, seeds, state, edges)
    split_shape = pltpu.VMEM((n_gy // 2, plan.k_dev, lat), F32)
    terms = pl.pallas_call(
        lambda *refs: legendre_kernel(plan, *refs),
        in_specs=[VMEM] * (n_gy + 5),
        out_specs=VMEM,
        out_shape=pltpu.VMEM((plan.k_dev + EDGE, lat), F32),
        scratch_shapes=[
            pltpu.VMEM((n_gy, plan.k_dev, lat), F32),
            pltpu.VMEM((slots + 1, 8 * GROUP, half), BF16),
            pltpu.VMEM((plan.love_width // GROUP, 1, ROWS), F32),
            pltpu.VMEM((slots + 1, 4 * GROUP, half), F32),
            pltpu.VMEM((UNROLL, CHAINS, 8 * GROUP, ROWS), BF16),
            pltpu.VMEM((UNROLL, CHAINS, 8 * GROUP, ROWS), BF16),
            split_shape, split_shape,
            pltpu.VMEM((2 * UNROLL * CHAINS, 2, half, ROWS), BF16),
        ]
        + sched_scratch,
        compiler_params=PARAMS,
        name="legendre",
    )(*blocks, early, late, unscale, love, sched)
    everything = spread_gx(terms)
    tile = jax.ShapeDtypeStruct((lon, lat), F32)
    b_table = jnp.asarray(plan.b_table)
    return pl.pallas_call(
        lambda *refs: finish_kernel(plan, *refs),
        in_specs=[VMEM] * (n_gx + 11),
        out_specs=[VMEM] * 4,
        out_shape=(tile,) * 4,
        scratch_shapes=[pltpu.VMEM((n_gx, plan.k_dev + EDGE, lat), F32)],
        compiler_params=PARAMS,
        name="finish",
    )(
        *everything, a_own, a_fold, b_table, blocks[n_gy - 1], blocks[1], edges,
        surface, depth, mask, east, north,
    )


def solution(mesh):
    spec = P("gx", "gy")
    return jax.shard_map(
        on_device,
        mesh=mesh,
        in_specs=(spec, spec, spec, spec, spec, P(), P()),
        out_specs=(spec,) * 4,
        check_vma=False,
    )
```

```python
import math

import numpy as np

import jax
import jax.numpy as jnp
from jax import lax
from jax.experimental import pallas as pl
from jax.experimental.pallas import tpu as pltpu
from jax.sharding import PartitionSpec as P

COURANT = 0.35
GROUP = 8
STEPS = 32
ROWS = GROUP * STEPS
CHAINS = 3
UNROLL = 2
EDGE = 8
EARLY = (6, 12)
F32 = jnp.float32
BF16 = jnp.bfloat16
HIGHEST = lax.Precision.HIGHEST
PARAMS = pltpu.CompilerParams(vmem_limit_bytes=16 * 1024 * 1024)


class Plan:
    def __init__(self, tile_lon, tile_lat, n_gx, n_gy, degrees):
        self.tile_lon, self.tile_lat = tile_lon, tile_lat
        self.n_gx, self.n_gy, self.degrees = n_gx, n_gy, degrees
        self.nlon, self.nlat = tile_lon * n_gx, tile_lat * n_gy
        self.half = self.nlat // 2
        self.n_groups = -(-degrees // GROUP)
        self.n_slots = -(-self.n_groups // n_gx)
        self.k_dev = 2 * self.n_slots * GROUP
        self.k_all = self.k_dev * n_gx
        self.group_of = np.array(
            [
                [s * n_gx + (c if s % 2 == 0 else n_gx - 1 - c) for s in range(self.n_slots)]
                for c in range(n_gx)
            ],
            np.int32,
        )
        self._schedule()
        self._tables()

    def _schedule(self):
        lists = []
        for c in range(self.n_gx):
            counts = []
            for s in range(self.n_slots):
                left = self.degrees - GROUP * int(self.group_of[c, s])
                counts.append(-(-max(left, 0) // STEPS))
            lists.append(counts)
        longest = max(-(-sum(counts) // CHAINS) for counts in lists)
        longest = max(longest, max(max(counts) for counts in lists))
        self.n_iter = -(-longest // UNROLL) * UNROLL
        per_row = self.n_iter * CHAINS * 2
        self.sched_width = -(-per_row // 128) * 128
        self.n_early = self.n_iter * EARLY[0] // EARLY[1]
        self.sched = np.zeros((self.n_gx, 1, self.sched_width), np.int32)
        for c, counts in enumerate(lists):
            chains, room = [[]], self.n_iter
            for s, count in enumerate(counts):
                if room >= count:
                    chains[-1] += [(s, k) for k in range(count)]
                    room -= count
                else:
                    head = count - room
                    chains[-1] += [(s, k) for k in range(head, count)]
                    chains.append([(s, k) for k in range(head)])
                    room = self.n_iter - head
            chains += [[] for _ in range(CHAINS - len(chains))]
            for h, chain in enumerate(chains):
                chain += [(self.n_slots, 0)] * (self.n_iter - len(chain))
                for i, item in enumerate(chain):
                    at = (i * CHAINS + h) * 2
                    self.sched[c, 0, at : at + 2] = item
        top = self.n_gx * (self.n_slots + 1) * GROUP
        self.love_width = -(-(max(top, self.degrees) + 2 * STEPS) // 128) * 128

    def _tables(self):
        rows = np.arange(self.nlat).reshape(2, self.half)
        theta = np.pi * (rows + 0.5) / self.nlat
        self.geo = np.zeros((2, 8, self.half), np.float32)
        self.geo[:, 0] = np.cos(theta)
        self.geo[:, 1] = np.log(np.sin(theta))
        all_theta = np.pi * (np.arange(self.nlat) + 0.5) / self.nlat
        quad = np.pi / self.nlat * (2.0 * np.pi / self.nlon) * np.sin(all_theta)
        self.quad = np.repeat(
            quad.reshape(self.n_gy, 1, self.tile_lat), 8, axis=1
        ).astype(np.float32)
        top = GROUP * (int(self.group_of.max()) + 1)
        factors = np.arange(1, top, dtype=np.float64)
        logs = np.concatenate([[0.0], np.cumsum(0.5 * np.log((2 * factors + 1) / (2 * factors)))])
        orders = self.group_of[:, :, None] * GROUP + np.arange(GROUP)[None, None, :]
        lanes = -(-self.n_gx // 128) * 128
        self.seed_logs = np.zeros((self.n_slots * GROUP, lanes), np.float32)
        self.seed_logs[:, : self.n_gx] = logs[orders].reshape(self.n_gx, -1).T
        lam = 2.0 * np.pi / self.nlon
        cols = np.arange(self.nlon)
        base = (self.group_of[:, :, None] * GROUP * cols[None, None, :]) % self.nlon
        u = np.stack([np.cos(lam * base), np.sin(lam * base)], axis=2)
        pad = -(-2 * self.n_slots // 8) * 8
        self.u_rows = pad
        self.u_table = np.zeros((self.n_gx, pad, self.nlon), np.float32)
        self.u_table[:, : 2 * self.n_slots] = u.reshape(self.n_gx, 2 * self.n_slots, self.nlon)
        small = (np.arange(GROUP)[:, None] * cols[None, :]) % self.nlon
        self.v_table = np.concatenate([np.cos(lam * small), np.sin(lam * small)]).astype(np.float32)
        m = np.concatenate(
            [np.tile(orders[c].reshape(-1), 2) for c in range(self.n_gx)]
        )
        sine = np.tile(np.repeat([0, 1], self.k_dev // 2), self.n_gx)
        nu = np.where(m == 0, 1.0, 2.0) * (m < self.degrees)
        starts = np.arange(self.n_gx) * self.tile_lon
        phase = lam * ((starts[:, None] * m[None, :]) % self.nlon)
        a1 = nu * np.where(sine == 0, np.cos(phase), np.sin(phase))
        a2 = nu * np.where(sine == 0, -np.sin(phase), np.cos(phase))
        self.a_table = np.zeros((self.n_gx, 8, self.k_all), np.float32)
        self.a_table[:, 0] = a1
        self.a_table[:, 1] = a2
        offsets = np.concatenate(
            [
                np.arange(self.tile_lon),
                [self.tile_lon, -1],
                np.zeros(EDGE - 2),
                np.arange(self.tile_lon)[::-1],
            ]
        ).astype(np.int64)
        phase = lam * ((offsets[:, None] * m[None, :]) % self.nlon)
        self.b_table = np.stack([np.cos(phase), np.sin(phase)]).astype(np.float32)
        self.o_rows = offsets.shape[0]


def iota(shape, axis):
    return lax.broadcasted_iota(jnp.int32, shape, axis)


def dot(a, b):
    return lax.dot_general(
        a, b, (((1,), (0,)), ((), ())), precision=HIGHEST, preferred_element_type=F32
    )


def dot3(a, b):
    a_hi, b_hi = a.astype(BF16), b.astype(BF16)
    a_lo = (a - a_hi.astype(F32)).astype(BF16)
    b_lo = (b - b_hi.astype(F32)).astype(BF16)
    n = a.shape[0]
    dims = (((1,), (0,)), ((), ()))
    both = jnp.concatenate([a_hi, a_lo], axis=0)
    big = lax.dot_general(both, b_hi, dims, preferred_element_type=F32)
    small = lax.dot_general(a_hi, b_lo, dims, preferred_element_type=F32)
    return big[:n] + (big[n:] + small)


def select(a, b):
    a_hi = a.astype(BF16)
    both = jnp.concatenate([a_hi, (a - a_hi.astype(F32)).astype(BF16)], axis=0)
    dims = (((1,), (0,)), ((), ()))
    parts = lax.dot_general(both, b.astype(BF16), dims, preferred_element_type=F32)
    return parts[: a.shape[0]] + parts[a.shape[0] :]


def rows_of(columns, size):
    height = columns[0].shape[0]
    diagonal = iota((height, size), 0) == iota((height, size), 1)
    rows = [jnp.sum(jnp.where(diagonal, x, 0.0), axis=0, keepdims=True) for x in columns]
    rows.append(jnp.zeros((EDGE - len(columns), size), F32))
    return jnp.concatenate(rows, axis=0)


def flip_matrix(size, flipped):
    row = iota((size, size), 0)
    col = iota((size, size), 1)
    target = jnp.where(flipped, size - 1 - col, col)
    return jnp.where(row == target, 1.0, 0.0).astype(F32)


def here():
    return lax.axis_index("gx"), lax.axis_index("gy")


def pack_kernel(plan, *refs):
    count = len(refs) // 2 - 1
    height, mask, depth, east = refs[:4]
    sources = refs[:count]
    out, surface_out = refs[count : count + 2]
    kept = refs[count + 2 : 2 * count + 1]
    height_v, sem = refs[2 * count + 1 :]
    c, r = here()
    targets = (height_v,) + tuple(kept)
    copies = []
    for k, (source, target) in enumerate(zip(sources, targets)):
        if k in SLICED_GX:
            source = source.at[c]
        elif k in SLICED_GY:
            source = source.at[r]
        elif k in SLICED_HALF:
            source = source.at[jnp.where(r < plan.n_gy // 2, 0, 1)]
        copies.append(pltpu.make_async_copy(source, target, sem.at[k]))
    for copy in copies:
        copy.start()
    for copy in copies[:4]:
        copy.wait()
    _, mask_v, depth_v, east_v = targets[:4]
    lon, lat = height_v.shape
    wet = mask_v[...].astype(F32)
    surface = wet * height_v[...]
    surface_out[...] = surface
    out[:lon, :] = surface
    out[lon : lon + 1, :] = depth_v[:1, :]
    out[lon + 1 : lon + 2, :] = wet[:1, :]
    out[lon + 2 : lon + 3, :] = depth_v[lon - 1 :, :]
    out[lon + 3 : lon + 4, :] = wet[lon - 1 :, :]
    out[lon + 4 : lon + 5, :] = east_v[lon - 1 :, :]
    columns = [array[:, lat - 1 :] for array in (depth_v, wet, surface)]
    out[lon + 5 :, :] = rows_of(columns, lat)[: EDGE - 5]
    for copy in copies[4:]:
        copy.wait()


def fourier_kernel(plan, *refs):
    n_gx, n_gy, slots = plan.n_gx, plan.n_gy, plan.n_slots
    tiles, refs = refs[: n_gx // 2], refs[n_gx // 2 :]
    u, v, quad, surface, depth, mask, north, fold_v = refs[:8]
    outs, edges, gathered, fold, sem = refs[9 : 9 + n_gy], *refs[9 + n_gy :]
    lon, lat = plan.tile_lon, plan.tile_lat
    c, r = here()
    fetch = pltpu.make_async_copy(fold_v, fold, sem)
    fetch.start()
    for k in range(n_gx):
        half_rows = slice((k % 2) * (lon + EDGE), (k % 2 + 1) * (lon + EDGE))
        gathered[c ^ k] = tiles[k // 2][half_rows, :]
    field = jnp.concatenate([gathered[d, :lon, :] for d in range(n_gx)], axis=0)
    vc, vs = v[:GROUP, :], v[GROUP:, :]
    cos_rows, sin_rows = [], []
    for s in range(slots):
        uc = u[2 * s : 2 * s + 1, :]
        us = u[2 * s + 1 : 2 * s + 2, :]
        cos_rows.append(uc * vc - us * vs)
        sin_rows.append(us * vc + uc * vs)
    trig = jnp.concatenate(cos_rows + sin_rows, axis=0)
    sums = dot3(trig, field) * quad[:1, :]
    flipped = select(sums, flip_matrix(lat, True))
    wet = mask[...].astype(F32)
    columns = [array[:, lat - 1 :] for array in (surface, depth, wet, north)]
    columns += [array[:, :1] for array in (surface, depth, wet)]
    halo = rows_of(columns, lat)
    for k in range(n_gy):
        target = lax.rem(r + k, n_gy)
        same = (r < n_gy // 2) == (target < n_gy // 2)
        outs[k][:EDGE, :] = halo
        outs[k][EDGE:, :] = jnp.where(same, sums, flipped)
    after = lax.rem(c + 1, n_gx)
    before = lax.rem(c + n_gx - 1, n_gx)
    fetch.wait()
    partner = fold[c]
    edges[0:1, :] = gathered[after, 0:1, :]
    edges[1:3, :] = gathered[after, lon : lon + 2, :]
    edges[3:4, :] = gathered[before, lon - 1 : lon, :]
    edges[4:7, :] = gathered[before, lon + 2 : lon + 5, :]
    edges[7:8, :] = jnp.zeros((1, lat), F32)
    edges[EDGE : EDGE + 3, :] = gathered[partner, lon + 5 : lon + EDGE, :]
    edges[EDGE + 3 :, :] = jnp.zeros((EDGE - 3, lat), F32)


def scheduled(plan, c, sched, i, h):
    at = (i * CHAINS + h) * 2
    slot, chunk = sched[0, at], sched[0, at + 1]
    even = lax.rem(slot, 2) == 0
    group = slot * plan.n_gx + jnp.where(even, c, plan.n_gx - 1 - c)
    return slot, chunk, group


def basis_early_kernel(
    plan, sched_v, geo, seed_logs, fold_v, a_table, p_out, seeds, unscale, state, a_own, a_fold,
    sched, fold, sem,
):
    slots, half = plan.n_slots, plan.half
    c, _ = here()
    fetch = pltpu.make_async_copy(sched_v, sched, sem.at[0])
    fetch.start()
    fetch_fold = pltpu.make_async_copy(fold_v, fold, sem.at[1])
    fetch_fold.start()
    fetch_own = pltpu.make_async_copy(a_table.at[c], a_own, sem.at[2])
    fetch_own.start()
    log_sin = geo[1:2, :]
    sub = iota((GROUP, half), 0)
    pick = iota(seed_logs.shape, 1) == c
    logs = jnp.sum(jnp.where(pick, seed_logs[...], 0.0), axis=1, keepdims=True)
    for s in range(slots):
        group = s * plan.n_gx + (c if s % 2 == 0 else plan.n_gx - 1 - c)
        order = (sub + group * GROUP).astype(F32)
        exponent = order * log_sin + logs[s * GROUP : (s + 1) * GROUP]
        shift = jnp.clip(-exponent - 80.0, 0.0, 80.0)
        seeds[s] = jnp.exp(exponent + shift) * (1.0 / math.sqrt(4.0 * math.pi))
        unscale[s] = jnp.exp(-shift)
    state[...] = jnp.zeros(state.shape, F32)
    seeds[slots] = jnp.zeros((GROUP, half), F32)
    unscale[slots] = jnp.zeros((GROUP, half), F32)
    fetch.wait()
    fetch_fold.wait()
    fetch_across = pltpu.make_async_copy(a_table.at[fold[c]], a_fold, sem.at[1])
    fetch_across.start()
    recurrence(plan, c, 0, plan.n_early, sched, geo, seeds, state, p_out)
    fetch_own.wait()
    fetch_across.wait()


def basis_late_kernel(plan, sched_v, geo, seeds, state_in, _, p_out, state, sched, sem):
    c, _ = here()
    fetch = pltpu.make_async_copy(sched_v, sched, sem)
    fetch.start()
    state[...] = state_in[...]
    fetch.wait()
    recurrence(plan, c, plan.n_early, plan.n_iter, sched, geo, seeds, state, p_out)


def recurrence(plan, c, start, stop, sched, geo, seeds, state, p_out):
    slots, half = plan.n_slots, plan.half
    sub = iota((GROUP, half), 0)
    x = jnp.broadcast_to(geo[0:1, :], (GROUP, half))
    sub_c = iota((GROUP, 128), 0)
    lane_c = iota((GROUP, 128), 1)

    def coefficients(i, h):
        _, chunk, group = scheduled(plan, c, sched, i, h)
        m0 = group * GROUP
        degree = (m0 + chunk * STEPS + lane_c).astype(F32)
        order = (m0 + sub_c).astype(F32)
        below = degree - 1.0
        growth = jnp.sqrt(
            jnp.maximum(4.0 * degree * degree - 1.0, 1.0)
            / jnp.maximum(degree * degree - order * order, 1.0)
        )
        damping = jnp.sqrt(
            jnp.maximum(below * below - order * order, 0.0)
            / jnp.maximum(4.0 * below * below - 1.0, 1.0)
        )
        return growth, growth * damping

    def begin(i, h):
        slot, chunk, _ = scheduled(plan, c, sched, i, h)
        started = jnp.where(chunk == 0, 0.0, 1.0).astype(F32)
        seed = seeds[slot] * (1.0 - started)
        return slot, seed, state[slot, 0], state[slot, 1]

    def body(i, carry):
        lanes = [begin(i, h) for h in range(CHAINS)]
        ahead = [coefficients(jnp.minimum(i + 1, stop - 1), h) for h in range(CHAINS)]
        previous = [lane[2] for lane in lanes]
        before = [lane[3] for lane in lanes]
        pairs = [[] for _ in range(CHAINS)]
        for t in range(STEPS):
            for h, (_, seed, _, _) in enumerate(lanes):
                growth, fall = carry[h]
                a = jnp.broadcast_to(growth[:, t : t + 1], (GROUP, half))
                b = jnp.broadcast_to(fall[:, t : t + 1], (GROUP, half))
                value = (a * x) * previous[h] - b * before[h]
                if t < GROUP:
                    value = value + jnp.where(sub == t, seed, 0.0)
                previous[h], before[h] = value, previous[h]
                pairs[h].append(value)
                if t % 2 == 1:
                    both = jnp.concatenate(pairs[h], axis=0)
                    both_hi = both.astype(BF16)
                    at = (t - 1) * GROUP
                    both_lo = (both - both_hi.astype(F32)).astype(BF16)
                    for k in range(half // 128):
                        lanes_k = slice(k * 128, (k + 1) * 128)
                        p_out[i - start, h, 0, k, at : at + 2 * GROUP, :] = both_hi[:, lanes_k]
                        p_out[i - start, h, 1, k, at : at + 2 * GROUP, :] = both_lo[:, lanes_k]
                    pairs[h] = []
        for h, lane in enumerate(lanes):
            state[lane[0], 0] = previous[h]
            state[lane[0], 1] = before[h]
        return tuple(ahead)

    lax.fori_loop(start, stop, body, tuple(coefficients(start, h) for h in range(CHAINS)))


def legendre_kernel(plan, *refs):
    n_gy, slots, half = plan.n_gy, plan.n_slots, plan.half
    lon, lat, k_half = plan.tile_lon, plan.tile_lat, plan.k_dev // 2
    blocks = refs[:n_gy]
    early, late, unscale, love, sched_v, out = refs[n_gy : n_gy + 6]
    (fabs, lhs, weights, acc, coeffs_a, coeffs_b, own_b, mirror_b, turned, sched, sem) = refs[n_gy + 6 :]
    c, r = here()
    fetch = pltpu.make_async_copy(sched_v, sched, sem)
    fetch.start()
    n_half = n_gy // 2
    for k in range(n_gy):
        fabs[lax.rem(r - k + n_gy, n_gy)] = blocks[k][EDGE:, :]
    first_row = jnp.where(r < n_half, 0, n_half)
    sym, anti = [], []
    for b in range(n_half):
        near, far = fabs[first_row + b], fabs[n_gy - 1 - first_row - b]
        sym.append(near + far)
        anti.append(near - far)
    sym = jnp.concatenate(sym, axis=1)
    anti = jnp.concatenate(anti, axis=1)
    for s in range(slots):
        lo, hi = s * GROUP, (s + 1) * GROUP
        rows = jnp.concatenate(
            [sym[lo:hi], anti[lo:hi], sym[k_half + lo : k_half + hi], anti[k_half + lo : k_half + hi]],
            axis=0,
        )
        rows = rows * jnp.concatenate([unscale[s]] * 4, axis=0)
        rows_hi = rows.astype(BF16)
        lhs[s, : 4 * GROUP, :] = rows_hi
        lhs[s, 4 * GROUP :, :] = (rows - rows_hi.astype(F32)).astype(BF16)
    acc[...] = jnp.zeros(acc.shape, F32)
    lhs[slots] = jnp.zeros((8 * GROUP, half), BF16)
    fetch.wait()
    row = iota((4 * GROUP, ROWS), 0)
    lane = iota((4 * GROUP, ROWS), 1)
    i_row, i_lane, t_lane = row % GROUP, lane % GROUP, lane // GROUP
    keep = jnp.where(
        (i_row == i_lane) & ((t_lane + i_row) % 2 == (row // GROUP) % 2), 1.0, 0.0
    ).astype(F32)
    starts = 128 // GROUP
    nt = (((1,), (1,)), ((), ()))
    nn = (((1,), (0,)), ((), ()))
    n = 4 * GROUP

    def matrix(i, h, part):
        basis, at = (early, i) if i < plan.n_early else (late, i - plan.n_early)
        return jnp.concatenate([basis[at, h, part, k] for k in range(half // 128)], axis=1)

    def products(i, h):
        left = lhs[scheduled(plan, c, sched, i, h)[0]]
        at = (i % (2 * UNROLL)) * CHAINS + h
        turned[at, 0] = matrix(i, h, 0).T
        one = lax.dot_general(left, turned[at, 0], nn, preferred_element_type=F32)
        if i < UNROLL:
            two = lax.dot_general(left[:n], matrix(i, h, 1), nt, preferred_element_type=F32)
        else:
            turned[at, 1] = matrix(i, h, 1).T
            two = lax.dot_general(left[:n], turned[at, 1], nn, preferred_element_type=F32)
        return one[:n] + one[n:] + two

    def coefficients(i, h, total):
        _, chunk, group = scheduled(plan, c, sched, i, h)
        begin = group + chunk * (STEPS // GROUP)
        at = (begin // starts + 1) * starts - 1 - lax.rem(begin, starts)
        coeff = total * keep * weights[at]
        coeff_hi = coeff.astype(BF16)
        coeff_lo = (coeff - coeff_hi.astype(F32)).astype(BF16)
        return jnp.concatenate([coeff_hi, coeff_lo], axis=0)

    def synthesise(i, h, right):
        three = lax.dot_general(right, matrix(i, h, 0), nn, preferred_element_type=F32)
        four = lax.dot_general(right[:n], matrix(i, h, 1), nn, preferred_element_type=F32)
        return three[:n] + three[n:] + four

    def analyse_all(k, into):
        for j in range(UNROLL):
            for h in range(CHAINS):
                i = k * UNROLL + j
                into[j, h] = coefficients(i, h, products(i, h))

    def synthesise_all(k, given):
        found = []
        for j in range(UNROLL):
            for h in range(CHAINS):
                i = k * UNROLL + j
                slot = scheduled(plan, c, sched, i, h)[0]
                found.append((slot, synthesise(i, h, given[j, h])))
        for slot, part in found:
            acc[slot] += part

    stages = plan.n_iter // UNROLL
    first = [[products(j, h) for h in range(CHAINS)] for j in range(UNROLL)]
    width = plan.love_width
    padded = jnp.concatenate(
        [love[...].reshape(1, -1), jnp.zeros((1, width - plan.degrees), F32)], axis=1
    )
    shifted = pltpu.roll(
        jnp.broadcast_to(padded, (starts, width)),
        width - GROUP * (starts - 1), 1, stride=GROUP, stride_axis=0,
    )
    shifted = jnp.concatenate(
        [shifted[:, k * 128 : (k + 1) * 128] for k in range(width // 128)], axis=0
    )
    spread = iota((128, ROWS), 1) // GROUP == iota((128, ROWS), 0)
    weights[...] = select(shifted, jnp.where(spread, 1.0, 0.0).astype(F32)).reshape(
        weights.shape
    )
    for j in range(UNROLL):
        for h in range(CHAINS):
            coeffs_a[j, h] = coefficients(j, h, first[j][h])

    trips = (stages - 1) // 2
    for k in range(trips):
        analyse_all(2 * k + 1, coeffs_b)
        synthesise_all(2 * k, coeffs_a)
        analyse_all(2 * k + 2, coeffs_a)
        synthesise_all(2 * k + 1, coeffs_b)
    if stages % 2 == 0:
        analyse_all(stages - 1, coeffs_b)
    synthesise_all(2 * trips, coeffs_a)
    if stages % 2 == 0:
        synthesise_all(stages - 1, coeffs_b)

    for s in range(slots):
        lo, hi = s * GROUP, (s + 1) * GROUP
        g = acc[s] * jnp.concatenate([unscale[s]] * 4, axis=0)
        for part in range(2):
            even = g[2 * part * GROUP : (2 * part + 1) * GROUP]
            odd = g[(2 * part + 1) * GROUP : (2 * part + 2) * GROUP]
            for b in range(n_half):
                lanes = slice(b * lat, (b + 1) * lat)
                where = slice(part * k_half + lo, part * k_half + hi)
                own_b[b, where, :] = even[:, lanes] + odd[:, lanes]
                mirror_b[b, where, :] = even[:, lanes] - odd[:, lanes]
    k_dev = plan.k_dev
    mine = r - first_row
    out[:k_dev, :] = own_b[mine]
    up = jnp.where(
        r == n_half - 1,
        mirror_b[mine][:, lat - 1 :],
        own_b[jnp.minimum(mine + 1, n_half - 1)][:, :1],
    )
    down = jnp.where(
        r == n_half, mirror_b[mine][:, :1], own_b[jnp.maximum(mine - 1, 0)][:, lat - 1 :]
    )
    out[k_dev:, :] = rows_of([up, down], lat)


def finish_kernel(plan, *refs):
    n_gx = plan.n_gx
    received, refs = refs[:n_gx], refs[n_gx:]
    a_own, a_fold, b_table, north_tile, south_tile, edges, surface_ref, depth_ref = refs[:8]
    mask, east_ref, north_ref, sal_out, east_out, north_out, height_out, terms = refs[8:]
    c, r = here()
    for k in range(n_gx):
        terms[c ^ k] = received[k][...]
    lon, lat = plan.tile_lon, plan.tile_lat
    split = lon + EDGE
    own_trig = a_own[0:1, :] * b_table[0, :split, :] + a_own[1:2, :] * b_table[1, :split, :]
    fold_trig = a_fold[0:1, :] * b_table[0, split:, :] + a_fold[1:2, :] * b_table[1, split:, :]
    trig = jnp.concatenate([own_trig, fold_trig], axis=0)
    k_dev = plan.k_dev
    main = jnp.concatenate([terms[d, :k_dev, :] for d in range(n_gx)], axis=0)
    sal_all = dot3(trig, main)
    up = jnp.concatenate([terms[d, k_dev : k_dev + 1, :k_dev] for d in range(n_gx)], axis=1)
    down = jnp.concatenate([terms[d, k_dev + 1 : k_dev + 2, :k_dev] for d in range(n_gx)], axis=1)
    sal_up = jnp.sum(trig[:lon] * up, axis=1, keepdims=True)
    sal_down = jnp.sum(trig[:lon] * down, axis=1, keepdims=True)
    sal = sal_all[:lon, :lat]
    sal_out[...] = sal
    is_top = r == plan.n_gy - 1
    sal_n = jnp.where(is_top, sal_all[split:, lat - 1 :], sal_up)
    sal_s = sal_down
    surface, depth = surface_ref[...], depth_ref[...]
    wet = mask[...].astype(F32)
    east, north = east_ref[...], north_ref[...]
    i, j = iota((lon, lat), 0), iota((lon, lat), 1)

    def column(row, picked):
        return jnp.sum(jnp.where(picked, row, 0.0), axis=1, keepdims=True)

    def beside(tile, k):
        return column(tile[k : k + 1, :], i == j)

    def fold_value(k):
        return column(edges[EDGE + k : EDGE + k + 1, :], i + j == lon - 1)

    surf_n = jnp.where(is_top, fold_value(2), beside(north_tile, 4))
    depth_n = jnp.where(is_top, fold_value(0), beside(north_tile, 5))
    wet_n = jnp.where(is_top, fold_value(1), beside(north_tile, 6))
    pressure = surface - sal
    row = iota((lon, lat), 0)
    lane = iota((lon, lat), 1)

    def east_of(field, edge):
        return jnp.where(row == lon - 1, edge, pltpu.roll(field, lon - 1, 0))

    def north_of(field, edge):
        return jnp.where(lane == lat - 1, edge, pltpu.roll(field, lat - 1, 1))

    p_e = edges[0:1, :] - sal_all[lon : lon + 1, :lat]
    p_w = edges[3:4, :] - sal_all[lon + 1 : lon + 2, :lat]
    east_next = wet * east_of(wet, edges[2:3, :]) * (
        east - COURANT * (east_of(pressure, p_e) - pressure)
    )
    north_next = wet * north_of(wet, wet_n) * (
        north - COURANT * (north_of(pressure, surf_n - sal_n) - pressure)
    )
    east_out[...] = east_next
    north_out[...] = north_next
    east_flux = 0.5 * (depth + east_of(depth, edges[1:2, :])) * east_next
    north_flux = 0.5 * (depth + north_of(depth, depth_n)) * north_next
    west_face = edges[5:6, :] * wet[:1] * (edges[6:7, :] - COURANT * (pressure[:1] - p_w))
    west_edge = 0.5 * (edges[4:5, :] + depth[:1]) * west_face
    south_face = beside(south_tile, 2) * wet[:, :1] * (
        beside(south_tile, 3) - COURANT * (pressure[:, :1] - (beside(south_tile, 0) - sal_s))
    )
    south_edge = 0.5 * (beside(south_tile, 1) + depth[:, :1]) * south_face
    south_edge = jnp.where(r > 0, south_edge, 0.0)
    west_flux = jnp.where(row == 0, west_edge, pltpu.roll(east_flux, 1, 0))
    south_flux = jnp.where(lane == 0, south_edge, pltpu.roll(north_flux, 1, 1))
    height_out[...] = wet * (
        surface - COURANT * (east_flux - west_flux + north_flux - south_flux)
    )


def spread_gx(x):
    size = lax.axis_size("gx")

    def swap(value, k):
        return lax.ppermute(value, "gx", [(i, i ^ k) for i in range(size)])

    parts = [x] + [None] * (size - 1)
    for k in sorted(range(2, size, 2), key=lambda k: -bin(k).count("1")):
        parts[k] = swap(x, k)
    for k in range(0, size, 2):
        parts[k + 1] = swap(parts[k], 1)
    return parts


def pairs_gx(x):
    size = lax.axis_size("gx")

    def swap(value, k):
        return lax.ppermute(value, "gx", [(i, i ^ k) for i in range(size)])

    both = jnp.concatenate([x, swap(x, 1)], axis=0)
    parts = [both] + [None] * (size // 2 - 1)
    for k in sorted(range(2, size, 2), key=lambda k: -bin(k).count("1")):
        parts[k // 2] = swap(both, k)
    return parts


VMEM = pl.BlockSpec(memory_space=pltpu.VMEM)
HBM = pl.BlockSpec(memory_space=pltpu.HBM)
SLICED_GX = (5, 10)
SLICED_GY = (7,)
SLICED_HALF = (8,)


def on_device(height, east_speed, north_speed, water_depth, ocean_mask, fold_partner, love_factor):
    lon, lat = height.shape
    n_gx, n_gy = lax.axis_size("gx"), lax.axis_size("gy")
    plan = Plan(lon, lat, n_gx, n_gy, love_factor.shape[0])
    slots, half = plan.n_slots, plan.half
    sent = lon + EDGE
    sources = (
        height, ocean_mask, water_depth, east_speed, north_speed, plan.u_table, plan.v_table,
        plan.quad, plan.geo, plan.seed_logs, plan.sched, love_factor, fold_partner,
    )
    sources = tuple(
        pltpu.with_memory_space_constraint(jnp.asarray(source), pltpu.HBM) for source in sources
    )
    kept_shapes = [
        source.shape[1:] if k in SLICED_GX + SLICED_GY + SLICED_HALF else source.shape
        for k, source in enumerate(sources)
    ]
    kept = [
        pltpu.VMEM(shape, source.dtype) for shape, source in zip(kept_shapes[1:], sources[1:])
    ]
    packed, surface, *kept = pl.pallas_call(
        lambda *refs: pack_kernel(plan, *refs),
        in_specs=[HBM] * len(sources),
        out_specs=[VMEM] * (len(sources) + 1),
        out_shape=(pltpu.VMEM((sent, lat), F32), pltpu.VMEM((lon, lat), F32), *kept),
        scratch_shapes=[pltpu.VMEM((lon, lat), F32), pltpu.SemaphoreType.DMA((len(sources),))],
        compiler_params=PARAMS,
        name="pack",
    )(*sources)
    mask, depth, east, north, u, v, quad, geo, seed_logs, sched, love, fold = kept
    tiles = pairs_gx(packed)
    a_table = pltpu.with_memory_space_constraint(jnp.asarray(plan.a_table), pltpu.HBM)
    table_shape = pltpu.VMEM((slots + 1, GROUP, half), F32)
    state_shape = pltpu.VMEM((slots + 1, 2, GROUP, half), F32)

    def basis_shape(count):
        return pltpu.VMEM((count, CHAINS, 2, half // 128, ROWS, 128), BF16)

    def basis_cost(count):
        return pl.CostEstimate(
            flops=5_000_000 * count, bytes_accessed=1_000_000, transcendentals=0
        )

    n_early, n_late = plan.n_early, plan.n_iter - plan.n_early
    early, seeds, unscale, state, a_own, a_fold = pl.pallas_call(
        lambda *refs: basis_early_kernel(plan, *refs),
        in_specs=[VMEM] * 4 + [HBM],
        out_specs=[VMEM] * 6,
        out_shape=(
            basis_shape(n_early), table_shape, table_shape, state_shape,
            pltpu.VMEM((8, plan.k_all), F32),
            pltpu.VMEM((8, plan.k_all), F32),
        ),
        scratch_shapes=[
            pltpu.SMEM((1, plan.sched_width), jnp.int32),
            pltpu.SMEM((n_gx,), jnp.int32),
            pltpu.SemaphoreType.DMA((3,)),
        ],
        cost_estimate=basis_cost(n_early),
        compiler_params=PARAMS,
        name="basis_early",
    )(sched, geo, seed_logs, fold, a_table)
    rows = EDGE + plan.k_dev
    fold_scratch = [pltpu.SMEM((n_gx,), jnp.int32), pltpu.SemaphoreType.DMA]
    *messages, edges = pl.pallas_call(
        lambda *refs: fourier_kernel(plan, *refs),
        in_specs=[VMEM] * (n_gx // 2 + 9),
        out_specs=[VMEM] * (n_gy + 1),
        out_shape=(
            *[pltpu.VMEM((rows, lat), F32) for _ in range(n_gy)],
            pltpu.VMEM((2 * EDGE, lat), F32),
        ),
        scratch_shapes=[pltpu.VMEM((n_gx, sent, lat), F32)] + fold_scratch,
        compiler_params=PARAMS,
        name="fourier",
    )(*tiles, u, v, quad, surface, depth, mask, north, fold, state)
    blocks = [messages[0]]
    for k in range(1, n_gy):
        ring = [(i, (i + k) % n_gy) for i in range(n_gy)]
        blocks.append(lax.ppermute(messages[k], "gy", ring))
    sched_scratch = [pltpu.SMEM((1, plan.sched_width), jnp.int32), pltpu.SemaphoreType.DMA]
    late = pl.pallas_call(
        lambda *refs: basis_late_kernel(plan, *refs),
        in_specs=[VMEM] * 5,
        out_specs=VMEM,
        out_shape=basis_shape(n_late),
        scratch_shapes=[
            state_shape,
            pltpu.SMEM((1, plan.sched_width), jnp.int32),
            pltpu.SemaphoreType.DMA,
        ],
        cost_estimate=basis_cost(n_late),
        compiler_params=PARAMS,
        name="basis_late",
    )(sched, geo, seeds, state, edges)
    split_shape = pltpu.VMEM((n_gy // 2, plan.k_dev, lat), F32)
    terms = pl.pallas_call(
        lambda *refs: legendre_kernel(plan, *refs),
        in_specs=[VMEM] * (n_gy + 5),
        out_specs=VMEM,
        out_shape=pltpu.VMEM((plan.k_dev + EDGE, lat), F32),
        scratch_shapes=[
            pltpu.VMEM((n_gy, plan.k_dev, lat), F32),
            pltpu.VMEM((slots + 1, 8 * GROUP, half), BF16),
            pltpu.VMEM((plan.love_width // GROUP, 1, ROWS), F32),
            pltpu.VMEM((slots + 1, 4 * GROUP, half), F32),
            pltpu.VMEM((UNROLL, CHAINS, 8 * GROUP, ROWS), BF16),
            pltpu.VMEM((UNROLL, CHAINS, 8 * GROUP, ROWS), BF16),
            split_shape, split_shape,
            pltpu.VMEM((2 * UNROLL * CHAINS, 2, half, ROWS), BF16),
        ]
        + sched_scratch,
        compiler_params=PARAMS,
        name="legendre",
    )(*blocks, early, late, unscale, love, sched)
    everything = spread_gx(terms)
    tile = jax.ShapeDtypeStruct((lon, lat), F32)
    b_table = jnp.asarray(plan.b_table)
    return pl.pallas_call(
        lambda *refs: finish_kernel(plan, *refs),
        in_specs=[VMEM] * (n_gx + 11),
        out_specs=[VMEM] * 4,
        out_shape=(tile,) * 4,
        scratch_shapes=[pltpu.VMEM((n_gx, plan.k_dev + EDGE, lat), F32)],
        compiler_params=PARAMS,
        name="finish",
    )(
        *everything, a_own, a_fold, b_table, blocks[n_gy - 1], blocks[1], edges,
        surface, depth, mask, east, north,
    )


def solution(mesh):
    spec = P("gx", "gy")
    return jax.shard_map(
        on_device,
        mesh=mesh,
        in_specs=(spec, spec, spec, spec, spec, P(), P()),
        out_specs=(spec,) * 4,
        check_vma=False,
    )
```
